256 devices in a mesh: seq: 128 (over y, z_hi, x, core), ch: 2 (over z_lo).
Axes of the slice: x: 4, y: 4, z: 8 (z_hi: 4, z_lo: 2; z = z_hi * 2 + z_lo), core: 2. Of those that a mesh axis runs over, the one named last changes fastest.
Arguments:
- tokens: bfloat16 [16384, 8192], P('seq', 'ch'), may hold values from -6 to 6
- query_in: bfloat16 [16384, 8192], P('seq', 'ch'), may hold values from -6 to 6
- key_in: bfloat16 [16384, 8192], P('seq', 'ch'), may hold values from -6 to 6
- proj_in: bfloat16 [8192, 1536], P('ch', 'seq'), may hold values from -0.0625 to 0.0625
- proj_out: bfloat16 [1536, 8192], P('seq', 'ch'), may hold values from -0.15625 to 0.15625
- short_taps: float32 [3, 7, 8192], P(None, None, 'ch'), may hold values from -2.4 to 2.4
- residues: float32 [16, 8192], P(None, 'ch'), may hold values from -1.8 to 1.8
- mode_rates: float32 [16, 8192], P(None, 'ch'), may hold values from 3.0517578e-05 to 0.03
- skip_gain: float32 [8192], P('ch'), may hold values from -3 to 3
Outputs:
- operator_out: bfloat16 [16384, 8192], P('seq', 'ch')
The draws below stay inside these ranges and needn't reach their ends.
All inputs are finite; a program needn't handle non-finite values.
Results may differ from the reference program's by a relative error of at most 0.0069.
Values may be sent and summed in bfloat16 or wider, within the bound.
A program may use at most 192 MiB of HBM per device.

```python
import math
import jax
import jax.numpy as jnp
from jax import lax

D = 8192
R = 1536
SHORT = 7
MODES = 16
SEQ = 16384


def steps_of(key, extent, cuts, low, top_value):
    gain, own = 1.0, jax.random.fold_in(key, 6)
    for axis_at, blocks in cuts:
        draws = jnp.exp(jax.random.uniform(jax.random.fold_in(own, axis_at), (blocks,), jnp.float32, low / len(cuts), top_value / len(cuts)))
        gain = gain * jnp.repeat(draws, extent[axis_at] // blocks).reshape([-1 if axis == axis_at else 1 for axis in range(len(extent))])
    return gain


def bell_draw(stream_key, shape, deviation, most, pieces=(), kind=jnp.bfloat16):
    entries = jax.random.normal(stream_key, shape, jnp.float32) * deviation
    if len(pieces) > 0:
        entries = steps_of(stream_key, shape, pieces, -0.22, 0.18) * entries
    return jnp.clip(entries, min=-most, max=most).astype(kind)


def setup_inputs(seed: int = 0) -> dict:
    key_list = jax.random.split(jax.random.key(seed), 10)
    return {
        "tokens": bell_draw(key_list[0], (SEQ, D), 1.0, 6.0, ((0, 128), (1, 2))),
        "query_in": bell_draw(key_list[1], (SEQ, D), 1.0, 6.0, ((0, 128), (1, 2))),
        "key_in": bell_draw(key_list[2], (SEQ, D), 1.0, 6.0, ((0, 128), (1, 2))),
        "proj_in": bell_draw(key_list[3], (D, R), D ** -0.5, 0.0625, ((0, 2), (1, 128))),
        "proj_out": bell_draw(key_list[4], (R, D), R ** -0.5, 0.15625, ((0, 128), (1, 2))),
        "short_taps": bell_draw(key_list[5], (3, SHORT, D), 0.4, 2.4, ((2, 2),), jnp.float32),
        "residues": bell_draw(key_list[6], (MODES, D), 0.3, 1.8, ((1, 2),), jnp.float32),
        "mode_rates": jnp.clip(jnp.exp(math.log(0.03) - 6.89065 * jax.random.uniform(key_list[7], (MODES, D), jnp.float32) ** steps_of(key_list[7], (MODES, D), ((1, 2),), -0.2, 0.2)), 3.0517578125e-05, 0.03),
        "skip_gain": bell_draw(key_list[8], (D,), 0.5, 3.0, ((0, 2),), jnp.float32),
    }


def causal_short(signal, filter_taps):
    margin_rows = filter_taps.shape[0] - 1
    length = signal.shape[0]
    padded = jnp.pad(signal, ((margin_rows, 0), (0, 0)))
    result = filter_taps[0] * padded[margin_rows:margin_rows + length]
    for offset in range(1, margin_rows + 1):
        result = result + filter_taps[offset] * padded[margin_rows - offset:margin_rows - offset + length]
    return result

def long_block(operands):
    mixed_block, residue_block, rate_block = operands
    positions = jnp.arange(SEQ).astype(jnp.float32)[:, None]
    impulse = jnp.zeros((SEQ, mixed_block.shape[1]), jnp.float32)
    for mode_index in range(MODES):
        impulse = impulse + residue_block[mode_index] * jnp.sqrt(rate_block[mode_index]) * jnp.exp(-rate_block[mode_index] * positions)
    spectrum = jnp.fft.rfft(mixed_block.astype(jnp.float32), n=2 * SEQ, axis=0) * jnp.fft.rfft(impulse, n=2 * SEQ, axis=0)
    return jnp.fft.irfft(spectrum, n=2 * SEQ, axis=0)[:SEQ].astype(jnp.bfloat16)

def reference(tokens, query_in, key_in, proj_in, proj_out, short_taps, residues, mode_rates, skip_gain):
    low_rank = jnp.dot(tokens, proj_in, preferred_element_type=jnp.float32).astype(jnp.bfloat16)
    value_proj = jnp.dot(low_rank, proj_out, preferred_element_type=jnp.float32).astype(jnp.bfloat16)
    query_short = causal_short(query_in.astype(jnp.float32), short_taps[0])
    key_short = causal_short(key_in.astype(jnp.float32), short_taps[1])
    value_short = causal_short(value_proj.astype(jnp.float32), short_taps[2])
    mixed = (key_short * value_short).astype(jnp.bfloat16)
    blocks = D // 128
    mixed_blocks = mixed.reshape(SEQ, blocks, 128).transpose(1, 0, 2)
    residue_blocks = residues.reshape(MODES, blocks, 128).transpose(1, 0, 2)
    rate_blocks = mode_rates.reshape(MODES, blocks, 128).transpose(1, 0, 2)
    convolved = lax.map(long_block, (mixed_blocks, residue_blocks, rate_blocks))
    convolved = convolved.transpose(1, 0, 2).reshape(SEQ, D)
    return (query_short * (convolved.astype(jnp.float32) + skip_gain * mixed.astype(jnp.float32))).astype(jnp.bfloat16)
```

```python
import jax
import jax.numpy as jnp
from jax import lax
from jax.experimental import pallas as pl
from jax.experimental.pallas import tpu as pltpu
from jax.sharding import Mesh
from jax.sharding import PartitionSpec as P

ROWS = 128
WIDE = 4096
LANES = 128
TILES = WIDE // LANES
GROUPS = TILES // 8
MODES = 16
TAPS = 7
SEQ_AXES = ("y", "zh", "x", "core")


def spread(source, edge, scratch):
    for tile in range(TILES):
        columns = slice(tile * LANES, (tile + 1) * LANES)
        scratch[tile * 8 : tile * 8 + 8, :] = edge[:, columns]

    @pl.loop(0, ROWS // 16)
    def _(pair):
        for tile in range(TILES):
            columns = slice(tile * LANES, (tile + 1) * LANES)
            block = source[pl.ds(pl.multiple_of(pair * 16, 16), 16), columns].astype(jnp.float32)
            base = pl.multiple_of((2 * pair + 1) * TILES * 8 + tile * 8, 8)
            scratch[pl.ds(base, 8), :] = block[:8]
            scratch[pl.ds(base + TILES * 8, 8), :] = block[8:]


def row_of(scratch, eight, group, row):
    start = (eight + (1 if row >= 0 else 0)) * TILES * 8 + group * 64 + row % 8
    return scratch[pl.ds(start, 8, stride=8), :]


def short(rows, taps, step):
    result = taps[0] * rows[step + 6]
    for offset in range(1, TAPS):
        result = result + taps[offset] * rows[step + 6 - offset]
    return result


def mix_kernel(key, value, key_edge, value_edge, taps, decay, mixed, state, key_rows, value_rows):
    spread(key, key_edge, key_rows)
    spread(value, value_edge, value_rows)
    for group in range(GROUPS):
        key_taps = [taps[1, j, group] for j in range(TAPS)]
        value_taps = [taps[2, j, group] for j in range(TAPS)]

        @pl.loop(0, ROWS // 8)
        def _(eight):
            keys = [row_of(key_rows, eight, group, r) for r in range(-6, 8)]
            values = [row_of(value_rows, eight, group, r) for r in range(-6, 8)]
            for step in range(8):
                product = short(keys, key_taps, step) * short(values, value_taps, step)
                product = product.astype(jnp.bfloat16).astype(jnp.float32)
                mixed[eight * 8 + step, group * 8 : group * 8 + 8, :] = product

    for group in range(GROUPS):
        rates = [decay[n, group] for n in range(MODES)]

        def advance(eight, held):
            held = list(held)
            for step in range(8):
                entry = mixed[eight * 8 + step, group * 8 : group * 8 + 8, :]
                held = [rates[n] * held[n] + entry for n in range(MODES)]
            return tuple(held)

        held = lax.fori_loop(
            0, ROWS // 8, advance, (jnp.zeros((8, LANES), jnp.float32),) * MODES
        )
        for n in range(MODES):
            state[pl.ds(group * 128 + n, 8, stride=16), :] = held[n]


def scan_kernel(arrived, decay, before):
    rate = decay[...]

    def advance(block, held):
        before[block] = held
        return rate * held + arrived[block]

    lax.fori_loop(0, arrived.shape[0], advance, jnp.zeros(rate.shape, jnp.float32))


def out_kernel(query, query_edge, mixed, state, taps, decay, weight, skip, out, query_rows, out_rows):
    spread(query, query_edge, query_rows)
    for group in range(GROUPS):
        rates = [decay[n, group] for n in range(MODES)]
        weights = [weight[n, group] for n in range(MODES)]

        def advance(eight, held):
            held = list(held)
            for step in range(8):
                entry = mixed[eight * 8 + step, group * 8 : group * 8 + 8, :]
                held = [rates[n] * held[n] + entry for n in range(MODES)]
                terms = [weights[n] * held[n] for n in range(MODES)]
                while len(terms) > 1:
                    terms = [terms[i] + terms[i + 1] for i in range(0, len(terms), 2)]
                start = eight * TILES * 8 + group * 64 + step
                out_rows[pl.ds(start, 8, stride=8), :] = terms[0]
            return tuple(held)

        first = tuple(state[pl.ds(group * 128 + n, 8, stride=16), :] for n in range(MODES))
        lax.fori_loop(0, ROWS // 8, advance, first)

    for group in range(GROUPS):
        query_taps = [taps[0, j, group] for j in range(TAPS)]
        skip_part = skip[group]

        @pl.loop(0, ROWS // 8)
        def _(eight):
            queries = [row_of(query_rows, eight, group, r) for r in range(-6, 8)]
            for step in range(8):
                entry = mixed[eight * 8 + step, group * 8 : group * 8 + 8, :]
                start = eight * TILES * 8 + group * 64 + step
                convolved = out_rows[pl.ds(start, 8, stride=8), :]
                convolved = convolved.astype(jnp.bfloat16).astype(jnp.float32)
                out_rows[pl.ds(start, 8, stride=8), :] = short(queries, query_taps, step) * (
                    convolved + skip_part * entry
                )

    @pl.loop(0, ROWS // 16)
    def _(pair):
        for tile in range(TILES):
            base = pl.multiple_of(2 * pair * TILES * 8 + tile * 8, 8)
            block = jnp.concatenate(
                [out_rows[pl.ds(base, 8), :], out_rows[pl.ds(base + TILES * 8, 8), :]], axis=0
            )
            out[pl.ds(pl.multiple_of(pair * 16, 16), 16), tile * LANES : (tile + 1) * LANES] = (
                block.astype(jnp.bfloat16)
            )


def grouped(value):
    return value.reshape(*value.shape[:-1], GROUPS, 8, LANES)


def long_part(query_in, key_in, value_proj, edges, short_taps, residues, mode_rates, skip_gain):
    f32 = jnp.float32
    rows_scratch = pltpu.VMEM(((ROWS + 8) * TILES, LANES), f32)
    taps = grouped(short_taps)
    decay = grouped(jnp.exp(-mode_rates))
    weight = grouped(residues * jnp.sqrt(mode_rates))
    mixed, state = pl.pallas_call(
        mix_kernel,
        out_shape=(
            jax.ShapeDtypeStruct((ROWS, TILES, LANES), f32),
            jax.ShapeDtypeStruct((TILES * MODES, LANES), f32),
        ),
        scratch_shapes=[rows_scratch, rows_scratch],
        compiler_params=pltpu.CompilerParams(vmem_limit_bytes=40 * 2**20),
    )(key_in, value_proj, edges[1], edges[2], taps, decay)
    seq = 128
    sent = state.reshape(seq, 4, LANES)
    arrived = lax.all_to_all(sent, SEQ_AXES, split_axis=0, concat_axis=0, tiled=True)
    me = lax.axis_index(SEQ_AXES)
    mine = lax.dynamic_slice(mode_rates, (me % 4 * 4, me // 4 * LANES), (4, LANES))
    before = pl.pallas_call(
        scan_kernel, out_shape=jax.ShapeDtypeStruct((seq, 4, LANES), f32)
    )(arrived, jnp.exp(-ROWS * mine))
    first = lax.all_to_all(before, SEQ_AXES, split_axis=0, concat_axis=0, tiled=True)
    return pl.pallas_call(
        out_kernel,
        out_shape=jax.ShapeDtypeStruct((ROWS, WIDE), jnp.bfloat16),
        scratch_shapes=[rows_scratch, pltpu.VMEM((ROWS * TILES, LANES), f32)],
        compiler_params=pltpu.CompilerParams(vmem_limit_bytes=40 * 2**20),
    )(
        query_in,
        edges[0],
        mixed,
        first.reshape(TILES * MODES, LANES),
        taps,
        decay,
        weight,
        grouped(skip_gain),
    )


def value_part(tokens, proj_in, proj_out):
    f32 = jnp.float32
    places = ("y", "zh", "x")
    swap = [(0, 1), (1, 0)]
    other_tokens = lax.ppermute(tokens, "core", swap)
    in_rows = lax.all_gather(proj_in.T, places, axis=0, tiled=True)
    out_rows = lax.all_gather(proj_out, places, axis=0, tiled=True)
    contract = (((1,), (1,)), ((), ()))
    chip_tokens = jnp.concatenate([tokens, other_tokens], axis=0)
    partial = lax.dot_general(chip_tokens, in_rows, contract, preferred_element_type=f32)
    other = lax.ppermute(partial, "ch", swap)
    low_rank = (partial + other).astype(jnp.bfloat16)
    sent = jnp.dot(low_rank[ROWS:], out_rows, preferred_element_type=f32)
    arrived = lax.ppermute(sent, "core", swap)
    kept = jnp.dot(low_rank[:ROWS], out_rows, preferred_element_type=f32)
    return (kept + arrived).astype(jnp.bfloat16)


def per_device(
    tokens, query_in, key_in, proj_in, proj_out, short_taps, residues, mode_rates, skip_gain
):
    value_proj = value_part(tokens, proj_in, proj_out)
    ring = [(i, i + 1) for i in range(127)]
    margin = TAPS - 1

    def edge_of(last):
        edge = lax.ppermute(last, SEQ_AXES, ring)
        return jnp.pad(edge.astype(jnp.float32), ((0, 0), (2, 0), (0, 0)))

    early = edge_of(jnp.stack([query_in[ROWS - margin :], key_in[ROWS - margin :]]))
    late = edge_of(value_proj[None, ROWS - margin :])
    edges = (early[0], early[1], late[0])
    return long_part(
        query_in, key_in, value_proj, edges, short_taps, residues, mode_rates, skip_gain
    )


def solution(mesh):
    split = Mesh(mesh.devices.reshape(4, 4, 4, 2, 2), ("y", "zh", "x", "core", "ch"))
    both = P(SEQ_AXES, "ch")
    placed = (
        both,
        both,
        both,
        P("ch", SEQ_AXES),
        both,
        P(None, None, "ch"),
        P(None, "ch"),
        P(None, "ch"),
        P("ch"),
    )
    return jax.shard_map(
        per_device, mesh=split, in_specs=placed, out_specs=both, check_vma=False
    )
```

```python
import jax
import jax.numpy as jnp
from jax import lax
from jax.experimental import pallas as pl
from jax.experimental.pallas import tpu as pltpu
from jax.sharding import Mesh
from jax.sharding import PartitionSpec as P

ROWS = 128
WIDE = 4096
LANES = 128
TILES = WIDE // LANES
GROUPS = TILES // 8
MODES = 16
TAPS = 7
SEQ_AXES = ("y", "zh", "x", "core")


def spread(source, edge, scratch):
    for tile in range(TILES):
        columns = slice(tile * LANES, (tile + 1) * LANES)
        scratch[tile * 8 : tile * 8 + 8, :] = edge[:, columns]

    @pl.loop(0, ROWS // 16)
    def _(pair):
        for tile in range(TILES):
            columns = slice(tile * LANES, (tile + 1) * LANES)
            block = source[pl.ds(pl.multiple_of(pair * 16, 16), 16), columns].astype(jnp.float32)
            base = pl.multiple_of((2 * pair + 1) * TILES * 8 + tile * 8, 8)
            scratch[pl.ds(base, 8), :] = block[:8]
            scratch[pl.ds(base + TILES * 8, 8), :] = block[8:]


def row_of(scratch, eight, group, row):
    start = (eight + (1 if row >= 0 else 0)) * TILES * 8 + group * 64 + row % 8
    return scratch[pl.ds(start, 8, stride=8), :]


def short(rows, taps, step):
    result = taps[0] * rows[step + 6]
    for offset in range(1, TAPS):
        result = result + taps[offset] * rows[step + 6 - offset]
    return result


def mix_kernel(key, value, key_edge, value_edge, taps, decay, mixed, state, key_rows, value_rows):
    spread(key, key_edge, key_rows)
    spread(value, value_edge, value_rows)
    for group in range(GROUPS):
        key_taps = [taps[1, j, group] for j in range(TAPS)]
        value_taps = [taps[2, j, group] for j in range(TAPS)]

        @pl.loop(0, ROWS // 8)
        def _(eight):
            keys = [row_of(key_rows, eight, group, r) for r in range(-6, 8)]
            values = [row_of(value_rows, eight, group, r) for r in range(-6, 8)]
            for step in range(8):
                product = short(keys, key_taps, step) * short(values, value_taps, step)
                product = product.astype(jnp.bfloat16).astype(jnp.float32)
                mixed[eight * 8 + step, group * 8 : group * 8 + 8, :] = product

    for group in range(GROUPS):
        rates = [decay[n, group] for n in range(MODES)]

        def advance(eight, held):
            held = list(held)
            for step in range(8):
                entry = mixed[eight * 8 + step, group * 8 : group * 8 + 8, :]
                held = [rates[n] * held[n] + entry for n in range(MODES)]
            return tuple(held)

        held = lax.fori_loop(
            0, ROWS // 8, advance, (jnp.zeros((8, LANES), jnp.float32),) * MODES
        )
        for n in range(MODES):
            state[pl.ds(group * 128 + n, 8, stride=16), :] = held[n]


def scan_kernel(arrived, decay, before):
    rate = decay[...]

    def advance(block, held):
        before[block] = held
        return rate * held + arrived[block]

    lax.fori_loop(0, arrived.shape[0], advance, jnp.zeros(rate.shape, jnp.float32))


def out_kernel(query, query_edge, mixed, state, taps, decay, weight, skip, out, query_rows, out_rows):
    spread(query, query_edge, query_rows)
    for group in range(GROUPS):
        rates = [decay[n, group] for n in range(MODES)]
        weights = [weight[n, group] for n in range(MODES)]

        def advance(eight, held):
            held = list(held)
            for step in range(8):
                entry = mixed[eight * 8 + step, group * 8 : group * 8 + 8, :]
                held = [rates[n] * held[n] + entry for n in range(MODES)]
                terms = [weights[n] * held[n] for n in range(MODES)]
                while len(terms) > 1:
                    terms = [terms[i] + terms[i + 1] for i in range(0, len(terms), 2)]
                start = eight * TILES * 8 + group * 64 + step
                out_rows[pl.ds(start, 8, stride=8), :] = terms[0]
            return tuple(held)

        first = tuple(state[pl.ds(group * 128 + n, 8, stride=16), :] for n in range(MODES))
        lax.fori_loop(0, ROWS // 8, advance, first)

    for group in range(GROUPS):
        query_taps = [taps[0, j, group] for j in range(TAPS)]
        skip_part = skip[group]

        @pl.loop(0, ROWS // 8)
        def _(eight):
            queries = [row_of(query_rows, eight, group, r) for r in range(-6, 8)]
            for step in range(8):
                entry = mixed[eight * 8 + step, group * 8 : group * 8 + 8, :]
                start = eight * TILES * 8 + group * 64 + step
                convolved = out_rows[pl.ds(start, 8, stride=8), :]
                convolved = convolved.astype(jnp.bfloat16).astype(jnp.float32)
                out_rows[pl.ds(start, 8, stride=8), :] = short(queries, query_taps, step) * (
                    convolved + skip_part * entry
                )

    @pl.loop(0, ROWS // 16)
    def _(pair):
        for tile in range(TILES):
            base = pl.multiple_of(2 * pair * TILES * 8 + tile * 8, 8)
            block = jnp.concatenate(
                [out_rows[pl.ds(base, 8), :], out_rows[pl.ds(base + TILES * 8, 8), :]], axis=0
            )
            out[pl.ds(pl.multiple_of(pair * 16, 16), 16), tile * LANES : (tile + 1) * LANES] = (
                block.astype(jnp.bfloat16)
            )


def grouped(value):
    return value.reshape(*value.shape[:-1], GROUPS, 8, LANES)


def long_part(query_in, key_in, value_proj, edges, short_taps, residues, mode_rates, skip_gain):
    f32 = jnp.float32
    rows_scratch = pltpu.VMEM(((ROWS + 8) * TILES, LANES), f32)
    taps = grouped(short_taps)
    decay = grouped(jnp.exp(-mode_rates))
    weight = grouped(residues * jnp.sqrt(mode_rates))
    mixed, state = pl.pallas_call(
        mix_kernel,
        out_shape=(
            jax.ShapeDtypeStruct((ROWS, TILES, LANES), f32),
            jax.ShapeDtypeStruct((TILES * MODES, LANES), f32),
        ),
        scratch_shapes=[rows_scratch, rows_scratch],
        compiler_params=pltpu.CompilerParams(vmem_limit_bytes=40 * 2**20),
    )(key_in, value_proj, edges[1], edges[2], taps, decay)
    seq = 128
    sent = state.reshape(seq, 4, LANES)
    arrived = lax.all_to_all(sent, SEQ_AXES, split_axis=0, concat_axis=0, tiled=True)
    me = lax.axis_index(SEQ_AXES)
    mine = lax.dynamic_slice(mode_rates, (me % 4 * 4, me // 4 * LANES), (4, LANES))
    before = pl.pallas_call(
        scan_kernel, out_shape=jax.ShapeDtypeStruct((seq, 4, LANES), f32)
    )(arrived, jnp.exp(-ROWS * mine))
    first = lax.all_to_all(before, SEQ_AXES, split_axis=0, concat_axis=0, tiled=True)
    return pl.pallas_call(
        out_kernel,
        out_shape=jax.ShapeDtypeStruct((ROWS, WIDE), jnp.bfloat16),
        scratch_shapes=[rows_scratch, pltpu.VMEM((ROWS * TILES, LANES), f32)],
        compiler_params=pltpu.CompilerParams(vmem_limit_bytes=40 * 2**20),
    )(
        query_in,
        edges[0],
        mixed,
        first.reshape(TILES * MODES, LANES),
        taps,
        decay,
        weight,
        grouped(skip_gain),
    )


MESH = pl.DeviceIdType.MESH
BLOCK = 48
QUARTER = 1024
UNITS = ((0, 0), (1, 0), (0, 1), (0, 3), (0, 2), (1, 1), (1, 3), (1, 2))


def value_kernel(
    tokens,
    pad_in,
    pad_out,
    value,
    chip_tokens,
    stage,
    weights,
    partial,
    theirs,
    low,
    total,
    arrived,
    own_sem,
    token_sems,
    stage_send,
    stage_recv,
    deep_send,
    deep_recv,
    ring_send,
    ring_recv,
    part_send,
    part_recv,
    swap_send,
    swap_recv,
):
    y, zh, x = lax.axis_index("y"), lax.axis_index("zh"), lax.axis_index("x")
    core, ch = lax.axis_index("core"), lax.axis_index("ch")
    place = {"x": x, "y": y}
    pads = (pad_in, pad_out)
    started = []

    def step(position, by):
        return lax.rem(position + by, 4)

    def copy(source, target, send, recv, device):
        return pltpu.make_async_remote_copy(
            src_ref=source,
            dst_ref=target,
            send_sem=send,
            recv_sem=recv,
            device_id=device,
            device_id_type=MESH,
        )

    def send(*arguments):
        made = copy(*arguments)
        made.start()
        started.append(made)

    barrier = pltpu.get_barrier_semaphore()
    greeted = [{"core": 1 - core}, {"ch": 1 - ch}]
    greeted += [{axis: step(at, by)} for axis, at in (("x", x), ("zh", zh)) for by in (1, 2, 3)]
    greeted += [{"y": step(y, by)} for by in (1, 3)]
    for device in greeted:
        pl.semaphore_signal(barrier, inc=1, device_id=device, device_id_type=MESH)
    own_copy = pltpu.make_async_copy(tokens, chip_tokens.at[0], own_sem)
    own_copy.start()
    pl.semaphore_wait(barrier, len(greeted))

    for f in range(2):
        for by in (1, 3, 2):
            to = step(x, by)
            columns = pl.ds(pl.multiple_of(to * QUARTER, QUARTER), QUARTER)
            send(
                pads[f].at[:, columns],
                stage.at[f, x],
                stage_send.at[f, by - 1],
                stage_recv.at[f, by - 1],
                {"x": to},
            )
    send(tokens, chip_tokens.at[1], token_sems.at[0], token_sems.at[1], {"core": 1 - core})

    def settle(f):
        columns = pl.ds(pl.multiple_of(x * QUARTER, QUARTER), QUARTER)
        own = pltpu.make_async_copy(pads[f].at[:, columns], stage.at[f, x], own_sem)
        own.start()
        own.wait()
        for by in (1, 3, 2):
            came = stage.at[f, step(x, 4 - by)]
            copy(came, came, stage_send.at[f, by - 1], stage_recv.at[f, by - 1], {"x": x}).wait_recv()
        parts = [stage[f, i].astype(jnp.float32)[:12] for i in range(4)]
        weights[f, y, zh, x] = jnp.concatenate(parts, axis=0).astype(jnp.bfloat16)

    def send_deep(f):
        block = weights.at[f, y, zh, x]
        for by in (1, 3, 2):
            send(block, block, deep_send.at[f, by - 1], deep_recv.at[f, by - 1], {"zh": step(zh, by)})

    def wait_deep(f, r):
        by = 4 - r
        block = weights.at[f, y, step(zh, r), x]
        copy(block, block, deep_send.at[f, by - 1], deep_recv.at[f, by - 1], {"zh": zh}).wait_recv()

    def ring(unit, late):
        f, r = UNITS[unit]
        deep = step(zh, r)
        across = (f + r) % 2 == 0
        axis = "x" if across != late else "y"
        at = place[axis]

        def item(i, half=None):
            if not late:
                columns = slice(None) if half is None else slice(half * 512, half * 512 + 512)
                if across:
                    return weights.at[f, y, deep, i, :, columns]
                return weights.at[f, i, deep, x, :, columns]
            blocks = slice(None) if half is None else slice(half * 2, half * 2 + 2)
            if across:
                return weights.at[f, i, deep, blocks]
            return weights.at[f, blocks, deep, i]

        base = 4 if late else 0
        plus, minus = step(at, 1), step(at, 3)

        def out(ref, slot, to):
            send(ref, ref, ring_send.at[unit, base + slot], ring_recv.at[unit, base + slot], {axis: to})

        def landed(ref, slot):
            copy(
                ref, ref, ring_send.at[unit, base + slot], ring_recv.at[unit, base + slot], {axis: at}
            ).wait_recv()

        def first():
            out(item(at), 0, plus)
            out(item(at), 1, minus)

        def forward():
            landed(item(minus), 0)
            out(item(minus, 0), 2, plus)
            landed(item(plus), 1)
            out(item(plus, 1), 3, minus)

        def finish():
            landed(item(step(at, 2), 0), 2)
            landed(item(step(at, 2), 1), 3)

        return first, forward, finish

    early = [ring(unit, False) for unit in range(8)]
    late = [ring(unit, True) for unit in range(8)]

    def unit_weights(f, r, quarter):
        return weights[f, :, step(zh, r), quarter].reshape(4 * BLOCK, QUARTER)

    def project(r):
        @pl.loop(0, 4)
        def _(quarter):
            columns = pl.ds(pl.multiple_of(quarter * QUARTER, QUARTER), QUARTER)
            part = lax.dot_general(
                chip_tokens[:, :, columns].reshape(2 * ROWS, QUARTER),
                unit_weights(0, r, quarter),
                (((1,), (1,)), ((), ())),
                preferred_element_type=jnp.float32,
            )

            @pl.when(quarter == 0)
            def _():
                partial[r] = part

            @pl.when(quarter > 0)
            def _():
                partial[r] += part

        send(partial.at[r], theirs.at[r], part_send.at[r], part_recv.at[r], {"ch": 1 - ch})

    def join(r):
        copy(partial.at[r], theirs.at[r], part_send.at[r], part_recv.at[r], {"ch": ch}).wait_recv()
        low[r] = (partial[r] + theirs[r]).astype(jnp.bfloat16)

    def expand(r, opening, closing):
        for quarter in range(4):
            part = jnp.dot(
                low[r], unit_weights(1, r, quarter), preferred_element_type=jnp.float32
            ).reshape(2, ROWS, QUARTER)
            if opening:
                total[:, quarter] = part
            else:
                total[:, quarter] += part
            if closing:
                send(
                    total.at[1, quarter],
                    arrived.at[quarter],
                    swap_send.at[quarter],
                    swap_recv.at[quarter],
                    {"core": 1 - core},
                )

    FIRST, FORWARD, FINISH = range(3)
    own_copy.wait()
    settle(0)
    early[0][FIRST]()
    send_deep(0)
    settle(1)
    early[1][FIRST]()
    send_deep(1)
    for unit in (0, 1):
        early[unit][FORWARD]()
    for unit in (0, 1):
        early[unit][FINISH]()
        late[unit][FIRST]()
    for group in ((2, 3, 4), (5, 6, 7)):
        for unit in group:
            wait_deep(*UNITS[unit])
            early[unit][FIRST]()
        for unit in group:
            early[unit][FORWARD]()
        for unit in group:
            early[unit][FINISH]()
            late[unit][FIRST]()
        if group[0] == 2:
            for unit in (0, 1):
                late[unit][FORWARD]()
    copy(tokens, chip_tokens.at[1], token_sems.at[0], token_sems.at[1], {"core": core}).wait_recv()
    late[0][FINISH]()
    project(0)
    late[1][FINISH]()
    late[2][FORWARD]()
    late[4][FORWARD]()
    late[3][FORWARD]()
    join(0)
    expand(0, True, False)
    for unit in (2, 4, 3):
        late[unit][FINISH]()
        project(UNITS[unit][1])
    late[5][FORWARD]()
    late[7][FORWARD]()
    late[6][FORWARD]()
    for r in (1, 2, 3):
        join(r)
    late[5][FINISH]()
    expand(1, False, False)
    late[7][FINISH]()
    expand(2, False, False)
    late[6][FINISH]()
    expand(3, False, True)
    for quarter in range(4):
        copy(
            arrived.at[quarter],
            arrived.at[quarter],
            swap_send.at[quarter],
            swap_recv.at[quarter],
            {"core": core},
        ).wait_recv()
        columns = slice(quarter * QUARTER, quarter * QUARTER + QUARTER)
        value[:, columns] = (total[0, quarter] + arrived[quarter]).astype(jnp.bfloat16)
    for made in started:
        made.wait_send()


def value_part(tokens, proj_in, proj_out):
    f32, bf16 = jnp.float32, jnp.bfloat16
    pad = ((0, 4), (0, 0))
    dma = pltpu.SemaphoreType.DMA
    return pl.pallas_call(
        value_kernel,
        out_shape=jax.ShapeDtypeStruct((ROWS, WIDE), bf16),
        in_specs=[pl.BlockSpec(memory_space=pltpu.VMEM)] * 3,
        out_specs=pl.BlockSpec(memory_space=pltpu.VMEM),
        scratch_shapes=[
            pltpu.VMEM((2, ROWS, WIDE), bf16),
            pltpu.VMEM((2, 4, 16, QUARTER), bf16),
            pltpu.VMEM((2, 4, 4, 4, BLOCK, QUARTER), bf16),
            pltpu.VMEM((4, 2 * ROWS, 4 * BLOCK), f32),
            pltpu.VMEM((4, 2 * ROWS, 4 * BLOCK), f32),
            pltpu.VMEM((4, 2 * ROWS, 4 * BLOCK), bf16),
            pltpu.VMEM((2, 4, ROWS, QUARTER), f32),
            pltpu.VMEM((4, ROWS, QUARTER), f32),
            dma,
            dma((2,)),
            dma((2, 3)),
            dma((2, 3)),
            dma((2, 3)),
            dma((2, 3)),
            dma((8, 8)),
            dma((8, 8)),
            dma((4,)),
            dma((4,)),
            dma((4,)),
            dma((4,)),
        ],
        compiler_params=pltpu.CompilerParams(
            collective_id=0, has_side_effects=True, vmem_limit_bytes=56 * 2**20
        ),
    )(tokens, jnp.pad(proj_in.T, pad), jnp.pad(proj_out, pad))


def per_device(
    tokens, query_in, key_in, proj_in, proj_out, short_taps, residues, mode_rates, skip_gain
):
    value_proj = value_part(tokens, proj_in, proj_out)
    ring = [(i, i + 1) for i in range(127)]
    margin = TAPS - 1

    def edge_of(last):
        edge = lax.ppermute(last, SEQ_AXES, ring)
        return jnp.pad(edge.astype(jnp.float32), ((0, 0), (2, 0), (0, 0)))

    early = edge_of(jnp.stack([query_in[ROWS - margin :], key_in[ROWS - margin :]]))
    late = edge_of(value_proj[None, ROWS - margin :])
    edges = (early[0], early[1], late[0])
    return long_part(
        query_in, key_in, value_proj, edges, short_taps, residues, mode_rates, skip_gain
    )


def solution(mesh):
    split = Mesh(mesh.devices.reshape(4, 4, 4, 2, 2), ("y", "zh", "x", "core", "ch"))
    both = P(SEQ_AXES, "ch")
    placed = (
        both,
        both,
        both,
        P("ch", SEQ_AXES),
        both,
        P(None, None, "ch"),
        P(None, "ch"),
        P(None, "ch"),
        P("ch"),
    )
    return jax.shard_map(
        per_device, mesh=split, in_specs=placed, out_specs=both, check_vma=False
    )
```

```python
import jax
import jax.numpy as jnp
from jax import lax
from jax.experimental import pallas as pl
from jax.experimental.pallas import tpu as pltpu
from jax.sharding import Mesh
from jax.sharding import PartitionSpec as P

ROWS = 128
WIDE = 4096
LANES = 128
TILES = WIDE // LANES
GROUPS = TILES // 8
MODES = 16
TAPS = 7
SEQ_AXES = ("y", "zh", "x", "core")
MESH = pl.DeviceIdType.MESH
BLOCK = 48
QUARTER = 1024
RANKS = 12
UNITS = ((0, 0), (1, 0), (0, 1), (0, 3), (0, 2), (1, 1), (1, 3), (1, 2))


def lanes_of(tile):
    return slice(tile * LANES, (tile + 1) * LANES)


def spread(source, edge, first_block, scratch):
    for tile in range(TILES):
        above = edge[:, lanes_of(tile)].astype(jnp.float32)
        scratch[tile * 8 : tile * 8 + 8, :] = jnp.where(first_block, 0.0, above)

    @pl.loop(0, ROWS // 16)
    def _(pair):
        for tile in range(TILES):
            rows = pl.ds(pl.multiple_of(pair * 16, 16), 16)
            block = source[rows, lanes_of(tile)].astype(jnp.float32)
            base = pl.multiple_of((2 * pair + 1) * TILES * 8 + tile * 8, 8)
            scratch[pl.ds(base, 8), :] = block[:8]
            scratch[pl.ds(base + TILES * 8, 8), :] = block[8:]


def row_of(scratch, eight, group, row):
    start = (eight + (1 if row >= 0 else 0)) * TILES * 8 + group * 64 + row % 8
    return scratch[pl.ds(start, 8, stride=8), :]


def short(rows, taps, step):
    result = taps[0] * rows[step + 6]
    for offset in range(1, TAPS):
        result = result + taps[offset] * rows[step + 6 - offset]
    return result


def summed(terms):
    while len(terms) > 1:
        terms = [terms[i] + terms[i + 1] for i in range(0, len(terms), 2)]
    return terms[0]


def operator_kernel(
    tokens,
    pad_in,
    pad_out,
    query_in,
    key_in,
    short_taps,
    residues,
    mode_rates,
    skip_gain,
    out,
    value,
    chip_tokens,
    stage,
    weights,
    partial,
    theirs,
    low,
    total,
    arrived,
    edges,
    rows,
    tap_rows,
    rate_rows,
    weight_rows,
    queries,
    mixed,
    local,
    states,
    carried,
    group_states,
    group_before,
    deep_states,
    wide_states,
    own_sem,
    token_sems,
    stage_send,
    stage_recv,
    deep_send,
    deep_recv,
    ring_send,
    ring_recv,
    part_send,
    part_recv,
    swap_send,
    swap_recv,
    edge_send,
    edge_recv,
    near_send,
    near_recv,
    scan_send,
    scan_recv,
    back_send,
    back_recv,
):
    y, zh, x = lax.axis_index("y"), lax.axis_index("zh"), lax.axis_index("x")
    core, ch = lax.axis_index("core"), lax.axis_index("ch")
    place = {"x": x, "y": y, "zh": zh}
    pads = (pad_in, pad_out)
    started = []
    near = x * 2 + core
    block_at = (y * 4 + zh) * 8 + near
    first_block = block_at == 0

    def step(position, by):
        return lax.rem(position + by, 4)

    def copy(source, target, send, recv, device):
        return pltpu.make_async_remote_copy(
            src_ref=source,
            dst_ref=target,
            send_sem=send,
            recv_sem=recv,
            device_id=device,
            device_id_type=MESH,
        )

    def send(*arguments):
        made = copy(*arguments)
        made.start()
        started.append(made)

    def near_device(by):
        to = lax.rem(near + by, 8)
        return to, {"x": to // 2, "core": lax.rem(to, 2)}

    def block_device(by):
        to = lax.rem(block_at + by, 128)
        return {
            "y": to // 32,
            "zh": lax.rem(to // 8, 4),
            "x": lax.rem(to // 2, 4),
            "core": lax.rem(to, 2),
        }

    def send_edge(i, source):
        send(
            source.at[pl.ds(ROWS - 8, 8)],
            edges.at[i],
            edge_send.at[i],
            edge_recv.at[i],
            block_device(1),
        )

    def wait_edge(i):
        edge = edges.at[i]
        copy(edge, edge, edge_send.at[i], edge_recv.at[i], {"ch": ch}).wait_recv()

    barrier = pltpu.get_barrier_semaphore()
    greeted = [{"ch": 1 - ch}, block_device(1), block_device(127)]
    greeted += [near_device(by)[1] for by in range(1, 8)]
    greeted += [{axis: step(place[axis], by)} for axis in ("zh", "y") for by in (1, 2, 3)]
    for device in greeted:
        pl.semaphore_signal(barrier, inc=1, device_id=device, device_id_type=MESH)
    own_copy = pltpu.make_async_copy(tokens, chip_tokens.at[0], own_sem)
    own_copy.start()
    pl.semaphore_wait(barrier, len(greeted))

    for f in range(2):
        for by in (1, 3, 2):
            to = step(x, by)
            columns = pl.ds(pl.multiple_of(to * QUARTER, QUARTER), QUARTER)
            send(
                pads[f].at[:, columns],
                stage.at[f, x],
                stage_send.at[f, by - 1],
                stage_recv.at[f, by - 1],
                {"x": to},
            )
    send(tokens, chip_tokens.at[1], token_sems.at[0], token_sems.at[1], {"core": 1 - core})
    for i, source in enumerate((query_in, key_in)):
        send_edge(i, source)

    def settle(f):
        columns = pl.ds(pl.multiple_of(x * QUARTER, QUARTER), QUARTER)
        own = pltpu.make_async_copy(pads[f].at[:, columns], stage.at[f, x], own_sem)
        own.start()
        own.wait()
        for by in (1, 3, 2):
            came = stage.at[f, step(x, 4 - by)]
            copy(came, came, stage_send.at[f, by - 1], stage_recv.at[f, by - 1], {"x": x}).wait_recv()
        parts = [stage[f, i].astype(jnp.float32) for i in range(4)]
        weights[f, y, zh, x] = jnp.concatenate(parts, axis=0).astype(jnp.bfloat16)

    def send_deep(f):
        block = weights.at[f, y, zh, x]
        for by in (1, 3, 2):
            send(block, block, deep_send.at[f, by - 1], deep_recv.at[f, by - 1], {"zh": step(zh, by)})

    def wait_deep(f, r):
        by = 4 - r
        block = weights.at[f, y, step(zh, r), x]
        copy(block, block, deep_send.at[f, by - 1], deep_recv.at[f, by - 1], {"zh": zh}).wait_recv()

    def ring(unit, late):
        f, r = UNITS[unit]
        deep = step(zh, r)
        across = (f + r) % 2 == 0
        axis = "x" if across != late else "y"
        at = place[axis]

        def item(i, half=None):
            if not late:
                columns = slice(None) if half is None else slice(half * 512, half * 512 + 512)
                if across:
                    return weights.at[f, y, deep, i, :, columns]
                return weights.at[f, i, deep, x, :, columns]
            blocks = slice(None) if half is None else slice(half * 2, half * 2 + 2)
            if across:
                return weights.at[f, i, deep, blocks]
            return weights.at[f, blocks, deep, i]

        base = 4 if late else 0
        plus, minus = step(at, 1), step(at, 3)

        def out(ref, slot, to):
            send(ref, ref, ring_send.at[unit, base + slot], ring_recv.at[unit, base + slot], {axis: to})

        def landed(ref, slot):
            copy(
                ref, ref, ring_send.at[unit, base + slot], ring_recv.at[unit, base + slot], {axis: at}
            ).wait_recv()

        def first():
            out(item(at), 0, plus)
            out(item(at), 1, minus)

        def forward():
            landed(item(minus), 0)
            out(item(minus, 0), 2, plus)
            landed(item(plus), 1)
            out(item(plus, 1), 3, minus)

        def finish():
            landed(item(step(at, 2), 0), 2)
            landed(item(step(at, 2), 1), 3)

        return first, forward, finish

    early = [ring(unit, False) for unit in range(8)]
    late = [ring(unit, True) for unit in range(8)]

    def unit_weights(f, r, quarter):
        return weights[f, :, step(zh, r), quarter].reshape(4 * BLOCK, QUARTER)

    def project(r):
        @pl.loop(0, 4)
        def _(quarter):
            columns = pl.ds(pl.multiple_of(quarter * QUARTER, QUARTER), QUARTER)
            part = lax.dot_general(
                chip_tokens[:, :, columns].reshape(2 * ROWS, QUARTER),
                unit_weights(0, r, quarter),
                (((1,), (1,)), ((), ())),
                preferred_element_type=jnp.float32,
            )

            @pl.when(quarter == 0)
            def _():
                partial[r] = part

            @pl.when(quarter > 0)
            def _():
                partial[r] += part

        send(partial.at[r], theirs.at[r], part_send.at[r], part_recv.at[r], {"ch": 1 - ch})

    def join(r):
        copy(partial.at[r], theirs.at[r], part_send.at[r], part_recv.at[r], {"ch": ch}).wait_recv()
        low[r] = (partial[r] + theirs[r]).astype(jnp.bfloat16)

    def expand(r, opening, closing):
        for quarter in range(4):
            part = jnp.dot(
                low[r], unit_weights(1, r, quarter), preferred_element_type=jnp.float32
            ).reshape(2, ROWS, QUARTER)
            if opening:
                total[:, quarter] = part
            else:
                total[:, quarter] += part
            if closing:
                send(
                    total.at[1, quarter],
                    arrived.at[quarter],
                    swap_send.at[quarter],
                    swap_recv.at[quarter],
                    {"core": 1 - core},
                )


    def tap_of(branch, offset, group):
        start = (branch * TILES + group * 8) * 8 + offset
        return tap_rows[pl.ds(start, 8, stride=8), :]

    def mode_of(ref, n, group):
        half, row = n // 8, n % 8
        return ref[half, pl.ds(group * 64 + row, 8, stride=8), :]

    def at_group(group):
        return slice(group * 8, group * 8 + 8)

    def filtered(branch, target):
        for group in range(GROUPS):
            taps = [tap_of(branch, j, group) for j in range(TAPS)]

            @pl.loop(0, ROWS // 8)
            def _(eight):
                window = [row_of(rows, eight, group, r) for r in range(-6, 8)]
                for i in range(8):
                    target(eight * 8 + i, group, short(window, taps, i))

    def prepare():
        for tile in range(TILES):
            for branch in range(3):
                base = (branch * TILES + tile) * 8
                tap_rows[base : base + TAPS, :] = short_taps[branch, :, lanes_of(tile)]
            for half in range(2):
                modes = slice(half * 8, half * 8 + 8)
                rate = mode_rates[modes, lanes_of(tile)]
                rate_rows[half, tile * 8 : tile * 8 + 8, :] = rate
                weight_rows[half, tile * 8 : tile * 8 + 8, :] = (
                    residues[modes, lanes_of(tile)] * jnp.sqrt(rate)
                )

        def keep_query(t, group, result):
            queries[t, at_group(group), :] = result

        def keep_key(t, group, result):
            mixed[t, at_group(group), :] = result

        wait_edge(0)
        spread(query_in, edges.at[0], first_block, rows)
        filtered(0, keep_query)
        wait_edge(1)
        spread(key_in, edges.at[1], first_block, rows)
        filtered(1, keep_key)

    def mix():
        def keep(t, group, result):
            product = mixed[t, at_group(group), :] * result
            mixed[t, at_group(group), :] = product.astype(jnp.bfloat16).astype(jnp.float32)

        wait_edge(2)
        spread(value, edges.at[2], first_block, rows)
        filtered(2, keep)

    def decays(group):
        return [jnp.exp(-mode_of(rate_rows, n, group)) for n in range(MODES)]

    zeros = (jnp.zeros((8, LANES), jnp.float32),) * MODES

    def summarize(group):
        rates = decays(group)

        def advance(eight, held):
            for i in range(8):
                entry = mixed[eight * 8 + i, at_group(group), :]
                held = tuple(rates[n] * held[n] + entry for n in range(MODES))
            return held

        held = lax.fori_loop(0, ROWS // 8, advance, zeros)
        for n in range(MODES):
            states[n // 8, pl.ds(group * 64 + n % 8, 8, stride=8), :] = held[n]

    def localize(group):
        rates = decays(group)
        weighting = [mode_of(weight_rows, n, group) for n in range(MODES)]

        def advance(eight, held):
            for i in range(8):
                entry = mixed[eight * 8 + i, at_group(group), :]
                held = tuple(rates[n] * held[n] + entry for n in range(MODES))
                local[eight * 8 + i, at_group(group), :] = summed(
                    [weighting[n] * held[n] for n in range(MODES)]
                )
            return held

        lax.fori_loop(0, ROWS // 8, advance, zeros)

    def finish_group(group):
        rates = decays(group)
        skip = skip_gain[at_group(group), :]
        first = tuple(
            mode_of(weight_rows, n, group) * mode_of(carried, n, group) for n in range(MODES)
        )

        def advance(eight, held):
            for i in range(8):
                held = tuple(rates[n] * held[n] for n in range(MODES))
                t = eight * 8 + i
                convolved = local[t, at_group(group), :] + summed(list(held))
                convolved = convolved.astype(jnp.bfloat16).astype(jnp.float32)
                result = queries[t, at_group(group), :] * (
                    convolved + skip * mixed[t, at_group(group), :]
                )
                rows[pl.ds(eight * TILES * 8 + group * 64 + i, 8, stride=8), :] = result
            return held

        lax.fori_loop(0, ROWS // 8, advance, first)

    def near_part(at):
        return pl.ds(pl.multiple_of(at * 32, 32), 32)

    def exchange_states():
        for by in range(1, 8):
            to, device = near_device(by)
            send(
                states.at[:, near_part(to)],
                group_states.at[near],
                near_send.at[by - 1],
                near_recv.at[by - 1],
                device,
            )
        localize(0)
        localize(1)
        rate = rate_rows[:, near_part(near), :]
        one = jnp.exp(-float(ROWS) * rate)
        eight = jnp.exp(-8.0 * ROWS * rate)
        group_states[near] = states[:, near_part(near), :]
        for by in range(1, 8):
            came = group_states.at[lax.rem(near + 8 - by, 8)]
            copy(came, came, near_send.at[by - 1], near_recv.at[by - 1], {"ch": ch}).wait_recv()
        held = jnp.zeros(rate.shape, jnp.float32)
        for k in range(8):
            group_before[k] = held
            held = one * held + group_states[k]

        def across(buffer, axis, slot, own, decay, cover):
            at = place[axis]
            buffer[at] = own
            for by in (1, 3, 2):
                send(
                    buffer.at[at],
                    buffer.at[at],
                    scan_send.at[slot, by - 1],
                    scan_recv.at[slot, by - 1],
                    {axis: step(at, by)},
                )
            cover()
            for by in (1, 3, 2):
                came = buffer.at[step(at, 4 - by)]
                copy(
                    came, came, scan_send.at[slot, by - 1], scan_recv.at[slot, by - 1], {"ch": ch}
                ).wait_recv()
            running = jnp.zeros(own.shape, jnp.float32)
            before = running
            for k in range(4):
                before = jnp.where(at == k, running, before)
                running = decay * running + buffer[k]
            return before, running

        deep_before, deep_total = across(
            deep_states, "zh", 0, held, eight, lambda: (localize(2), localize(3))
        )
        wide_before, _ = across(
            wide_states, "y", 1, deep_total, jnp.exp(-32.0 * ROWS * rate), lambda: None
        )
        shift = jnp.exp(rate * (-8.0 * ROWS * zh.astype(jnp.float32)))
        entering = deep_before + shift * wide_before
        for k in range(8):
            group_before[k] += entering
            entering = one * entering
        for by in range(1, 8):
            to, device = near_device(by)
            send(
                group_before.at[to],
                carried.at[:, near_part(near)],
                back_send.at[by - 1],
                back_recv.at[by - 1],
                device,
            )
        carried[:, near_part(near), :] = group_before[near]
        for by in range(1, 8):
            came = carried.at[:, near_part(lax.rem(near + 8 - by, 8))]
            copy(came, came, back_send.at[by - 1], back_recv.at[by - 1], {"ch": ch}).wait_recv()

    FIRST, FORWARD, FINISH = range(3)
    own_copy.wait()
    settle(0)
    early[0][FIRST]()
    send_deep(0)
    settle(1)
    early[1][FIRST]()
    send_deep(1)
    for unit in (0, 1):
        early[unit][FORWARD]()
    for unit in (0, 1):
        early[unit][FINISH]()
        late[unit][FIRST]()
    for group in ((2, 3, 4), (5, 6, 7)):
        for unit in group:
            wait_deep(*UNITS[unit])
            early[unit][FIRST]()
        for unit in group:
            early[unit][FORWARD]()
        for unit in group:
            early[unit][FINISH]()
            late[unit][FIRST]()
        if group[0] == 2:
            for unit in (0, 1):
                late[unit][FORWARD]()
    prepare()
    copy(tokens, chip_tokens.at[1], token_sems.at[0], token_sems.at[1], {"core": core}).wait_recv()
    late[0][FINISH]()
    project(0)
    late[1][FINISH]()
    late[2][FORWARD]()
    late[4][FORWARD]()
    late[3][FORWARD]()
    join(0)
    expand(0, True, False)
    for unit in (2, 4, 3):
        late[unit][FINISH]()
        project(UNITS[unit][1])
    late[5][FORWARD]()
    late[7][FORWARD]()
    late[6][FORWARD]()
    for r in (1, 2, 3):
        join(r)
    late[5][FINISH]()
    expand(1, False, False)
    late[7][FINISH]()
    expand(2, False, False)
    late[6][FINISH]()
    expand(3, False, True)
    for quarter in range(4):
        copy(
            arrived.at[quarter],
            arrived.at[quarter],
            swap_send.at[quarter],
            swap_recv.at[quarter],
            {"core": core},
        ).wait_recv()
        columns = slice(quarter * QUARTER, quarter * QUARTER + QUARTER)
        value[:, columns] = (total[0, quarter] + arrived[quarter]).astype(jnp.bfloat16)
    send_edge(2, value)
    mix()
    for group in range(GROUPS):
        summarize(group)
    exchange_states()
    for group in range(GROUPS):
        finish_group(group)

    @pl.loop(0, ROWS // 16)
    def _(pair):
        for tile in range(TILES):
            base = pl.multiple_of(2 * pair * TILES * 8 + tile * 8, 8)
            block = jnp.concatenate(
                [rows[pl.ds(base, 8), :], rows[pl.ds(base + TILES * 8, 8), :]], axis=0
            )
            out[pl.ds(pl.multiple_of(pair * 16, 16), 16), lanes_of(tile)] = block.astype(
                jnp.bfloat16
            )

    for made in started:
        made.wait_send()


def per_device(
    tokens, query_in, key_in, proj_in, proj_out, short_taps, residues, mode_rates, skip_gain
):
    f32, bf16 = jnp.float32, jnp.bfloat16
    dma = pltpu.SemaphoreType.DMA
    return pl.pallas_call(
        operator_kernel,
        out_shape=jax.ShapeDtypeStruct((ROWS, WIDE), bf16),
        in_specs=[pl.BlockSpec(memory_space=pltpu.VMEM)] * 9,
        out_specs=pl.BlockSpec(memory_space=pltpu.VMEM),
        scratch_shapes=[
            pltpu.VMEM((ROWS, WIDE), bf16),
            pltpu.VMEM((2, ROWS, WIDE), bf16),
            pltpu.VMEM((2, 4, RANKS, QUARTER), bf16),
            pltpu.VMEM((2, 4, 4, 4, BLOCK, QUARTER), bf16),
            pltpu.VMEM((4, 2 * ROWS, 4 * BLOCK), f32),
            pltpu.VMEM((4, 2 * ROWS, 4 * BLOCK), f32),
            pltpu.VMEM((4, 2 * ROWS, 4 * BLOCK), bf16),
            pltpu.VMEM((2, 4, ROWS, QUARTER), f32),
            pltpu.VMEM((4, ROWS, QUARTER), f32),
            pltpu.VMEM((3, 8, WIDE), bf16),
            pltpu.VMEM(((ROWS + 8) * TILES, LANES), f32),
            pltpu.VMEM((3 * TILES * 8, LANES), f32),
            pltpu.VMEM((2, TILES * 8, LANES), f32),
            pltpu.VMEM((2, TILES * 8, LANES), f32),
            pltpu.VMEM((ROWS, TILES, LANES), f32),
            pltpu.VMEM((ROWS, TILES, LANES), f32),
            pltpu.VMEM((ROWS, TILES, LANES), f32),
            pltpu.VMEM((2, TILES * 8, LANES), f32),
            pltpu.VMEM((2, TILES * 8, LANES), f32),
            pltpu.VMEM((8, 2, 32, LANES), f32),
            pltpu.VMEM((8, 2, 32, LANES), f32),
            pltpu.VMEM((4, 2, 32, LANES), f32),
            pltpu.VMEM((4, 2, 32, LANES), f32),
            dma,
            dma((2,)),
            dma((2, 3)),
            dma((2, 3)),
            dma((2, 3)),
            dma((2, 3)),
            dma((8, 8)),
            dma((8, 8)),
            dma((4,)),
            dma((4,)),
            dma((4,)),
            dma((4,)),
            dma((3,)),
            dma((3,)),
            dma((7,)),
            dma((7,)),
            dma((2, 3)),
            dma((2, 3)),
            dma((7,)),
            dma((7,)),
        ],
        compiler_params=pltpu.CompilerParams(
            collective_id=0, has_side_effects=True, vmem_limit_bytes=60 * 2**20
        ),
    )(
        tokens,
        proj_in.T,
        proj_out,
        query_in,
        key_in,
        short_taps,
        residues,
        mode_rates,
        skip_gain.reshape(TILES, LANES),
    )


def solution(mesh):
    split = Mesh(mesh.devices.reshape(4, 4, 4, 2, 2), ("y", "zh", "x", "core", "ch"))
    both = P(SEQ_AXES, "ch")
    placed = (
        both,
        both,
        both,
        P("ch", SEQ_AXES),
        both,
        P(None, None, "ch"),
        P(None, "ch"),
        P(None, "ch"),
        P("ch"),
    )
    return jax.shard_map(
        per_device, mesh=split, in_specs=placed, out_specs=both, check_vma=False
    )
```

```python
import jax
import jax.numpy as jnp
from jax import lax
from jax.experimental import pallas as pl
from jax.experimental.pallas import tpu as pltpu
from jax.sharding import Mesh
from jax.sharding import PartitionSpec as P

ROWS = 128
WIDE = 4096
LANES = 128
TILES = WIDE // LANES
GROUPS = TILES // 8
MODES = 16
TAPS = 7
SEQ_AXES = ("y", "zh", "x", "core")
MESH = pl.DeviceIdType.MESH
BLOCK = 48
QUARTER = 1024
RANKS = 12
UNITS = ((0, 0), (1, 0), (0, 1), (0, 3), (0, 2), (1, 1), (1, 3), (1, 2))


def lanes_of(tile):
    return slice(tile * LANES, (tile + 1) * LANES)


def spread_edge(edge, first_block, scratch):
    for tile in range(TILES):
        above = edge[:, lanes_of(tile)].astype(jnp.float32)
        scratch[tile * 8 : tile * 8 + 8, :] = jnp.where(first_block, 0.0, above)


def spread(source, edge, first_block, scratch):
    spread_edge(edge, first_block, scratch)

    @pl.loop(0, ROWS // 16)
    def _(pair):
        for tile in range(TILES):
            rows = pl.ds(pl.multiple_of(pair * 16, 16), 16)
            block = source[rows, lanes_of(tile)].astype(jnp.float32)
            base = pl.multiple_of((2 * pair + 1) * TILES * 8 + tile * 8, 8)
            scratch[pl.ds(base, 8), :] = block[:8]
            scratch[pl.ds(base + TILES * 8, 8), :] = block[8:]


def row_of(scratch, eight, group, row):
    start = (eight + (1 if row >= 0 else 0)) * TILES * 8 + group * 64 + row % 8
    return scratch[pl.ds(start, 8, stride=8), :]


def short(rows, taps, step):
    result = taps[0] * rows[step + 6]
    for offset in range(1, TAPS):
        result = result + taps[offset] * rows[step + 6 - offset]
    return result


def summed(terms):
    while len(terms) > 1:
        terms = [terms[i] + terms[i + 1] for i in range(0, len(terms), 2)]
    return terms[0]


def operator_kernel(
    tokens,
    pad_in,
    pad_out,
    query_in,
    key_in,
    short_taps,
    residues,
    mode_rates,
    skip_gain,
    out,
    last,
    chip_tokens,
    stage,
    weights,
    partial,
    theirs,
    low,
    total,
    arrived,
    edges,
    rows,
    tap_rows,
    rate_rows,
    weight_rows,
    queries,
    mixed,
    local,
    states,
    carried,
    group_states,
    group_before,
    deep_states,
    wide_states,
    own_sem,
    token_sems,
    stage_send,
    stage_recv,
    deep_send,
    deep_recv,
    ring_send,
    ring_recv,
    part_send,
    part_recv,
    swap_send,
    swap_recv,
    edge_send,
    edge_recv,
    near_send,
    near_recv,
    scan_send,
    scan_recv,
    back_send,
    back_recv,
):
    y, zh, x = lax.axis_index("y"), lax.axis_index("zh"), lax.axis_index("x")
    core, ch = lax.axis_index("core"), lax.axis_index("ch")
    place = {"x": x, "y": y, "zh": zh}
    pads = (pad_in, pad_out)
    started = []
    near = x * 2 + core
    block_at = (y * 4 + zh) * 8 + near
    first_block = block_at == 0

    def step(position, by):
        return lax.rem(position + by, 4)

    def copy(source, target, send, recv, device):
        return pltpu.make_async_remote_copy(
            src_ref=source,
            dst_ref=target,
            send_sem=send,
            recv_sem=recv,
            device_id=device,
            device_id_type=MESH,
        )

    def send(*arguments):
        made = copy(*arguments)
        made.start()
        started.append(made)

    def near_device(by):
        to = lax.rem(near + by, 8)
        return to, {"x": to // 2, "core": lax.rem(to, 2)}

    def block_device(by):
        to = lax.rem(block_at + by, 128)
        return {
            "y": to // 32,
            "zh": lax.rem(to // 8, 4),
            "x": lax.rem(to // 2, 4),
            "core": lax.rem(to, 2),
        }

    def send_edge(i, source):
        send(
            source.at[pl.ds(ROWS - 8, 8)],
            edges.at[i],
            edge_send.at[i],
            edge_recv.at[i],
            block_device(1),
        )

    def wait_edge(i):
        edge = edges.at[i]
        copy(edge, edge, edge_send.at[i], edge_recv.at[i], {"ch": ch}).wait_recv()

    barrier = pltpu.get_barrier_semaphore()
    greeted = [{"ch": 1 - ch}, block_device(1), block_device(127)]
    greeted += [near_device(by)[1] for by in range(1, 8)]
    greeted += [{axis: step(place[axis], by)} for axis in ("zh", "y") for by in (1, 2, 3)]
    for device in greeted:
        pl.semaphore_signal(barrier, inc=1, device_id=device, device_id_type=MESH)
    own_copy = pltpu.make_async_copy(tokens, chip_tokens.at[0], own_sem)
    own_copy.start()
    pl.semaphore_wait(barrier, len(greeted))

    for f in range(2):
        for by in (1, 3, 2):
            to = step(x, by)
            columns = pl.ds(pl.multiple_of(to * QUARTER, QUARTER), QUARTER)
            send(
                pads[f].at[:, columns],
                stage.at[f, x],
                stage_send.at[f, by - 1],
                stage_recv.at[f, by - 1],
                {"x": to},
            )
    send(tokens, chip_tokens.at[1], token_sems.at[0], token_sems.at[1], {"core": 1 - core})
    for i, source in enumerate((query_in, key_in)):
        send_edge(i, source)

    def settle(f):
        columns = pl.ds(pl.multiple_of(x * QUARTER, QUARTER), QUARTER)
        own = pltpu.make_async_copy(pads[f].at[:, columns], stage.at[f, x], own_sem)
        own.start()
        own.wait()
        for by in (1, 3, 2):
            came = stage.at[f, step(x, 4 - by)]
            copy(came, came, stage_send.at[f, by - 1], stage_recv.at[f, by - 1], {"x": x}).wait_recv()
        parts = [stage[f, i].astype(jnp.float32) for i in range(4)]
        weights[f, y, zh, x] = jnp.concatenate(parts, axis=0).astype(jnp.bfloat16)

    def ring(axis, item, send_sems, recv_sems):
        at = place[axis]
        plus, minus, far = step(at, 1), step(at, 3), step(at, 2)

        def out(ref, slot, to):
            send(ref, ref, send_sems(slot), recv_sems(slot), {axis: to})

        def landed(ref, slot):
            copy(ref, ref, send_sems(slot), recv_sems(slot), {axis: at}).wait_recv()

        def first():
            out(item(at), 0, plus)
            out(item(at), 1, minus)

        def forward():
            landed(item(minus), 0)
            out(item(minus, 0), 2, plus)
            landed(item(plus), 1)
            out(item(plus, 1), 3, minus)

        def finish():
            landed(item(far, 0), 2)
            landed(item(far, 1), 3)

        return first, forward, finish

    def half_columns(half):
        return slice(None) if half is None else slice(half * 512, half * 512 + 512)

    def half_blocks(half):
        return slice(None) if half is None else slice(half * 2, half * 2 + 2)

    def deep_ring(f):
        return ring(
            "zh",
            lambda i, half=None: weights.at[f, y, i, x, :, half_columns(half)],
            lambda slot: deep_send.at[f, slot],
            lambda slot: deep_recv.at[f, slot],
        )

    def unit_ring(unit, late):
        f, r = UNITS[unit]
        deep = step(zh, r)
        across = unit % 2 == 0

        def item(i, half=None):
            if late:
                if across:
                    return weights.at[f, i, deep, half_blocks(half)]
                return weights.at[f, half_blocks(half), deep, i]
            if across:
                return weights.at[f, y, deep, i, :, half_columns(half)]
            return weights.at[f, i, deep, x, :, half_columns(half)]

        base = 4 if late else 0
        return ring(
            "x" if across != late else "y",
            item,
            lambda slot: ring_send.at[unit, base + slot],
            lambda slot: ring_recv.at[unit, base + slot],
        )

    deep = [deep_ring(f) for f in range(2)]
    early = [unit_ring(unit, False) for unit in range(8)]
    late = [unit_ring(unit, True) for unit in range(8)]

    def unit_weights(f, r, quarter):
        return weights[f, :, step(zh, r), quarter].reshape(4 * BLOCK, QUARTER)

    def project(r):
        @pl.loop(0, 4)
        def _(quarter):
            columns = pl.ds(pl.multiple_of(quarter * QUARTER, QUARTER), QUARTER)
            part = lax.dot_general(
                chip_tokens[:, :, columns].reshape(2 * ROWS, QUARTER),
                unit_weights(0, r, quarter),
                (((1,), (1,)), ((), ())),
                preferred_element_type=jnp.float32,
            )

            @pl.when(quarter == 0)
            def _():
                partial[r] = part

            @pl.when(quarter > 0)
            def _():
                partial[r] += part

        send(partial.at[r], theirs.at[r], part_send.at[r], part_recv.at[r], {"ch": 1 - ch})

    def join(r):
        copy(partial.at[r], theirs.at[r], part_send.at[r], part_recv.at[r], {"ch": ch}).wait_recv()
        low[r] = (partial[r] + theirs[r]).astype(jnp.bfloat16)

    def expand(r, opening, closing):
        for quarter in range(4):
            part = jnp.dot(
                low[r], unit_weights(1, r, quarter), preferred_element_type=jnp.float32
            ).reshape(2, ROWS, QUARTER)
            if opening:
                total[:, quarter] = part
            else:
                total[:, quarter] += part
            if closing:
                send(
                    total.at[1, quarter],
                    arrived.at[quarter],
                    swap_send.at[quarter],
                    swap_recv.at[quarter],
                    {"core": 1 - core},
                )


    def tap_of(branch, offset, group):
        start = (branch * TILES + group * 8) * 8 + offset
        return tap_rows[pl.ds(start, 8, stride=8), :]

    def mode_of(ref, n, group):
        half, row = n // 8, n % 8
        return ref[half, pl.ds(group * 64 + row, 8, stride=8), :]

    def at_group(group):
        return slice(group * 8, group * 8 + 8)

    def filtered(branch, target, begin=0, end=ROWS // 8):
        for group in range(GROUPS):
            taps = [tap_of(branch, j, group) for j in range(TAPS)]

            @pl.loop(begin, end)
            def _(eight):
                window = [row_of(rows, eight, group, r) for r in range(-6, 8)]
                for i in range(8):
                    target(eight * 8 + i, group, short(window, taps, i))

    def prepare():
        for tile in range(TILES):
            for branch in range(3):
                base = (branch * TILES + tile) * 8
                tap_rows[base : base + TAPS, :] = short_taps[branch, :, lanes_of(tile)]
            for half in range(2):
                modes = slice(half * 8, half * 8 + 8)
                rate = mode_rates[modes, lanes_of(tile)]
                rate_rows[half, tile * 8 : tile * 8 + 8, :] = rate
                weight_rows[half, tile * 8 : tile * 8 + 8, :] = (
                    residues[modes, lanes_of(tile)] * jnp.sqrt(rate)
                )

        def keep_query(t, group, result):
            queries[t, at_group(group), :] = result

        def keep_key(t, group, result):
            mixed[t, at_group(group), :] = result

        wait_edge(0)
        spread(query_in, edges.at[0], first_block, rows)
        filtered(0, keep_query)
        wait_edge(1)
        spread(key_in, edges.at[1], first_block, rows)
        filtered(1, keep_key)

    def gather_value():
        for quarter in range(4):
            came = arrived.at[quarter]
            copy(came, came, swap_send.at[quarter], swap_recv.at[quarter], {"ch": ch}).wait_recv()

        def block_rows(pair):
            for tile in range(TILES):
                quarter, columns = tile // 8, lanes_of(tile % 8)
                where = pl.ds(pl.multiple_of(pair * 16, 16), 16)
                block = total[0, quarter, where, columns] + arrived[quarter, where, columns]
                block = block.astype(jnp.bfloat16)
                if isinstance(pair, int):
                    last[:, lanes_of(tile)] = block[8:]
                block = block.astype(jnp.float32)
                base = pl.multiple_of((2 * pair + 1) * TILES * 8 + tile * 8, 8)
                rows[pl.ds(base, 8), :] = block[:8]
                rows[pl.ds(base + TILES * 8, 8), :] = block[8:]

        block_rows(ROWS // 16 - 1)
        send(last, edges.at[2], edge_send.at[2], edge_recv.at[2], block_device(1))
        pl.loop(0, ROWS // 16 - 1)(block_rows)

    def mix():
        def keep(t, group, result):
            product = mixed[t, at_group(group), :] * result
            mixed[t, at_group(group), :] = product.astype(jnp.bfloat16).astype(jnp.float32)

        filtered(2, keep, 1, ROWS // 8)

    def mix_first():
        def keep(t, group, result):
            product = mixed[t, at_group(group), :] * result
            mixed[t, at_group(group), :] = product.astype(jnp.bfloat16).astype(jnp.float32)

        wait_edge(2)
        spread_edge(edges.at[2], first_block, rows)
        filtered(2, keep, 0, 1)

    def decays(group):
        return [jnp.exp(-mode_of(rate_rows, n, group)) for n in range(MODES)]

    zeros = (jnp.zeros((8, LANES), jnp.float32),) * MODES

    def run_modes(group, rates, begin, end, held):
        def advance(eight, held):
            for i in range(8):
                entry = mixed[eight * 8 + i, at_group(group), :]
                held = tuple(rates[n] * held[n] + entry for n in range(MODES))
            return held

        return lax.fori_loop(begin, end, advance, held)

    def store_states(group, held):
        for n in range(MODES):
            states[n // 8, pl.ds(group * 64 + n % 8, 8, stride=8), :] = held[n]

    def summarize(group):
        store_states(group, run_modes(group, decays(group), 1, ROWS // 8, zeros))

    def summarize_first(group):
        held = run_modes(group, decays(group), 0, 1, zeros)
        rest = [jnp.exp(-float(ROWS - 8) * mode_of(rate_rows, n, group)) for n in range(MODES)]
        store_states(
            group, [mode_of(states, n, group) + rest[n] * held[n] for n in range(MODES)]
        )

    def localize(group):
        rates = decays(group)
        weighting = [mode_of(weight_rows, n, group) for n in range(MODES)]

        def advance(eight, held):
            for i in range(8):
                entry = mixed[eight * 8 + i, at_group(group), :]
                held = tuple(rates[n] * held[n] + entry for n in range(MODES))
                local[eight * 8 + i, at_group(group), :] = summed(
                    [weighting[n] * held[n] for n in range(MODES)]
                )
            return held

        lax.fori_loop(0, ROWS // 8, advance, zeros)

    def finish_group(group):
        rates = decays(group)
        skip = skip_gain[at_group(group), :]
        first = tuple(
            mode_of(weight_rows, n, group) * mode_of(carried, n, group) for n in range(MODES)
        )

        def advance(eight, held):
            for i in range(8):
                held = tuple(rates[n] * held[n] for n in range(MODES))
                t = eight * 8 + i
                convolved = local[t, at_group(group), :] + summed(list(held))
                convolved = convolved.astype(jnp.bfloat16).astype(jnp.float32)
                result = queries[t, at_group(group), :] * (
                    convolved + skip * mixed[t, at_group(group), :]
                )
                out[pl.ds(eight * TILES * 8 + group * 64 + i, 8, stride=8), :] = result
            return held

        lax.fori_loop(0, ROWS // 8, advance, first)

    def near_part(at):
        return pl.ds(pl.multiple_of(at * 32, 32), 32)

    def exchange_states():
        for by in range(1, 8):
            to, device = near_device(by)
            send(
                states.at[:, near_part(to)],
                group_states.at[near],
                near_send.at[by - 1],
                near_recv.at[by - 1],
                device,
            )
        localize(0)
        localize(1)
        rate = rate_rows[:, near_part(near), :]
        one = jnp.exp(-float(ROWS) * rate)
        eight = jnp.exp(-8.0 * ROWS * rate)
        group_states[near] = states[:, near_part(near), :]
        for by in range(1, 8):
            came = group_states.at[lax.rem(near + 8 - by, 8)]
            copy(came, came, near_send.at[by - 1], near_recv.at[by - 1], {"ch": ch}).wait_recv()
        held = jnp.zeros(rate.shape, jnp.float32)
        for k in range(8):
            group_before[k] = held
            held = one * held + group_states[k]

        def across(buffer, axis, slot, own, decay, cover):
            at = place[axis]
            buffer[at] = own
            for by in (1, 3, 2):
                send(
                    buffer.at[at],
                    buffer.at[at],
                    scan_send.at[slot, by - 1],
                    scan_recv.at[slot, by - 1],
                    {axis: step(at, by)},
                )
            cover()
            for by in (1, 3, 2):
                came = buffer.at[step(at, 4 - by)]
                copy(
                    came, came, scan_send.at[slot, by - 1], scan_recv.at[slot, by - 1], {"ch": ch}
                ).wait_recv()
            running = jnp.zeros(own.shape, jnp.float32)
            before = running
            for k in range(4):
                before = jnp.where(at == k, running, before)
                running = decay * running + buffer[k]
            return before, running

        deep_before, deep_total = across(
            deep_states, "zh", 0, held, eight, lambda: (localize(2), localize(3))
        )
        wide_before, _ = across(
            wide_states, "y", 1, deep_total, jnp.exp(-32.0 * ROWS * rate), lambda: None
        )
        shift = jnp.exp(rate * (-8.0 * ROWS * zh.astype(jnp.float32)))
        entering = deep_before + shift * wide_before
        for k in range(8):
            group_before[k] += entering
            entering = one * entering
        for by in range(1, 8):
            to, device = near_device(by)
            send(
                group_before.at[to],
                carried.at[:, near_part(near)],
                back_send.at[by - 1],
                back_recv.at[by - 1],
                device,
            )
        carried[:, near_part(near), :] = group_before[near]
        for by in range(1, 8):
            came = carried.at[:, near_part(lax.rem(near + 8 - by, 8))]
            copy(came, came, back_send.at[by - 1], back_recv.at[by - 1], {"ch": ch}).wait_recv()

    FIRST, FORWARD, FINISH = range(3)

    def both(rings, pair, action):
        for unit in (2 * pair, 2 * pair + 1):
            rings[unit][action]()

    own_copy.wait()
    settle(0)
    early[0][FIRST]()
    deep[0][FIRST]()
    settle(1)
    early[1][FIRST]()
    deep[1][FIRST]()
    both(early, 0, FORWARD)
    deep[0][FORWARD]()
    both(early, 1, FIRST)
    both(early, 0, FINISH)
    both(late, 0, FIRST)
    both(early, 1, FORWARD)
    deep[0][FINISH]()
    deep[1][FORWARD]()
    both(early, 2, FIRST)
    deep[1][FINISH]()
    prepare()
    both(late, 0, FORWARD)
    both(early, 1, FINISH)
    both(late, 1, FIRST)
    both(early, 2, FORWARD)
    both(early, 3, FIRST)
    copy(tokens, chip_tokens.at[1], token_sems.at[0], token_sems.at[1], {"core": core}).wait_recv()
    both(late, 0, FINISH)
    project(0)
    both(late, 1, FORWARD)
    both(early, 2, FINISH)
    both(late, 2, FIRST)
    both(early, 3, FORWARD)
    both(late, 1, FINISH)
    project(1)
    project(3)
    join(0)
    expand(0, True, False)
    both(late, 2, FORWARD)
    both(early, 3, FINISH)
    both(late, 3, FIRST)
    both(late, 2, FINISH)
    project(2)
    join(1)
    expand(1, False, False)
    join(3)
    both(late, 3, FORWARD)
    join(2)
    late[6][FINISH]()
    expand(3, False, False)
    late[7][FINISH]()
    expand(2, False, True)
    gather_value()
    mix()
    for group in range(GROUPS):
        summarize(group)
    mix_first()
    for group in range(GROUPS):
        summarize_first(group)
    exchange_states()
    for group in range(GROUPS):
        finish_group(group)
    for made in started:
        made.wait_send()


def per_device(
    tokens, query_in, key_in, proj_in, proj_out, short_taps, residues, mode_rates, skip_gain
):
    f32, bf16 = jnp.float32, jnp.bfloat16
    dma = pltpu.SemaphoreType.DMA
    tiles = pl.pallas_call(
        operator_kernel,
        out_shape=jax.ShapeDtypeStruct((ROWS * TILES, LANES), f32),
        in_specs=[pl.BlockSpec(memory_space=pltpu.VMEM)] * 9,
        out_specs=pl.BlockSpec(memory_space=pltpu.VMEM),
        scratch_shapes=[
            pltpu.VMEM((8, WIDE), bf16),
            pltpu.VMEM((2, ROWS, WIDE), bf16),
            pltpu.VMEM((2, 4, RANKS, QUARTER), bf16),
            pltpu.VMEM((2, 4, 4, 4, BLOCK, QUARTER), bf16),
            pltpu.VMEM((4, 2 * ROWS, 4 * BLOCK), f32),
            pltpu.VMEM((4, 2 * ROWS, 4 * BLOCK), f32),
            pltpu.VMEM((4, 2 * ROWS, 4 * BLOCK), bf16),
            pltpu.VMEM((2, 4, ROWS, QUARTER), f32),
            pltpu.VMEM((4, ROWS, QUARTER), f32),
            pltpu.VMEM((3, 8, WIDE), bf16),
            pltpu.VMEM(((ROWS + 8) * TILES, LANES), f32),
            pltpu.VMEM((3 * TILES * 8, LANES), f32),
            pltpu.VMEM((2, TILES * 8, LANES), f32),
            pltpu.VMEM((2, TILES * 8, LANES), f32),
            pltpu.VMEM((ROWS, TILES, LANES), f32),
            pltpu.VMEM((ROWS, TILES, LANES), f32),
            pltpu.VMEM((ROWS, TILES, LANES), f32),
            pltpu.VMEM((2, TILES * 8, LANES), f32),
            pltpu.VMEM((2, TILES * 8, LANES), f32),
            pltpu.VMEM((8, 2, 32, LANES), f32),
            pltpu.VMEM((8, 2, 32, LANES), f32),
            pltpu.VMEM((4, 2, 32, LANES), f32),
            pltpu.VMEM((4, 2, 32, LANES), f32),
            dma,
            dma((2,)),
            dma((2, 3)),
            dma((2, 3)),
            dma((2, 4)),
            dma((2, 4)),
            dma((8, 8)),
            dma((8, 8)),
            dma((4,)),
            dma((4,)),
            dma((4,)),
            dma((4,)),
            dma((3,)),
            dma((3,)),
            dma((7,)),
            dma((7,)),
            dma((2, 3)),
            dma((2, 3)),
            dma((7,)),
            dma((7,)),
        ],
        compiler_params=pltpu.CompilerParams(
            collective_id=0, has_side_effects=True, vmem_limit_bytes=60 * 2**20
        ),
    )(
        tokens,
        proj_in.T,
        proj_out,
        query_in,
        key_in,
        short_taps,
        residues,
        mode_rates,
        skip_gain.reshape(TILES, LANES),
    )
    tiles = tiles.reshape(ROWS // 8, TILES, 8, LANES).transpose(0, 2, 1, 3)
    return tiles.reshape(ROWS, WIDE).astype(bf16)


def solution(mesh):
    split = Mesh(mesh.devices.reshape(4, 4, 4, 2, 2), ("y", "zh", "x", "core", "ch"))
    both = P(SEQ_AXES, "ch")
    placed = (
        both,
        both,
        both,
        P("ch", SEQ_AXES),
        both,
        P(None, None, "ch"),
        P(None, "ch"),
        P(None, "ch"),
        P("ch"),
    )
    return jax.shard_map(
        per_device, mesh=split, in_specs=placed, out_specs=both, check_vma=False
    )
```

```python
import jax
import jax.numpy as jnp
from jax import lax
from jax.experimental import pallas as pl
from jax.experimental.pallas import tpu as pltpu
from jax.sharding import Mesh
from jax.sharding import PartitionSpec as P

ROWS = 128
WIDE = 4096
LANES = 128
TILES = WIDE // LANES
GROUPS = TILES // 8
MODES = 16
TAPS = 7
SEQ_AXES = ("y", "zh", "x", "core")
MESH = pl.DeviceIdType.MESH
BLOCK = 48
QUARTER = 1024
RANKS = 12
UNITS = ((0, 0), (1, 0), (0, 1), (0, 3), (0, 2), (1, 1), (1, 3), (1, 2))


def lanes_of(tile):
    return slice(tile * LANES, (tile + 1) * LANES)


def spread_edge(edge, first_block, scratch):
    for tile in range(TILES):
        above = edge[:, lanes_of(tile)].astype(jnp.float32)
        scratch[tile * 8 : tile * 8 + 8, :] = jnp.where(first_block, 0.0, above)


def spread(source, edge, first_block, scratch):
    spread_edge(edge, first_block, scratch)

    @pl.loop(0, ROWS // 16)
    def _(pair):
        for tile in range(TILES):
            rows = pl.ds(pl.multiple_of(pair * 16, 16), 16)
            block = source[rows, lanes_of(tile)].astype(jnp.float32)
            base = pl.multiple_of((2 * pair + 1) * TILES * 8 + tile * 8, 8)
            scratch[pl.ds(base, 8), :] = block[:8]
            scratch[pl.ds(base + TILES * 8, 8), :] = block[8:]


def row_of(scratch, eight, group, row):
    start = (eight + (1 if row >= 0 else 0)) * TILES * 8 + group * 64 + row % 8
    return scratch[pl.ds(start, 8, stride=8), :]


def short(rows, taps, step):
    result = taps[0] * rows[step + 6]
    for offset in range(1, TAPS):
        result = result + taps[offset] * rows[step + 6 - offset]
    return result


def summed(terms):
    while len(terms) > 1:
        terms = [terms[i] + terms[i + 1] for i in range(0, len(terms), 2)]
    return terms[0]


def operator_kernel(
    tokens,
    pad_in,
    pad_out,
    query_in,
    key_in,
    short_taps,
    residues,
    mode_rates,
    skip_gain,
    out,
    last,
    chip_tokens,
    stage,
    weights,
    partial,
    theirs,
    low,
    total,
    arrived,
    edges,
    rows,
    tap_rows,
    rate_rows,
    weight_rows,
    queries,
    mixed,
    local,
    states,
    carried,
    group_states,
    group_before,
    deep_states,
    wide_states,
    own_sem,
    token_sems,
    stage_send,
    stage_recv,
    deep_send,
    deep_recv,
    ring_send,
    ring_recv,
    piece_send,
    part_send,
    part_recv,
    swap_send,
    swap_recv,
    edge_send,
    edge_recv,
    near_send,
    near_recv,
    scan_send,
    scan_recv,
    back_send,
    back_recv,
):
    y, zh, x = lax.axis_index("y"), lax.axis_index("zh"), lax.axis_index("x")
    core, ch = lax.axis_index("core"), lax.axis_index("ch")
    place = {"x": x, "y": y, "zh": zh}
    pads = (pad_in, pad_out)
    started = []
    near = x * 2 + core
    block_at = (y * 4 + zh) * 8 + near
    first_block = block_at == 0

    def step(position, by):
        return lax.rem(position + by, 4)

    def copy(source, target, send, recv, device):
        return pltpu.make_async_remote_copy(
            src_ref=source,
            dst_ref=target,
            send_sem=send,
            recv_sem=recv,
            device_id=device,
            device_id_type=MESH,
        )

    def send(*arguments):
        made = copy(*arguments)
        made.start()
        started.append(made)

    def near_device(by):
        to = lax.rem(near + by, 8)
        return to, {"x": to // 2, "core": lax.rem(to, 2)}

    def block_device(by):
        to = lax.rem(block_at + by, 128)
        return {
            "y": to // 32,
            "zh": lax.rem(to // 8, 4),
            "x": lax.rem(to // 2, 4),
            "core": lax.rem(to, 2),
        }

    def send_edge(i, source):
        send(
            source.at[pl.ds(ROWS - 8, 8)],
            edges.at[i],
            edge_send.at[i],
            edge_recv.at[i],
            block_device(1),
        )

    def wait_edge(i):
        edge = edges.at[i]
        copy(edge, edge, edge_send.at[i], edge_recv.at[i], {"ch": ch}).wait_recv()

    barrier = pltpu.get_barrier_semaphore()
    greeted = [{"ch": 1 - ch}, block_device(1), block_device(127)]
    greeted += [near_device(by)[1] for by in range(1, 8)]
    greeted += [{axis: step(place[axis], by)} for axis in ("zh", "y") for by in (1, 2, 3)]
    for device in greeted:
        pl.semaphore_signal(barrier, inc=1, device_id=device, device_id_type=MESH)
    own_copy = pltpu.make_async_copy(tokens, chip_tokens.at[0], own_sem)
    own_copy.start()
    pl.semaphore_wait(barrier, len(greeted))

    for f in range(2):
        for by in (1, 3, 2):
            to = step(x, by)
            columns = pl.ds(pl.multiple_of(to * QUARTER, QUARTER), QUARTER)
            send(
                pads[f].at[:, columns],
                stage.at[f, x],
                stage_send.at[f, by - 1],
                stage_recv.at[f, by - 1],
                {"x": to},
            )
    send(tokens, chip_tokens.at[1], token_sems.at[0], token_sems.at[1], {"core": 1 - core})
    for i, source in enumerate((query_in, key_in)):
        send_edge(i, source)

    def settle(f):
        columns = pl.ds(pl.multiple_of(x * QUARTER, QUARTER), QUARTER)
        own = pltpu.make_async_copy(pads[f].at[:, columns], stage.at[f, x], own_sem)
        own.start()
        own.wait()
        for by in (1, 3, 2):
            came = stage.at[f, step(x, 4 - by)]
            copy(came, came, stage_send.at[f, by - 1], stage_recv.at[f, by - 1], {"x": x}).wait_recv()
        parts = [stage[f, i].astype(jnp.float32) for i in range(4)]
        weights[f, y, zh, x] = jnp.concatenate(parts, axis=0).astype(jnp.bfloat16)

    def ring(axis, item, send_sems, recv_sems, split=False):
        at = place[axis]
        plus, minus, far = step(at, 1), step(at, 3), step(at, 2)

        def out(ref, slot, to):
            send(ref, ref, send_sems(slot), recv_sems(slot), {axis: to})

        def landed(ref, slot):
            copy(ref, ref, send_sems(slot), recv_sems(slot), {axis: at}).wait_recv()

        def first():
            if split:
                out(item(at, 0), 0, plus)
                out(item(at, 1), 1, minus)
                out(item(at, 1), 4, plus)
                out(item(at, 0), 5, minus)
            else:
                out(item(at), 0, plus)
                out(item(at), 1, minus)

        def forward():
            landed(item(minus, 0 if split else None), 0)
            out(item(minus, 0), 2, plus)
            landed(item(plus, 1 if split else None), 1)
            out(item(plus, 1), 3, minus)

        def finish():
            if split:
                landed(item(minus, 1), 4)
                landed(item(plus, 0), 5)
            landed(item(far, 0), 2)
            landed(item(far, 1), 3)

        return first, forward, finish

    def half_columns(half):
        return slice(None) if half is None else slice(half * 512, half * 512 + 512)

    def half_blocks(half):
        return slice(None) if half is None else slice(half * 2, half * 2 + 2)

    def deep_ring(f):
        return ring(
            "zh",
            lambda i, half=None: weights.at[f, y, i, x, :, half_columns(half)],
            lambda slot: deep_send.at[f, slot],
            lambda slot: deep_recv.at[f, slot],
        )

    def unit_ring(unit, late):
        f, r = UNITS[unit]
        deep = step(zh, r)
        across = unit % 2 == 0

        def item(i, half=None):
            if late:
                if across:
                    return weights.at[f, i, deep, half_blocks(half)]
                return weights.at[f, half_blocks(half), deep, i]
            if across:
                return weights.at[f, y, deep, i, :, half_columns(half)]
            return weights.at[f, i, deep, x, :, half_columns(half)]

        base = 4 if late else 0
        return ring(
            "x" if across != late else "y",
            item,
            lambda slot: ring_send.at[unit, base + slot],
            lambda slot: ring_recv.at[unit, base + slot],
            late and unit >= 2,
        )

    def open_late(unit, by):
        deep = zh
        if unit == 0:
            axis, piece = "y", weights.at[0, y, deep, step(x, by)]
        else:
            axis, piece = "x", weights.at[1, step(y, by), deep, x]
        for slot, to in ((0, 1), (1, 3)):
            send(
                piece,
                piece,
                piece_send.at[unit, by, slot],
                ring_recv.at[unit, 4 + slot],
                {axis: step(place[axis], to)},
            )

    deep = [deep_ring(f) for f in range(2)]
    early = [unit_ring(unit, False) for unit in range(8)]
    late = [unit_ring(unit, True) for unit in range(8)]

    def unit_weights(f, r, quarter):
        return weights[f, :, step(zh, r), quarter].reshape(4 * BLOCK, QUARTER)

    def project(r):
        @pl.loop(0, 4)
        def _(quarter):
            columns = pl.ds(pl.multiple_of(quarter * QUARTER, QUARTER), QUARTER)
            part = lax.dot_general(
                chip_tokens[:, :, columns].reshape(2 * ROWS, QUARTER),
                unit_weights(0, r, quarter),
                (((1,), (1,)), ((), ())),
                preferred_element_type=jnp.float32,
            )

            @pl.when(quarter == 0)
            def _():
                partial[r] = part

            @pl.when(quarter > 0)
            def _():
                partial[r] += part

        send(partial.at[r], theirs.at[r], part_send.at[r], part_recv.at[r], {"ch": 1 - ch})

    def join(r):
        copy(partial.at[r], theirs.at[r], part_send.at[r], part_recv.at[r], {"ch": ch}).wait_recv()
        low[r] = (partial[r] + theirs[r]).astype(jnp.bfloat16)

    def expand(r, opening, closing):
        for quarter in range(4):
            part = jnp.dot(
                low[r], unit_weights(1, r, quarter), preferred_element_type=jnp.float32
            ).reshape(2, ROWS, QUARTER)
            if opening:
                total[:, quarter] = part
            else:
                total[:, quarter] += part
            if closing:
                send(
                    total.at[1, quarter],
                    arrived.at[quarter],
                    swap_send.at[quarter],
                    swap_recv.at[quarter],
                    {"core": 1 - core},
                )


    def tap_of(branch, offset, group):
        start = (branch * TILES + group * 8) * 8 + offset
        return tap_rows[pl.ds(start, 8, stride=8), :]

    def mode_of(ref, n, group):
        half, row = n // 8, n % 8
        return ref[half, pl.ds(group * 64 + row, 8, stride=8), :]

    def state_of(ref, n, group):
        return ref[group // 2, n // 8, pl.ds(group % 2 * 8 + n % 8, 8, stride=16), :]

    def at_group(group):
        return slice(group * 8, group * 8 + 8)

    def filtered(branch, target, begin=0, end=ROWS // 8):
        for group in range(GROUPS):
            taps = [tap_of(branch, j, group) for j in range(TAPS)]

            @pl.loop(begin, end)
            def _(eight):
                window = [row_of(rows, eight, group, r) for r in range(-6, 8)]
                for i in range(8):
                    target(eight * 8 + i, group, short(window, taps, i))

    def prepare():
        for tile in range(TILES):
            for branch in range(3):
                base = (branch * TILES + tile) * 8
                tap_rows[base : base + TAPS, :] = short_taps[branch, :, lanes_of(tile)]
            for half in range(2):
                modes = slice(half * 8, half * 8 + 8)
                rate = mode_rates[modes, lanes_of(tile)]
                rate_rows[half, tile * 8 : tile * 8 + 8, :] = rate
                weight_rows[half, tile * 8 : tile * 8 + 8, :] = (
                    residues[modes, lanes_of(tile)] * jnp.sqrt(rate)
                )

        def keep_query(t, group, result):
            queries[t, at_group(group), :] = result

        def keep_key(t, group, result):
            mixed[t, at_group(group), :] = result

        wait_edge(0)
        spread(query_in, edges.at[0], first_block, rows)
        filtered(0, keep_query)
        wait_edge(1)
        spread(key_in, edges.at[1], first_block, rows)
        filtered(1, keep_key)

    def gather_value():
        for quarter in range(4):
            came = arrived.at[quarter]
            copy(came, came, swap_send.at[quarter], swap_recv.at[quarter], {"ch": ch}).wait_recv()

        def block_rows(pair):
            for tile in range(TILES):
                quarter, columns = tile // 8, lanes_of(tile % 8)
                where = pl.ds(pl.multiple_of(pair * 16, 16), 16)
                block = total[0, quarter, where, columns] + arrived[quarter, where, columns]
                block = block.astype(jnp.bfloat16)
                if isinstance(pair, int):
                    last[:, lanes_of(tile)] = block[8:]
                block = block.astype(jnp.float32)
                base = pl.multiple_of((2 * pair + 1) * TILES * 8 + tile * 8, 8)
                rows[pl.ds(base, 8), :] = block[:8]
                rows[pl.ds(base + TILES * 8, 8), :] = block[8:]

        block_rows(ROWS // 16 - 1)
        send(last, edges.at[2], edge_send.at[2], edge_recv.at[2], block_device(1))
        pl.loop(0, ROWS // 16 - 1)(block_rows)

    def mix():
        def keep(t, group, result):
            product = mixed[t, at_group(group), :] * result
            mixed[t, at_group(group), :] = product.astype(jnp.bfloat16).astype(jnp.float32)

        filtered(2, keep, 1, ROWS // 8)

    def mix_first():
        def keep(t, group, result):
            product = mixed[t, at_group(group), :] * result
            mixed[t, at_group(group), :] = product.astype(jnp.bfloat16).astype(jnp.float32)

        wait_edge(2)
        spread_edge(edges.at[2], first_block, rows)
        filtered(2, keep, 0, 1)

    def decays(group):
        return [jnp.exp(-mode_of(rate_rows, n, group)) for n in range(MODES)]

    zeros = (jnp.zeros((8, LANES), jnp.float32),) * MODES

    def run_modes(group, rates, begin, end, held):
        def advance(eight, held):
            for i in range(8):
                entry = mixed[eight * 8 + i, at_group(group), :]
                held = tuple(rates[n] * held[n] + entry for n in range(MODES))
            return held

        return lax.fori_loop(begin, end, advance, held)

    def store_states(group, held):
        for n in range(MODES):
            states[group // 2, n // 8, pl.ds(group % 2 * 8 + n % 8, 8, stride=16), :] = held[n]

    def summarize(group):
        store_states(group, run_modes(group, decays(group), 1, ROWS // 8, zeros))

    def summarize_first(group):
        held = run_modes(group, decays(group), 0, 1, zeros)
        rest = [jnp.exp(-float(ROWS - 8) * mode_of(rate_rows, n, group)) for n in range(MODES)]
        store_states(
            group, [state_of(states, n, group) + rest[n] * held[n] for n in range(MODES)]
        )

    def localize(group):
        rates = decays(group)
        weighting = [mode_of(weight_rows, n, group) for n in range(MODES)]

        def advance(eight, held):
            for i in range(8):
                entry = mixed[eight * 8 + i, at_group(group), :]
                held = tuple(rates[n] * held[n] + entry for n in range(MODES))
                local[eight * 8 + i, at_group(group), :] = summed(
                    [weighting[n] * held[n] for n in range(MODES)]
                )
            return held

        lax.fori_loop(0, ROWS // 8, advance, zeros)

    def finish_group(group):
        rates = decays(group)
        skip = skip_gain[at_group(group), :]
        first = tuple(
            mode_of(weight_rows, n, group) * state_of(carried, n, group) for n in range(MODES)
        )

        def advance(eight, held):
            for i in range(8):
                held = tuple(rates[n] * held[n] for n in range(MODES))
                t = eight * 8 + i
                convolved = local[t, at_group(group), :] + summed(list(held))
                convolved = convolved.astype(jnp.bfloat16).astype(jnp.float32)
                result = queries[t, at_group(group), :] * (
                    convolved + skip * mixed[t, at_group(group), :]
                )
                out[pl.ds(eight * TILES * 8 + group * 64 + i, 8, stride=8), :] = result
            return held

        lax.fori_loop(0, ROWS // 8, advance, first)

    def near_part(at):
        return pl.ds(pl.multiple_of(at * 16, 16), 16)

    def near_rates(half):
        starts = [pl.multiple_of((2 * half + i) * 64 + near * 8, 8) for i in range(2)]
        return jnp.concatenate([rate_rows[:, pl.ds(start, 8), :] for start in starts], axis=1)

    def wait_all(buffer, sends, recvs, offsets, index):
        for by in offsets:
            came = buffer(index(by))
            copy(came, came, sends.at[by - 1], recvs.at[by - 1], {"ch": ch}).wait_recv()

    def send_near(half):
        for by in range(1, 8):
            to, device = near_device(by)
            send(
                states.at[half, :, near_part(to)],
                group_states.at[half, near],
                near_send.at[half, by - 1],
                near_recv.at[half, by - 1],
                device,
            )

    def send_across(buffer, slot, axis, half):
        own = buffer.at[half, place[axis]]
        for by in (2, 1, 3):
            send(
                own,
                own,
                scan_send.at[slot, half, by - 1],
                scan_recv.at[slot, half, by - 1],
                {axis: step(place[axis], by)},
            )

    def scan_across(buffer, slot, axis, half, decay):
        at = place[axis]
        wait_all(
            lambda i: buffer.at[half, i],
            scan_send.at[slot, half],
            scan_recv.at[slot, half],
            (1, 3, 2),
            lambda by: step(at, 4 - by),
        )
        running = jnp.zeros(decay.shape, jnp.float32)
        before = running
        for k in range(4):
            before = jnp.where(at == k, running, before)
            running = decay * running + buffer[half, k]
        return before, running

    def before_near(by):
        return lax.rem(near + 8 - by, 8)

    def scan_near(half):
        one = jnp.exp(-float(ROWS) * near_rates(half))
        group_states[half, near] = states[half, :, near_part(near), :]
        wait_all(
            lambda i: group_states.at[half, i],
            near_send.at[half],
            near_recv.at[half],
            range(1, 8),
            before_near,
        )
        held = jnp.zeros(one.shape, jnp.float32)
        for k in range(8):
            group_before[half, k] = held
            held = one * held + group_states[half, k]
        deep_states[half, zh] = held
        send_across(deep_states, 0, "zh", half)

    def scan_deep(half):
        decay = jnp.exp(-8.0 * ROWS * near_rates(half))
        before, running = scan_across(deep_states, 0, "zh", half, decay)
        wide_states[half, y] = running
        send_across(wide_states, 1, "y", half)
        return before

    def scan_wide(half, deep_before):
        rate = near_rates(half)
        one = jnp.exp(-float(ROWS) * rate)
        wide_before, _ = scan_across(wide_states, 1, "y", half, jnp.exp(-32.0 * ROWS * rate))
        shift = jnp.exp(rate * (-8.0 * ROWS * zh.astype(jnp.float32)))
        entering = deep_before + shift * wide_before
        for k in range(8):
            group_before[half, k] += entering
            entering = one * entering
        for by in range(1, 8):
            to, device = near_device(by)
            send(
                group_before.at[half, to],
                carried.at[half, :, near_part(near)],
                back_send.at[half, by - 1],
                back_recv.at[half, by - 1],
                device,
            )
        carried[half, :, near_part(near), :] = group_before[half, near]

    def wait_back(half):
        wait_all(
            lambda i: carried.at[half, :, near_part(i)],
            back_send.at[half],
            back_recv.at[half],
            range(1, 8),
            before_near,
        )

    FIRST, FORWARD, FINISH = range(3)

    def both(rings, pair, action):
        for unit in (2 * pair, 2 * pair + 1):
            rings[unit][action]()

    own_copy.wait()
    settle(0)
    early[0][FIRST]()
    deep[0][FIRST]()
    open_late(0, 0)
    settle(1)
    early[1][FIRST]()
    deep[1][FIRST]()
    open_late(1, 0)
    for unit in (0, 1):
        early[unit][FORWARD]()
        open_late(unit, 1)
        open_late(unit, 3)
    deep[0][FORWARD]()
    both(early, 1, FIRST)
    for unit in (0, 1):
        early[unit][FINISH]()
        open_late(unit, 2)
    both(early, 1, FORWARD)
    deep[0][FINISH]()
    deep[1][FORWARD]()
    both(early, 2, FIRST)
    deep[1][FINISH]()
    prepare()
    both(late, 0, FORWARD)
    both(early, 1, FINISH)
    both(late, 1, FIRST)
    both(early, 2, FORWARD)
    both(early, 3, FIRST)
    copy(tokens, chip_tokens.at[1], token_sems.at[0], token_sems.at[1], {"core": core}).wait_recv()
    both(late, 0, FINISH)
    project(0)
    both(late, 1, FORWARD)
    both(early, 2, FINISH)
    both(late, 2, FIRST)
    both(early, 3, FORWARD)
    both(late, 1, FINISH)
    project(1)
    project(3)
    join(0)
    expand(0, True, False)
    both(late, 2, FORWARD)
    both(early, 3, FINISH)
    both(late, 3, FIRST)
    both(late, 2, FINISH)
    project(2)
    join(1)
    expand(1, False, False)
    join(3)
    both(late, 3, FORWARD)
    join(2)
    late[6][FINISH]()
    expand(3, False, False)
    late[7][FINISH]()
    expand(2, False, True)
    gather_value()
    mix()
    summarize(0)
    summarize(1)
    mix_first()
    summarize_first(0)
    summarize_first(1)
    send_near(0)
    summarize(2)
    summarize(3)
    summarize_first(2)
    summarize_first(3)
    send_near(1)
    localize(0)
    localize(1)
    scan_near(0)
    localize(2)
    scan_near(1)
    localize(3)
    deep_before = [scan_deep(0)]
    deep_before.append(scan_deep(1))
    scan_wide(0, deep_before[0])
    scan_wide(1, deep_before[1])
    wait_back(0)
    finish_group(0)
    finish_group(1)
    wait_back(1)
    finish_group(2)
    finish_group(3)
    for made in started:
        made.wait_send()


def per_device(
    tokens, query_in, key_in, proj_in, proj_out, short_taps, residues, mode_rates, skip_gain
):
    f32, bf16 = jnp.float32, jnp.bfloat16
    dma = pltpu.SemaphoreType.DMA
    tiles = pl.pallas_call(
        operator_kernel,
        out_shape=jax.ShapeDtypeStruct((ROWS * TILES, LANES), f32),
        in_specs=[pl.BlockSpec(memory_space=pltpu.VMEM)] * 9,
        out_specs=pl.BlockSpec(memory_space=pltpu.VMEM),
        scratch_shapes=[
            pltpu.VMEM((8, WIDE), bf16),
            pltpu.VMEM((2, ROWS, WIDE), bf16),
            pltpu.VMEM((2, 4, RANKS, QUARTER), bf16),
            pltpu.VMEM((2, 4, 4, 4, BLOCK, QUARTER), bf16),
            pltpu.VMEM((4, 2 * ROWS, 4 * BLOCK), f32),
            pltpu.VMEM((4, 2 * ROWS, 4 * BLOCK), f32),
            pltpu.VMEM((4, 2 * ROWS, 4 * BLOCK), bf16),
            pltpu.VMEM((2, 4, ROWS, QUARTER), f32),
            pltpu.VMEM((4, ROWS, QUARTER), f32),
            pltpu.VMEM((3, 8, WIDE), bf16),
            pltpu.VMEM(((ROWS + 8) * TILES, LANES), f32),
            pltpu.VMEM((3 * TILES * 8, LANES), f32),
            pltpu.VMEM((2, TILES * 8, LANES), f32),
            pltpu.VMEM((2, TILES * 8, LANES), f32),
            pltpu.VMEM((ROWS, TILES, LANES), f32),
            pltpu.VMEM((ROWS, TILES, LANES), f32),
            pltpu.VMEM((ROWS, TILES, LANES), f32),
            pltpu.VMEM((2, 2, TILES * 4, LANES), f32),
            pltpu.VMEM((2, 2, TILES * 4, LANES), f32),
            pltpu.VMEM((2, 8, 2, 16, LANES), f32),
            pltpu.VMEM((2, 8, 2, 16, LANES), f32),
            pltpu.VMEM((2, 4, 2, 16, LANES), f32),
            pltpu.VMEM((2, 4, 2, 16, LANES), f32),
            dma,
            dma((2,)),
            dma((2, 3)),
            dma((2, 3)),
            dma((2, 4)),
            dma((2, 4)),
            dma((8, 10)),
            dma((8, 10)),
            dma((2, 4, 2)),
            dma((4,)),
            dma((4,)),
            dma((4,)),
            dma((4,)),
            dma((3,)),
            dma((3,)),
            dma((2, 7)),
            dma((2, 7)),
            dma((2, 2, 3)),
            dma((2, 2, 3)),
            dma((2, 7)),
            dma((2, 7)),
        ],
        compiler_params=pltpu.CompilerParams(
            collective_id=0, has_side_effects=True, vmem_limit_bytes=60 * 2**20
        ),
    )(
        tokens,
        proj_in.T,
        proj_out,
        query_in,
        key_in,
        short_taps,
        residues,
        mode_rates,
        skip_gain.reshape(TILES, LANES),
    )
    tiles = tiles.reshape(ROWS // 8, TILES, 8, LANES).transpose(0, 2, 1, 3)
    return tiles.reshape(ROWS, WIDE).astype(bf16)


def solution(mesh):
    split = Mesh(mesh.devices.reshape(4, 4, 4, 2, 2), ("y", "zh", "x", "core", "ch"))
    both = P(SEQ_AXES, "ch")
    placed = (
        both,
        both,
        both,
        P("ch", SEQ_AXES),
        both,
        P(None, None, "ch"),
        P(None, "ch"),
        P(None, "ch"),
        P("ch"),
    )
    return jax.shard_map(
        per_device, mesh=split, in_specs=placed, out_specs=both, check_vma=False
    )
```

```python
import jax
import jax.numpy as jnp
from jax import lax
from jax.experimental import pallas as pl
from jax.experimental.pallas import tpu as pltpu
from jax.sharding import Mesh
from jax.sharding import PartitionSpec as P

ROWS = 128
WIDE = 4096
LANES = 128
TILES = WIDE // LANES
GROUPS = TILES // 8
MODES = 16
TAPS = 7
SEQ_AXES = ("y", "zh", "x", "core")
MESH = pl.DeviceIdType.MESH
BLOCK = 48
QUARTER = 1024
RANKS = 12
UNITS = ((0, 0), (1, 0), (0, 1), (0, 3), (0, 2), (1, 1), (1, 3), (1, 2))


def lanes_of(tile):
    return slice(tile * LANES, (tile + 1) * LANES)


def spread_edge(edge, first_block, scratch):
    for tile in range(TILES):
        above = edge[:, lanes_of(tile)].astype(jnp.float32)
        scratch[tile * 8 : tile * 8 + 8, :] = jnp.where(first_block, 0.0, above)


def spread(source, edge, first_block, scratch):
    spread_edge(edge, first_block, scratch)

    @pl.loop(0, ROWS // 16)
    def _(pair):
        for tile in range(TILES):
            rows = pl.ds(pl.multiple_of(pair * 16, 16), 16)
            block = source[rows, lanes_of(tile)].astype(jnp.float32)
            base = pl.multiple_of((2 * pair + 1) * TILES * 8 + tile * 8, 8)
            scratch[pl.ds(base, 8), :] = block[:8]
            scratch[pl.ds(base + TILES * 8, 8), :] = block[8:]


def row_of(scratch, eight, group, row):
    start = (eight + (1 if row >= 0 else 0)) * TILES * 8 + group * 64 + row % 8
    return scratch[pl.ds(start, 8, stride=8), :]


def short(rows, taps, step):
    result = taps[0] * rows[step + 6]
    for offset in range(1, TAPS):
        result = result + taps[offset] * rows[step + 6 - offset]
    return result


def summed(terms):
    while len(terms) > 1:
        terms = [terms[i] + terms[i + 1] for i in range(0, len(terms), 2)]
    return terms[0]


def operator_kernel(
    tokens,
    pad_in,
    pad_out,
    query_in,
    key_in,
    short_taps,
    residues,
    mode_rates,
    skip_gain,
    out,
    last,
    chip_tokens,
    stage,
    weights,
    partial,
    theirs,
    low,
    total,
    arrived,
    edges,
    rows,
    tap_rows,
    rate_rows,
    weight_rows,
    queries,
    mixed,
    local,
    states,
    carried,
    group_states,
    group_before,
    deep_states,
    wide_states,
    own_sem,
    token_sems,
    stage_send,
    stage_recv,
    deep_send,
    deep_recv,
    ring_send,
    ring_recv,
    piece_send,
    part_send,
    part_recv,
    swap_send,
    swap_recv,
    edge_send,
    edge_recv,
    near_send,
    near_recv,
    scan_send,
    scan_recv,
    back_send,
    back_recv,
):
    y, zh, x = lax.axis_index("y"), lax.axis_index("zh"), lax.axis_index("x")
    core, ch = lax.axis_index("core"), lax.axis_index("ch")
    place = {"x": x, "y": y, "zh": zh}
    pads = (pad_in, pad_out)
    started = []
    near = x * 2 + core
    block_at = (y * 4 + zh) * 8 + near
    first_block = block_at == 0

    def step(position, by):
        return lax.rem(position + by, 4)

    def copy(source, target, send, recv, device):
        return pltpu.make_async_remote_copy(
            src_ref=source,
            dst_ref=target,
            send_sem=send,
            recv_sem=recv,
            device_id=device,
            device_id_type=MESH,
        )

    def send(*arguments):
        made = copy(*arguments)
        made.start()
        started.append(made)

    def near_device(by):
        to = lax.rem(near + by, 8)
        return to, {"x": to // 2, "core": lax.rem(to, 2)}

    def block_device(by):
        to = lax.rem(block_at + by, 128)
        return {
            "y": to // 32,
            "zh": lax.rem(to // 8, 4),
            "x": lax.rem(to // 2, 4),
            "core": lax.rem(to, 2),
        }

    def send_edge(i, source):
        send(
            source.at[pl.ds(ROWS - 8, 8)],
            edges.at[i],
            edge_send.at[i],
            edge_recv.at[i],
            block_device(1),
        )

    def wait_edge(i):
        edge = edges.at[i]
        copy(edge, edge, edge_send.at[i], edge_recv.at[i], {"ch": ch}).wait_recv()

    barrier = pltpu.get_barrier_semaphore()
    greeted = [{"ch": 1 - ch}, block_device(1), block_device(127)]
    greeted += [near_device(by)[1] for by in range(1, 8)]
    greeted += [{axis: step(place[axis], by)} for axis in ("zh", "y") for by in (1, 2, 3)]
    for device in greeted:
        pl.semaphore_signal(barrier, inc=1, device_id=device, device_id_type=MESH)
    own_copy = pltpu.make_async_copy(tokens, chip_tokens.at[0], own_sem)
    own_copy.start()
    pl.semaphore_wait(barrier, len(greeted))

    for f in range(2):
        for by in (1, 3, 2):
            to = step(x, by)
            columns = pl.ds(pl.multiple_of(to * QUARTER, QUARTER), QUARTER)
            send(
                pads[f].at[:, columns],
                stage.at[f, x],
                stage_send.at[f, by - 1],
                stage_recv.at[f, by - 1],
                {"x": to},
            )
    send(tokens, chip_tokens.at[1], token_sems.at[0], token_sems.at[1], {"core": 1 - core})
    for i, source in enumerate((query_in, key_in)):
        send_edge(i, source)

    def settle(f):
        columns = pl.ds(pl.multiple_of(x * QUARTER, QUARTER), QUARTER)
        own = pltpu.make_async_copy(pads[f].at[:, columns], stage.at[f, x], own_sem)
        own.start()
        own.wait()
        for by in (1, 3, 2):
            came = stage.at[f, step(x, 4 - by)]
            copy(came, came, stage_send.at[f, by - 1], stage_recv.at[f, by - 1], {"x": x}).wait_recv()
        parts = [stage[f, i].astype(jnp.float32) for i in range(4)]
        weights[f, y, zh, x] = jnp.concatenate(parts, axis=0).astype(jnp.bfloat16)

    def ring(axis, item, send_sems, recv_sems, split=False):
        at = place[axis]
        plus, minus, far = step(at, 1), step(at, 3), step(at, 2)

        def out(ref, slot, to):
            send(ref, ref, send_sems(slot), recv_sems(slot), {axis: to})

        def landed(ref, slot):
            copy(ref, ref, send_sems(slot), recv_sems(slot), {axis: at}).wait_recv()

        def first():
            if split:
                out(item(at, 0), 0, plus)
                out(item(at, 1), 1, minus)
                out(item(at, 1), 4, plus)
                out(item(at, 0), 5, minus)
            else:
                out(item(at), 0, plus)
                out(item(at), 1, minus)

        def forward():
            landed(item(minus, 0 if split else None), 0)
            out(item(minus, 0), 2, plus)
            landed(item(plus, 1 if split else None), 1)
            out(item(plus, 1), 3, minus)

        def finish():
            if split:
                landed(item(minus, 1), 4)
                landed(item(plus, 0), 5)
            landed(item(far, 0), 2)
            landed(item(far, 1), 3)

        return first, forward, finish

    def half_columns(half):
        return slice(None) if half is None else slice(half * 512, half * 512 + 512)

    def half_blocks(half):
        return slice(None) if half is None else slice(half * 2, half * 2 + 2)

    def deep_ring(f):
        return ring(
            "zh",
            lambda i, half=None: weights.at[f, y, i, x, :, half_columns(half)],
            lambda slot: deep_send.at[f, slot],
            lambda slot: deep_recv.at[f, slot],
        )

    def unit_ring(unit, late):
        f, r = UNITS[unit]
        deep = step(zh, r)
        across = unit % 2 == 0

        def item(i, half=None):
            if late:
                if across:
                    return weights.at[f, i, deep, half_blocks(half)]
                return weights.at[f, half_blocks(half), deep, i]
            if across:
                return weights.at[f, y, deep, i, :, half_columns(half)]
            return weights.at[f, i, deep, x, :, half_columns(half)]

        base = 4 if late else 0
        return ring(
            "x" if across != late else "y",
            item,
            lambda slot: ring_send.at[unit, base + slot],
            lambda slot: ring_recv.at[unit, base + slot],
            late and unit >= 2,
        )

    def open_late(unit, by):
        deep = zh
        if unit == 0:
            axis, piece = "y", weights.at[0, y, deep, step(x, by)]
        else:
            axis, piece = "x", weights.at[1, step(y, by), deep, x]
        for slot, to in ((0, 1), (1, 3)):
            send(
                piece,
                piece,
                piece_send.at[unit, by, slot],
                ring_recv.at[unit, 4 + slot],
                {axis: step(place[axis], to)},
            )

    deep = [deep_ring(f) for f in range(2)]
    early = [unit_ring(unit, False) for unit in range(8)]
    late = [unit_ring(unit, True) for unit in range(8)]

    def unit_weights(f, r, quarter):
        return weights[f, :, step(zh, r), quarter].reshape(4 * BLOCK, QUARTER)

    def project(r):
        @pl.loop(0, 4)
        def _(quarter):
            columns = pl.ds(pl.multiple_of(quarter * QUARTER, QUARTER), QUARTER)
            part = lax.dot_general(
                chip_tokens[:, :, columns].reshape(2 * ROWS, QUARTER),
                unit_weights(0, r, quarter),
                (((1,), (1,)), ((), ())),
                preferred_element_type=jnp.float32,
            )

            @pl.when(quarter == 0)
            def _():
                partial[r] = part

            @pl.when(quarter > 0)
            def _():
                partial[r] += part

        send(partial.at[r], theirs.at[r], part_send.at[r], part_recv.at[r], {"ch": 1 - ch})

    def join(r):
        copy(partial.at[r], theirs.at[r], part_send.at[r], part_recv.at[r], {"ch": ch}).wait_recv()
        low[r] = (partial[r] + theirs[r]).astype(jnp.bfloat16)

    def expand(r, opening, closing):
        for quarter in range(4):
            part = jnp.dot(
                low[r], unit_weights(1, r, quarter), preferred_element_type=jnp.float32
            ).reshape(2, ROWS, QUARTER)
            if opening:
                total[:, quarter] = part
            else:
                total[:, quarter] += part
            if closing:
                send(
                    total.at[1, quarter],
                    arrived.at[quarter],
                    swap_send.at[quarter],
                    swap_recv.at[quarter],
                    {"core": 1 - core},
                )


    def tap_of(branch, offset, group):
        start = (branch * TILES + group * 8) * 8 + offset
        return tap_rows[pl.ds(start, 8, stride=8), :]

    def mode_of(ref, n, group):
        half, row = n // 8, n % 8
        return ref[half, pl.ds(group * 64 + row, 8, stride=8), :]

    def state_of(ref, n, group):
        return ref[group // 2, n // 8, pl.ds(group % 2 * 8 + n % 8, 8, stride=16), :]

    def at_group(group):
        return slice(group * 8, group * 8 + 8)

    def filtered(branch, target, begin=0, end=ROWS // 8):
        for group in range(GROUPS):
            taps = [tap_of(branch, j, group) for j in range(TAPS)]

            @pl.loop(begin, end)
            def _(eight):
                window = [row_of(rows, eight, group, r) for r in range(-6, 8)]
                for i in range(8):
                    target(eight * 8 + i, group, short(window, taps, i))

    def prepare():
        for tile in range(TILES):
            for branch in range(3):
                base = (branch * TILES + tile) * 8
                tap_rows[base : base + TAPS, :] = short_taps[branch, :, lanes_of(tile)]
            for half in range(2):
                modes = slice(half * 8, half * 8 + 8)
                rate = mode_rates[modes, lanes_of(tile)]
                rate_rows[half, tile * 8 : tile * 8 + 8, :] = rate
                weight_rows[half, tile * 8 : tile * 8 + 8, :] = (
                    residues[modes, lanes_of(tile)] * jnp.sqrt(rate)
                )

        def keep_query(t, group, result):
            queries[t, at_group(group), :] = result

        def keep_key(t, group, result):
            mixed[t, at_group(group), :] = result

        wait_edge(0)
        spread(query_in, edges.at[0], first_block, rows)
        filtered(0, keep_query)
        wait_edge(1)
        spread(key_in, edges.at[1], first_block, rows)
        filtered(1, keep_key)

    def gather_value():
        for quarter in range(4):
            came = arrived.at[quarter]
            copy(came, came, swap_send.at[quarter], swap_recv.at[quarter], {"ch": ch}).wait_recv()

        def block_rows(pair):
            for tile in range(TILES):
                quarter, columns = tile // 8, lanes_of(tile % 8)
                where = pl.ds(pl.multiple_of(pair * 16, 16), 16)
                block = total[0, quarter, where, columns] + arrived[quarter, where, columns]
                block = block.astype(jnp.bfloat16)
                if isinstance(pair, int):
                    last[:, lanes_of(tile)] = block[8:]
                block = block.astype(jnp.float32)
                base = pl.multiple_of((2 * pair + 1) * TILES * 8 + tile * 8, 8)
                rows[pl.ds(base, 8), :] = block[:8]
                rows[pl.ds(base + TILES * 8, 8), :] = block[8:]

        block_rows(ROWS // 16 - 1)
        send(last, edges.at[2], edge_send.at[2], edge_recv.at[2], block_device(1))
        pl.loop(0, ROWS // 16 - 1)(block_rows)

    def mix():
        def keep(t, group, result):
            product = mixed[t, at_group(group), :] * result
            mixed[t, at_group(group), :] = product.astype(jnp.bfloat16).astype(jnp.float32)

        filtered(2, keep, 1, ROWS // 8)

    def mix_first():
        def keep(t, group, result):
            product = mixed[t, at_group(group), :] * result
            mixed[t, at_group(group), :] = product.astype(jnp.bfloat16).astype(jnp.float32)

        wait_edge(2)
        spread_edge(edges.at[2], first_block, rows)
        filtered(2, keep, 0, 1)

    def decays(group):
        return [jnp.exp(-mode_of(rate_rows, n, group)) for n in range(MODES)]

    zeros = (jnp.zeros((8, LANES), jnp.float32),) * MODES

    def run_modes(group, rates, begin, end, held):
        def advance(eight, held):
            for i in range(8):
                entry = mixed[eight * 8 + i, at_group(group), :]
                held = tuple(rates[n] * held[n] + entry for n in range(MODES))
            return held

        return lax.fori_loop(begin, end, advance, held)

    def store_states(group, held):
        for n in range(MODES):
            states[group // 2, n // 8, pl.ds(group % 2 * 8 + n % 8, 8, stride=16), :] = held[n]

    def summarize(group):
        store_states(group, run_modes(group, decays(group), 1, ROWS // 8, zeros))

    def summarize_first(group):
        held = run_modes(group, decays(group), 0, 1, zeros)
        rest = [jnp.exp(-float(ROWS - 8) * mode_of(rate_rows, n, group)) for n in range(MODES)]
        store_states(
            group, [state_of(states, n, group) + rest[n] * held[n] for n in range(MODES)]
        )

    def localize(group):
        rates = decays(group)
        weighting = [mode_of(weight_rows, n, group) for n in range(MODES)]

        def advance(eight, held):
            for i in range(8):
                entry = mixed[eight * 8 + i, at_group(group), :]
                held = tuple(rates[n] * held[n] + entry for n in range(MODES))
                local[eight * 8 + i, at_group(group), :] = summed(
                    [weighting[n] * held[n] for n in range(MODES)]
                )
            return held

        lax.fori_loop(0, ROWS // 8, advance, zeros)

    def finish_group(group):
        rates = decays(group)
        skip = skip_gain[at_group(group), :]
        first = tuple(
            mode_of(weight_rows, n, group) * state_of(carried, n, group) for n in range(MODES)
        )

        def advance(eight, held):
            for i in range(8):
                held = tuple(rates[n] * held[n] for n in range(MODES))
                t = eight * 8 + i
                convolved = local[t, at_group(group), :] + summed(list(held))
                convolved = convolved.astype(jnp.bfloat16).astype(jnp.float32)
                result = queries[t, at_group(group), :] * (
                    convolved + skip * mixed[t, at_group(group), :]
                )
                out[pl.ds(eight * TILES * 8 + group * 64 + i, 8, stride=8), :] = result
            return held

        lax.fori_loop(0, ROWS // 8, advance, first)

    def near_part(at):
        return pl.ds(pl.multiple_of(at * 16, 16), 16)

    def near_rates(half):
        starts = [pl.multiple_of((2 * half + i) * 64 + near * 8, 8) for i in range(2)]
        return jnp.concatenate([rate_rows[:, pl.ds(start, 8), :] for start in starts], axis=1)

    def wait_all(buffer, sends, recvs, offsets, index):
        for by in offsets:
            came = buffer(index(by))
            copy(came, came, sends.at[by - 1], recvs.at[by - 1], {"ch": ch}).wait_recv()

    def send_near(half):
        for by in range(1, 8):
            to, device = near_device(by)
            send(
                states.at[half, :, near_part(to)],
                group_states.at[half, near],
                near_send.at[half, by - 1],
                near_recv.at[half, by - 1],
                device,
            )

    def send_across(buffer, slot, axis, half):
        own = buffer.at[half, place[axis]]
        for by in (2, 1, 3):
            send(
                own,
                own,
                scan_send.at[slot, half, by - 1],
                scan_recv.at[slot, half, by - 1],
                {axis: step(place[axis], by)},
            )

    def scan_across(buffer, slot, axis, half, decay):
        at = place[axis]
        wait_all(
            lambda i: buffer.at[half, i],
            scan_send.at[slot, half],
            scan_recv.at[slot, half],
            (1, 3, 2),
            lambda by: step(at, 4 - by),
        )
        running = jnp.zeros(decay.shape, jnp.float32)
        before = running
        for k in range(4):
            before = jnp.where(at == k, running, before)
            running = decay * running + buffer[half, k]
        return before, running

    def before_near(by):
        return lax.rem(near + 8 - by, 8)

    def scan_near(half):
        one = jnp.exp(-float(ROWS) * near_rates(half))
        group_states[half, near] = states[half, :, near_part(near), :]
        wait_all(
            lambda i: group_states.at[half, i],
            near_send.at[half],
            near_recv.at[half],
            range(1, 8),
            before_near,
        )
        held = jnp.zeros(one.shape, jnp.float32)
        for k in range(8):
            group_before[half, k] = held
            held = one * held + group_states[half, k]
        deep_states[half, zh] = held
        send_across(deep_states, 0, "zh", half)

    def scan_deep(half):
        decay = jnp.exp(-8.0 * ROWS * near_rates(half))
        before, running = scan_across(deep_states, 0, "zh", half, decay)
        wide_states[half, y] = running
        send_across(wide_states, 1, "y", half)
        return before

    def scan_wide(half, deep_before):
        rate = near_rates(half)
        one = jnp.exp(-float(ROWS) * rate)
        wide_before, _ = scan_across(wide_states, 1, "y", half, jnp.exp(-32.0 * ROWS * rate))
        shift = jnp.exp(rate * (-8.0 * ROWS * zh.astype(jnp.float32)))
        entering = deep_before + shift * wide_before
        for k in range(8):
            group_before[half, k] += entering
            entering = one * entering
        for by in range(1, 8):
            to, device = near_device(by)
            send(
                group_before.at[half, to],
                carried.at[half, :, near_part(near)],
                back_send.at[half, by - 1],
                back_recv.at[half, by - 1],
                device,
            )
        carried[half, :, near_part(near), :] = group_before[half, near]

    def wait_back(half):
        wait_all(
            lambda i: carried.at[half, :, near_part(i)],
            back_send.at[half],
            back_recv.at[half],
            range(1, 8),
            before_near,
        )

    FIRST, FORWARD, FINISH = range(3)

    def both(rings, pair, action):
        for unit in (2 * pair, 2 * pair + 1):
            rings[unit][action]()

    own_copy.wait()
    settle(0)
    early[0][FIRST]()
    deep[0][FIRST]()
    open_late(0, 0)
    settle(1)
    early[1][FIRST]()
    deep[1][FIRST]()
    open_late(1, 0)
    for unit in (0, 1):
        early[unit][FORWARD]()
        open_late(unit, 1)
        open_late(unit, 3)
    deep[0][FORWARD]()
    both(early, 1, FIRST)
    for unit in (0, 1):
        early[unit][FINISH]()
        open_late(unit, 2)
    both(early, 1, FORWARD)
    deep[0][FINISH]()
    deep[1][FORWARD]()
    both(early, 2, FIRST)
    both(late, 0, FORWARD)
    both(early, 1, FINISH)
    both(late, 1, FIRST)
    prepare()
    deep[1][FINISH]()
    both(early, 2, FORWARD)
    both(early, 3, FIRST)
    copy(tokens, chip_tokens.at[1], token_sems.at[0], token_sems.at[1], {"core": core}).wait_recv()
    both(late, 0, FINISH)
    project(0)
    both(late, 1, FORWARD)
    both(early, 2, FINISH)
    both(late, 2, FIRST)
    both(early, 3, FORWARD)
    both(late, 1, FINISH)
    project(1)
    project(3)
    join(0)
    expand(0, True, False)
    both(late, 2, FORWARD)
    both(early, 3, FINISH)
    both(late, 3, FIRST)
    both(late, 2, FINISH)
    project(2)
    join(1)
    expand(1, False, False)
    join(3)
    both(late, 3, FORWARD)
    late[6][FINISH]()
    expand(3, False, False)
    join(2)
    late[7][FINISH]()
    expand(2, False, True)
    gather_value()
    mix()
    summarize(0)
    summarize(1)
    mix_first()
    summarize_first(0)
    summarize_first(1)
    send_near(0)
    summarize(2)
    summarize(3)
    summarize_first(2)
    summarize_first(3)
    send_near(1)
    localize(0)
    localize(1)
    scan_near(0)
    localize(2)
    scan_near(1)
    localize(3)
    deep_before = [scan_deep(0)]
    deep_before.append(scan_deep(1))
    scan_wide(0, deep_before[0])
    scan_wide(1, deep_before[1])
    wait_back(0)
    finish_group(0)
    finish_group(1)
    wait_back(1)
    finish_group(2)
    finish_group(3)
    for made in started:
        made.wait_send()


def per_device(
    tokens, query_in, key_in, proj_in, proj_out, short_taps, residues, mode_rates, skip_gain
):
    f32, bf16 = jnp.float32, jnp.bfloat16
    dma = pltpu.SemaphoreType.DMA
    tiles = pl.pallas_call(
        operator_kernel,
        out_shape=jax.ShapeDtypeStruct((ROWS * TILES, LANES), f32),
        in_specs=[pl.BlockSpec(memory_space=pltpu.VMEM)] * 9,
        out_specs=pl.BlockSpec(memory_space=pltpu.VMEM),
        scratch_shapes=[
            pltpu.VMEM((8, WIDE), bf16),
            pltpu.VMEM((2, ROWS, WIDE), bf16),
            pltpu.VMEM((2, 4, RANKS, QUARTER), bf16),
            pltpu.VMEM((2, 4, 4, 4, BLOCK, QUARTER), bf16),
            pltpu.VMEM((4, 2 * ROWS, 4 * BLOCK), f32),
            pltpu.VMEM((4, 2 * ROWS, 4 * BLOCK), f32),
            pltpu.VMEM((4, 2 * ROWS, 4 * BLOCK), bf16),
            pltpu.VMEM((2, 4, ROWS, QUARTER), f32),
            pltpu.VMEM((4, ROWS, QUARTER), f32),
            pltpu.VMEM((3, 8, WIDE), bf16),
            pltpu.VMEM(((ROWS + 8) * TILES, LANES), f32),
            pltpu.VMEM((3 * TILES * 8, LANES), f32),
            pltpu.VMEM((2, TILES * 8, LANES), f32),
            pltpu.VMEM((2, TILES * 8, LANES), f32),
            pltpu.VMEM((ROWS, TILES, LANES), f32),
            pltpu.VMEM((ROWS, TILES, LANES), f32),
            pltpu.VMEM((ROWS, TILES, LANES), f32),
            pltpu.VMEM((2, 2, TILES * 4, LANES), f32),
            pltpu.VMEM((2, 2, TILES * 4, LANES), f32),
            pltpu.VMEM((2, 8, 2, 16, LANES), f32),
            pltpu.VMEM((2, 8, 2, 16, LANES), f32),
            pltpu.VMEM((2, 4, 2, 16, LANES), f32),
            pltpu.VMEM((2, 4, 2, 16, LANES), f32),
            dma,
            dma((2,)),
            dma((2, 3)),
            dma((2, 3)),
            dma((2, 4)),
            dma((2, 4)),
            dma((8, 10)),
            dma((8, 10)),
            dma((2, 4, 2)),
            dma((4,)),
            dma((4,)),
            dma((4,)),
            dma((4,)),
            dma((3,)),
            dma((3,)),
            dma((2, 7)),
            dma((2, 7)),
            dma((2, 2, 3)),
            dma((2, 2, 3)),
            dma((2, 7)),
            dma((2, 7)),
        ],
        compiler_params=pltpu.CompilerParams(
            collective_id=0, has_side_effects=True, vmem_limit_bytes=60 * 2**20
        ),
    )(
        tokens,
        proj_in.T,
        proj_out,
        query_in,
        key_in,
        short_taps,
        residues,
        mode_rates,
        skip_gain.reshape(TILES, LANES),
    )
    tiles = tiles.reshape(ROWS // 8, TILES, 8, LANES).transpose(0, 2, 1, 3)
    return tiles.reshape(ROWS, WIDE).astype(bf16)


def solution(mesh):
    split = Mesh(mesh.devices.reshape(4, 4, 4, 2, 2), ("y", "zh", "x", "core", "ch"))
    both = P(SEQ_AXES, "ch")
    placed = (
        both,
        both,
        both,
        P("ch", SEQ_AXES),
        both,
        P(None, None, "ch"),
        P(None, "ch"),
        P(None, "ch"),
        P("ch"),
    )
    return jax.shard_map(
        per_device, mesh=split, in_specs=placed, out_specs=both, check_vma=False
    )
```

```python
import jax
import jax.numpy as jnp
from jax import lax
from jax.experimental import pallas as pl
from jax.experimental.pallas import tpu as pltpu
from jax.sharding import Mesh
from jax.sharding import PartitionSpec as P

ROWS = 128
WIDE = 4096
LANES = 128
TILES = WIDE // LANES
GROUPS = TILES // 8
MODES = 16
TAPS = 7
SEQ_AXES = ("y", "zh", "x", "core")
MESH = pl.DeviceIdType.MESH
BLOCK = 48
QUARTER = 1024
RANKS = 12
UNITS = ((0, 0), (1, 0), (0, 1), (0, 3), (0, 2), (1, 1), (1, 3), (1, 2))


def lanes_of(tile):
    return slice(tile * LANES, (tile + 1) * LANES)


def spread_edge(edge, first_block, scratch):
    for tile in range(TILES):
        above = edge[:, lanes_of(tile)].astype(jnp.float32)
        scratch[tile * 8 : tile * 8 + 8, :] = jnp.where(first_block, 0.0, above)


def spread(source, edge, first_block, scratch):
    spread_edge(edge, first_block, scratch)

    @pl.loop(0, ROWS // 16)
    def _(pair):
        for tile in range(TILES):
            rows = pl.ds(pl.multiple_of(pair * 16, 16), 16)
            block = source[rows, lanes_of(tile)].astype(jnp.float32)
            base = pl.multiple_of((2 * pair + 1) * TILES * 8 + tile * 8, 8)
            scratch[pl.ds(base, 8), :] = block[:8]
            scratch[pl.ds(base + TILES * 8, 8), :] = block[8:]


def row_of(scratch, eight, group, row):
    start = (eight + (1 if row >= 0 else 0)) * TILES * 8 + group * 64 + row % 8
    return scratch[pl.ds(start, 8, stride=8), :]


def short(rows, taps, step):
    result = taps[0] * rows[step + 6]
    for offset in range(1, TAPS):
        result = result + taps[offset] * rows[step + 6 - offset]
    return result


def summed(terms):
    while len(terms) > 1:
        terms = [terms[i] + terms[i + 1] for i in range(0, len(terms), 2)]
    return terms[0]


def operator_kernel(
    tokens,
    pad_in,
    pad_out,
    query_in,
    key_in,
    short_taps,
    residues,
    mode_rates,
    skip_gain,
    out,
    last,
    chip_tokens,
    stage,
    weights,
    partial,
    theirs,
    low,
    total,
    arrived,
    edges,
    rows,
    tap_rows,
    rate_rows,
    weight_rows,
    queries,
    mixed,
    local,
    states,
    carried,
    group_states,
    group_before,
    deep_states,
    wide_states,
    own_sem,
    token_sems,
    stage_send,
    stage_recv,
    deep_send,
    deep_recv,
    ring_send,
    ring_recv,
    piece_send,
    far_send,
    far_recv,
    part_send,
    part_recv,
    swap_send,
    swap_recv,
    edge_send,
    edge_recv,
    near_send,
    near_recv,
    scan_send,
    scan_recv,
    back_send,
    back_recv,
):
    y, zh, x = lax.axis_index("y"), lax.axis_index("zh"), lax.axis_index("x")
    core, ch = lax.axis_index("core"), lax.axis_index("ch")
    place = {"x": x, "y": y, "zh": zh}
    pads = (pad_in, pad_out)
    started = []
    near = x * 2 + core
    block_at = (y * 4 + zh) * 8 + near
    first_block = block_at == 0

    def step(position, by):
        return lax.rem(position + by, 4)

    def copy(source, target, send, recv, device):
        return pltpu.make_async_remote_copy(
            src_ref=source,
            dst_ref=target,
            send_sem=send,
            recv_sem=recv,
            device_id=device,
            device_id_type=MESH,
        )

    def send(*arguments):
        made = copy(*arguments)
        made.start()
        started.append(made)

    def near_device(by):
        to = lax.rem(near + by, 8)
        return to, {"x": to // 2, "core": lax.rem(to, 2)}

    def block_device(by):
        to = lax.rem(block_at + by, 128)
        return {
            "y": to // 32,
            "zh": lax.rem(to // 8, 4),
            "x": lax.rem(to // 2, 4),
            "core": lax.rem(to, 2),
        }

    def send_edge(i, source):
        send(
            source.at[pl.ds(ROWS - 8, 8)],
            edges.at[i],
            edge_send.at[i],
            edge_recv.at[i],
            block_device(1),
        )

    def wait_edge(i):
        edge = edges.at[i]
        copy(edge, edge, edge_send.at[i], edge_recv.at[i], {"ch": ch}).wait_recv()

    barrier = pltpu.get_barrier_semaphore()
    greeted = [{"ch": 1 - ch}, block_device(1), block_device(127)]
    greeted += [near_device(by)[1] for by in range(1, 8)]
    greeted += [{axis: step(place[axis], by)} for axis in ("zh", "y") for by in (1, 2, 3)]
    for device in greeted:
        pl.semaphore_signal(barrier, inc=1, device_id=device, device_id_type=MESH)
    own_copy = pltpu.make_async_copy(tokens, chip_tokens.at[0], own_sem)
    own_copy.start()
    pl.semaphore_wait(barrier, len(greeted))

    for f in range(2):
        for by in (1, 3, 2):
            to = step(x, by)
            columns = pl.ds(pl.multiple_of(to * QUARTER, QUARTER), QUARTER)
            send(
                pads[f].at[:, columns],
                stage.at[f, x],
                stage_send.at[f, by - 1],
                stage_recv.at[f, by - 1],
                {"x": to},
            )
    send(tokens, chip_tokens.at[1], token_sems.at[0], token_sems.at[1], {"core": 1 - core})
    for i, source in enumerate((query_in, key_in)):
        send_edge(i, source)

    def settle(f):
        columns = pl.ds(pl.multiple_of(x * QUARTER, QUARTER), QUARTER)
        own = pltpu.make_async_copy(pads[f].at[:, columns], stage.at[f, x], own_sem)
        own.start()
        own.wait()
        for by in (1, 3, 2):
            came = stage.at[f, step(x, 4 - by)]
            copy(came, came, stage_send.at[f, by - 1], stage_recv.at[f, by - 1], {"x": x}).wait_recv()
        parts = [stage[f, i].astype(jnp.float32) for i in range(4)]
        weights[f, y, zh, x] = jnp.concatenate(parts, axis=0).astype(jnp.bfloat16)

    def ring(axis, item, send_sems, recv_sems, split=False, relayed=None):
        at = place[axis]
        plus, minus, far = step(at, 1), step(at, 3), step(at, 2)

        def out(ref, slot, to):
            send(ref, ref, send_sems(slot), recv_sems(slot), {axis: to})

        def landed(ref, slot):
            copy(ref, ref, send_sems(slot), recv_sems(slot), {axis: at}).wait_recv()

        def first():
            if split:
                out(item(at, 0), 0, plus)
                out(item(at, 1), 1, minus)
                out(item(at, 1), 4, plus)
                out(item(at, 0), 5, minus)
            else:
                out(item(at), 0, plus)
                out(item(at), 1, minus)

        def forward():
            landed(item(minus, 0 if split else None), 0)
            if relayed is None:
                out(item(minus, 0), 2, plus)
            landed(item(plus, 1 if split else None), 1)
            if relayed is None:
                out(item(plus, 1), 3, minus)

        def finish_near():
            if split:
                landed(item(minus, 1), 4)
                landed(item(plus, 0), 5)

        def finish_far():
            if relayed is None:
                landed(item(far, 0), 2)
                landed(item(far, 1), 3)
            else:
                came = item(far)
                copy(came, came, far_send.at[relayed], far_recv.at[relayed], {axis: at}).wait_recv()

        def finish():
            finish_near()
            finish_far()

        return first, forward, finish, finish_near, finish_far

    def half_columns(half):
        return slice(None) if half is None else slice(half * 512, half * 512 + 512)

    def half_blocks(half):
        return slice(None) if half is None else slice(half * 2, half * 2 + 2)

    def deep_ring(f):
        return ring(
            "zh",
            lambda i, half=None: weights.at[f, y, i, x, :, half_columns(half)],
            lambda slot: deep_send.at[f, slot],
            lambda slot: deep_recv.at[f, slot],
        )

    def unit_ring(unit, late):
        f, r = UNITS[unit]
        deep = step(zh, r)
        across = unit % 2 == 0

        def item(i, half=None):
            if late:
                if across:
                    return weights.at[f, i, deep, half_blocks(half)]
                return weights.at[f, half_blocks(half), deep, i]
            if across:
                return weights.at[f, y, deep, i, :, half_columns(half)]
            return weights.at[f, i, deep, x, :, half_columns(half)]

        base = 4 if late else 0
        return ring(
            "x" if across != late else "y",
            item,
            lambda slot: ring_send.at[unit, base + slot],
            lambda slot: ring_recv.at[unit, base + slot],
            late and unit >= 2,
            {5: 0, 6: 1}.get(unit) if late else None,
        )

    def relay_far():
        column = weights.at[1, :, zh, step(x, 2)]
        send(column, column, far_send.at[0], far_recv.at[0], {"zh": step(zh, 3)})
        strip = weights.at[1, step(y, 2), zh]
        send(strip, strip, far_send.at[1], far_recv.at[1], {"zh": step(zh, 1)})

    def open_late(unit, by):
        deep = zh
        if unit == 0:
            axis, piece = "y", weights.at[0, y, deep, step(x, by)]
        else:
            axis, piece = "x", weights.at[1, step(y, by), deep, x]
        for slot, to in ((0, 1), (1, 3)):
            send(
                piece,
                piece,
                piece_send.at[unit, by, slot],
                ring_recv.at[unit, 4 + slot],
                {axis: step(place[axis], to)},
            )

    deep = [deep_ring(f) for f in range(2)]
    early = [unit_ring(unit, False) for unit in range(8)]
    late = [unit_ring(unit, True) for unit in range(8)]

    def unit_weights(f, r, quarter):
        return weights[f, :, step(zh, r), quarter].reshape(4 * BLOCK, QUARTER)

    def project(r):
        @pl.loop(0, 4)
        def _(quarter):
            columns = pl.ds(pl.multiple_of(quarter * QUARTER, QUARTER), QUARTER)
            part = lax.dot_general(
                chip_tokens[:, :, columns].reshape(2 * ROWS, QUARTER),
                unit_weights(0, r, quarter),
                (((1,), (1,)), ((), ())),
                preferred_element_type=jnp.float32,
            )

            @pl.when(quarter == 0)
            def _():
                partial[r] = part

            @pl.when(quarter > 0)
            def _():
                partial[r] += part

        send(partial.at[r], theirs.at[r], part_send.at[r], part_recv.at[r], {"ch": 1 - ch})

    def join(r):
        copy(partial.at[r], theirs.at[r], part_send.at[r], part_recv.at[r], {"ch": ch}).wait_recv()
        low[r] = (partial[r] + theirs[r]).astype(jnp.bfloat16)

    def product(r, quarter):
        return jnp.dot(
            low[r], unit_weights(1, r, quarter), preferred_element_type=jnp.float32
        ).reshape(2, ROWS, QUARTER)

    def expand(r, opening):
        for quarter in range(4):
            if opening:
                total[:, quarter] = product(r, quarter)
            else:
                total[:, quarter] += product(r, quarter)

    def close(r, by):
        quarter = step(x, by)
        total[:, quarter] += product(r, quarter)
        send(
            total.at[1, quarter],
            arrived.at[quarter],
            swap_send.at[by],
            swap_recv.at[by],
            {"core": 1 - core},
        )

    def tap_of(branch, offset, group):
        start = (branch * TILES + group * 8) * 8 + offset
        return tap_rows[pl.ds(start, 8, stride=8), :]

    def mode_of(ref, n, group):
        half, row = n // 8, n % 8
        return ref[half, pl.ds(group * 64 + row, 8, stride=8), :]

    def state_of(ref, n, group):
        return ref[group // 2, n // 8, pl.ds(group % 2 * 8 + n % 8, 8, stride=16), :]

    def at_group(group):
        return slice(group * 8, group * 8 + 8)

    def filtered(branch, target, begin=0, end=ROWS // 8):
        for group in range(GROUPS):
            taps = [tap_of(branch, j, group) for j in range(TAPS)]

            @pl.loop(begin, end)
            def _(eight):
                window = [row_of(rows, eight, group, r) for r in range(-6, 8)]
                for i in range(8):
                    target(eight * 8 + i, group, short(window, taps, i))

    def prepare():
        for tile in range(TILES):
            for branch in range(3):
                base = (branch * TILES + tile) * 8
                tap_rows[base : base + TAPS, :] = short_taps[branch, :, lanes_of(tile)]
            for half in range(2):
                modes = slice(half * 8, half * 8 + 8)
                rate = mode_rates[modes, lanes_of(tile)]
                rate_rows[half, tile * 8 : tile * 8 + 8, :] = rate
                weight_rows[half, tile * 8 : tile * 8 + 8, :] = (
                    residues[modes, lanes_of(tile)] * jnp.sqrt(rate)
                )

        def keep_query(t, group, result):
            queries[t, at_group(group), :] = result

        def keep_key(t, group, result):
            mixed[t, at_group(group), :] = result

        wait_edge(0)
        spread(query_in, edges.at[0], first_block, rows)
        filtered(0, keep_query)
        wait_edge(1)
        spread(key_in, edges.at[1], first_block, rows)
        filtered(1, keep_key)

    def gather_value():
        for by in range(4):
            came = arrived.at[step(x, by)]
            copy(came, came, swap_send.at[by], swap_recv.at[by], {"ch": ch}).wait_recv()

        def block_rows(pair):
            for tile in range(TILES):
                quarter, columns = tile // 8, lanes_of(tile % 8)
                where = pl.ds(pl.multiple_of(pair * 16, 16), 16)
                block = total[0, quarter, where, columns] + arrived[quarter, where, columns]
                block = block.astype(jnp.bfloat16)
                if isinstance(pair, int):
                    last[:, lanes_of(tile)] = block[8:]
                block = block.astype(jnp.float32)
                base = pl.multiple_of((2 * pair + 1) * TILES * 8 + tile * 8, 8)
                rows[pl.ds(base, 8), :] = block[:8]
                rows[pl.ds(base + TILES * 8, 8), :] = block[8:]

        block_rows(ROWS // 16 - 1)
        send(last, edges.at[2], edge_send.at[2], edge_recv.at[2], block_device(1))
        pl.loop(0, ROWS // 16 - 1)(block_rows)

    def mix():
        def keep(t, group, result):
            product = mixed[t, at_group(group), :] * result
            mixed[t, at_group(group), :] = product.astype(jnp.bfloat16).astype(jnp.float32)

        filtered(2, keep, 1, ROWS // 8)

    def mix_first():
        def keep(t, group, result):
            product = mixed[t, at_group(group), :] * result
            mixed[t, at_group(group), :] = product.astype(jnp.bfloat16).astype(jnp.float32)

        wait_edge(2)
        spread_edge(edges.at[2], first_block, rows)
        filtered(2, keep, 0, 1)

    def decays(group):
        return [jnp.exp(-mode_of(rate_rows, n, group)) for n in range(MODES)]

    zeros = (jnp.zeros((8, LANES), jnp.float32),) * MODES

    def run_modes(group, rates, begin, end, held):
        def advance(eight, held):
            for i in range(8):
                entry = mixed[eight * 8 + i, at_group(group), :]
                held = tuple(rates[n] * held[n] + entry for n in range(MODES))
            return held

        return lax.fori_loop(begin, end, advance, held)

    def store_states(group, held):
        for n in range(MODES):
            states[group // 2, n // 8, pl.ds(group % 2 * 8 + n % 8, 8, stride=16), :] = held[n]

    def summarize(group):
        store_states(group, run_modes(group, decays(group), 1, ROWS // 8, zeros))

    def summarize_first(group):
        held = run_modes(group, decays(group), 0, 1, zeros)
        rest = [jnp.exp(-float(ROWS - 8) * mode_of(rate_rows, n, group)) for n in range(MODES)]
        store_states(
            group, [state_of(states, n, group) + rest[n] * held[n] for n in range(MODES)]
        )

    def localize(group):
        rates = decays(group)
        weighting = [mode_of(weight_rows, n, group) for n in range(MODES)]

        def advance(eight, held):
            for i in range(8):
                entry = mixed[eight * 8 + i, at_group(group), :]
                held = tuple(rates[n] * held[n] + entry for n in range(MODES))
                local[eight * 8 + i, at_group(group), :] = summed(
                    [weighting[n] * held[n] for n in range(MODES)]
                )
            return held

        lax.fori_loop(0, ROWS // 8, advance, zeros)

    def finish_group(group):
        rates = decays(group)
        skip = skip_gain[at_group(group), :]
        first = tuple(
            mode_of(weight_rows, n, group) * state_of(carried, n, group) for n in range(MODES)
        )

        def advance(eight, held):
            for i in range(8):
                held = tuple(rates[n] * held[n] for n in range(MODES))
                t = eight * 8 + i
                convolved = local[t, at_group(group), :] + summed(list(held))
                convolved = convolved.astype(jnp.bfloat16).astype(jnp.float32)
                result = queries[t, at_group(group), :] * (
                    convolved + skip * mixed[t, at_group(group), :]
                )
                out[pl.ds(eight * TILES * 8 + group * 64 + i, 8, stride=8), :] = result
            return held

        lax.fori_loop(0, ROWS // 8, advance, first)

    def near_part(at):
        return pl.ds(pl.multiple_of(at * 16, 16), 16)

    def near_rates(half):
        starts = [pl.multiple_of((2 * half + i) * 64 + near * 8, 8) for i in range(2)]
        return jnp.concatenate([rate_rows[:, pl.ds(start, 8), :] for start in starts], axis=1)

    def wait_all(buffer, sends, recvs, offsets, index):
        for by in offsets:
            came = buffer(index(by))
            copy(came, came, sends.at[by - 1], recvs.at[by - 1], {"ch": ch}).wait_recv()

    def send_near(half):
        for by in range(1, 8):
            to, device = near_device(by)
            send(
                states.at[half, :, near_part(to)],
                group_states.at[half, near],
                near_send.at[half, by - 1],
                near_recv.at[half, by - 1],
                device,
            )

    def send_across(buffer, slot, axis, half):
        own = buffer.at[half, place[axis]]
        for by in (2, 1, 3):
            send(
                own,
                own,
                scan_send.at[slot, half, by - 1],
                scan_recv.at[slot, half, by - 1],
                {axis: step(place[axis], by)},
            )

    def scan_across(buffer, slot, axis, half, decay):
        at = place[axis]
        wait_all(
            lambda i: buffer.at[half, i],
            scan_send.at[slot, half],
            scan_recv.at[slot, half],
            (1, 3, 2),
            lambda by: step(at, 4 - by),
        )
        running = jnp.zeros(decay.shape, jnp.float32)
        before = running
        for k in range(4):
            before = jnp.where(at == k, running, before)
            running = decay * running + buffer[half, k]
        return before, running

    def before_near(by):
        return lax.rem(near + 8 - by, 8)

    def scan_near(half):
        one = jnp.exp(-float(ROWS) * near_rates(half))
        group_states[half, near] = states[half, :, near_part(near), :]
        wait_all(
            lambda i: group_states.at[half, i],
            near_send.at[half],
            near_recv.at[half],
            range(1, 8),
            before_near,
        )
        held = jnp.zeros(one.shape, jnp.float32)
        for k in range(8):
            group_before[half, k] = held
            held = one * held + group_states[half, k]
        deep_states[half, zh] = held
        send_across(deep_states, 0, "zh", half)

    def scan_deep(half):
        decay = jnp.exp(-8.0 * ROWS * near_rates(half))
        before, running = scan_across(deep_states, 0, "zh", half, decay)
        wide_states[half, y] = running
        send_across(wide_states, 1, "y", half)
        return before

    def scan_wide(half, deep_before):
        rate = near_rates(half)
        one = jnp.exp(-float(ROWS) * rate)
        wide_before, _ = scan_across(wide_states, 1, "y", half, jnp.exp(-32.0 * ROWS * rate))
        shift = jnp.exp(rate * (-8.0 * ROWS * zh.astype(jnp.float32)))
        entering = deep_before + shift * wide_before
        for k in range(8):
            group_before[half, k] += entering
            entering = one * entering
        for by in range(1, 8):
            to, device = near_device(by)
            send(
                group_before.at[half, to],
                carried.at[half, :, near_part(near)],
                back_send.at[half, by - 1],
                back_recv.at[half, by - 1],
                device,
            )
        carried[half, :, near_part(near), :] = group_before[half, near]

    def wait_back(half):
        wait_all(
            lambda i: carried.at[half, :, near_part(i)],
            back_send.at[half],
            back_recv.at[half],
            range(1, 8),
            before_near,
        )

    FIRST, FORWARD, FINISH, NEAR, FAR = range(5)

    def both(rings, pair, action):
        for unit in (2 * pair, 2 * pair + 1):
            rings[unit][action]()

    own_copy.wait()
    settle(0)
    early[0][FIRST]()
    deep[0][FIRST]()
    open_late(0, 0)
    settle(1)
    early[1][FIRST]()
    deep[1][FIRST]()
    open_late(1, 0)
    for unit in (0, 1):
        early[unit][FORWARD]()
        open_late(unit, 1)
        open_late(unit, 3)
    deep[0][FORWARD]()
    both(early, 1, FIRST)
    for unit in (0, 1):
        early[unit][FINISH]()
        open_late(unit, 2)
    both(early, 1, FORWARD)
    deep[0][FINISH]()
    deep[1][FORWARD]()
    both(early, 2, FIRST)
    both(late, 0, FORWARD)
    both(early, 1, FINISH)
    both(late, 1, FIRST)
    prepare()
    deep[1][FINISH]()
    both(early, 2, FORWARD)
    both(early, 3, FIRST)
    copy(tokens, chip_tokens.at[1], token_sems.at[0], token_sems.at[1], {"core": core}).wait_recv()
    both(late, 0, FINISH)
    project(0)
    relay_far()
    both(late, 1, FORWARD)
    both(early, 2, FINISH)
    both(late, 2, FIRST)
    both(early, 3, FORWARD)
    both(late, 1, FINISH)
    project(1)
    project(3)
    both(late, 2, FORWARD)
    both(early, 3, FINISH)
    both(late, 3, FIRST)
    join(0)
    expand(0, True)
    late[4][FINISH]()
    project(2)
    late[5][FINISH]()
    join(1)
    expand(1, False)
    both(late, 3, FORWARD)
    join(3)
    late[6][FINISH]()
    expand(3, False)
    join(2)
    close(2, 0)
    late[7][NEAR]()
    close(2, 1)
    close(2, 3)
    late[7][FAR]()
    close(2, 2)
    gather_value()
    mix()
    summarize(0)
    summarize(1)
    mix_first()
    summarize_first(0)
    summarize_first(1)
    send_near(0)
    summarize(2)
    summarize(3)
    summarize_first(2)
    summarize_first(3)
    send_near(1)
    localize(0)
    localize(1)
    scan_near(0)
    localize(2)
    scan_near(1)
    localize(3)
    deep_before = [scan_deep(0)]
    deep_before.append(scan_deep(1))
    scan_wide(0, deep_before[0])
    scan_wide(1, deep_before[1])
    wait_back(0)
    finish_group(0)
    finish_group(1)
    wait_back(1)
    finish_group(2)
    finish_group(3)
    for made in started:
        made.wait_send()


def per_device(
    tokens, query_in, key_in, proj_in, proj_out, short_taps, residues, mode_rates, skip_gain
):
    f32, bf16 = jnp.float32, jnp.bfloat16
    dma = pltpu.SemaphoreType.DMA
    tiles = pl.pallas_call(
        operator_kernel,
        out_shape=jax.ShapeDtypeStruct((ROWS * TILES, LANES), f32),
        in_specs=[pl.BlockSpec(memory_space=pltpu.VMEM)] * 9,
        out_specs=pl.BlockSpec(memory_space=pltpu.VMEM),
        scratch_shapes=[
            pltpu.VMEM((8, WIDE), bf16),
            pltpu.VMEM((2, ROWS, WIDE), bf16),
            pltpu.VMEM((2, 4, RANKS, QUARTER), bf16),
            pltpu.VMEM((2, 4, 4, 4, BLOCK, QUARTER), bf16),
            pltpu.VMEM((4, 2 * ROWS, 4 * BLOCK), f32),
            pltpu.VMEM((4, 2 * ROWS, 4 * BLOCK), f32),
            pltpu.VMEM((4, 2 * ROWS, 4 * BLOCK), bf16),
            pltpu.VMEM((2, 4, ROWS, QUARTER), f32),
            pltpu.VMEM((4, ROWS, QUARTER), f32),
            pltpu.VMEM((3, 8, WIDE), bf16),
            pltpu.VMEM(((ROWS + 8) * TILES, LANES), f32),
            pltpu.VMEM((3 * TILES * 8, LANES), f32),
            pltpu.VMEM((2, TILES * 8, LANES), f32),
            pltpu.VMEM((2, TILES * 8, LANES), f32),
            pltpu.VMEM((ROWS, TILES, LANES), f32),
            pltpu.VMEM((ROWS, TILES, LANES), f32),
            pltpu.VMEM((ROWS, TILES, LANES), f32),
            pltpu.VMEM((2, 2, TILES * 4, LANES), f32),
            pltpu.VMEM((2, 2, TILES * 4, LANES), f32),
            pltpu.VMEM((2, 8, 2, 16, LANES), f32),
            pltpu.VMEM((2, 8, 2, 16, LANES), f32),
            pltpu.VMEM((2, 4, 2, 16, LANES), f32),
            pltpu.VMEM((2, 4, 2, 16, LANES), f32),
            dma,
            dma((2,)),
            dma((2, 3)),
            dma((2, 3)),
            dma((2, 4)),
            dma((2, 4)),
            dma((8, 10)),
            dma((8, 10)),
            dma((2, 4, 2)),
            dma((2,)),
            dma((2,)),
            dma((4,)),
            dma((4,)),
            dma((4,)),
            dma((4,)),
            dma((3,)),
            dma((3,)),
            dma((2, 7)),
            dma((2, 7)),
            dma((2, 2, 3)),
            dma((2, 2, 3)),
            dma((2, 7)),
            dma((2, 7)),
        ],
        compiler_params=pltpu.CompilerParams(
            collective_id=0, has_side_effects=True, vmem_limit_bytes=60 * 2**20
        ),
    )(
        tokens,
        proj_in.T,
        proj_out,
        query_in,
        key_in,
        short_taps,
        residues,
        mode_rates,
        skip_gain.reshape(TILES, LANES),
    )
    tiles = tiles.reshape(ROWS // 8, TILES, 8, LANES).transpose(0, 2, 1, 3)
    return tiles.reshape(ROWS, WIDE).astype(bf16)


def solution(mesh):
    split = Mesh(mesh.devices.reshape(4, 4, 4, 2, 2), ("y", "zh", "x", "core", "ch"))
    both = P(SEQ_AXES, "ch")
    placed = (
        both,
        both,
        both,
        P("ch", SEQ_AXES),
        both,
        P(None, None, "ch"),
        P(None, "ch"),
        P(None, "ch"),
        P("ch"),
    )
    return jax.shard_map(
        per_device, mesh=split, in_specs=placed, out_specs=both, check_vma=False
    )
```

```python
import jax
import jax.numpy as jnp
from jax import lax
from jax.experimental import pallas as pl
from jax.experimental.pallas import tpu as pltpu
from jax.sharding import Mesh
from jax.sharding import PartitionSpec as P

ROWS = 128
WIDE = 4096
LANES = 128
TILES = WIDE // LANES
GROUPS = TILES // 8
MODES = 16
TAPS = 7
SEQ_AXES = ("y", "zh", "x", "core")
MESH = pl.DeviceIdType.MESH
BLOCK = 48
QUARTER = 1024
RANKS = 12
UNITS = ((0, 0), (1, 0), (0, 1), (0, 3), (0, 2), (1, 2), (1, 3), (1, 1))


def lanes_of(tile):
    return slice(tile * LANES, (tile + 1) * LANES)


def spread_edge(edge, first_block, scratch):
    for tile in range(TILES):
        above = edge[:, lanes_of(tile)].astype(jnp.float32)
        scratch[tile * 8 : tile * 8 + 8, :] = jnp.where(first_block, 0.0, above)


def spread(source, edge, first_block, scratch):
    spread_edge(edge, first_block, scratch)

    @pl.loop(0, ROWS // 16)
    def _(pair):
        for tile in range(TILES):
            rows = pl.ds(pl.multiple_of(pair * 16, 16), 16)
            block = source[rows, lanes_of(tile)].astype(jnp.float32)
            base = pl.multiple_of((2 * pair + 1) * TILES * 8 + tile * 8, 8)
            scratch[pl.ds(base, 8), :] = block[:8]
            scratch[pl.ds(base + TILES * 8, 8), :] = block[8:]


def row_of(scratch, eight, group, row):
    start = (eight + (1 if row >= 0 else 0)) * TILES * 8 + group * 64 + row % 8
    return scratch[pl.ds(start, 8, stride=8), :]


def short(rows, taps, step):
    result = taps[0] * rows[step + 6]
    for offset in range(1, TAPS):
        result = result + taps[offset] * rows[step + 6 - offset]
    return result


def summed(terms):
    while len(terms) > 1:
        terms = [terms[i] + terms[i + 1] for i in range(0, len(terms), 2)]
    return terms[0]


def operator_kernel(
    tokens,
    pad_in,
    pad_out,
    query_in,
    key_in,
    short_taps,
    residues,
    mode_rates,
    skip_gain,
    out,
    last,
    chip_tokens,
    stage,
    weights,
    partial,
    theirs,
    low,
    total,
    arrived,
    edges,
    rows,
    tap_rows,
    rate_rows,
    weight_rows,
    queries,
    mixed,
    local,
    states,
    carried,
    group_states,
    group_before,
    deep_states,
    wide_states,
    own_sem,
    token_sems,
    stage_send,
    stage_recv,
    deep_send,
    deep_recv,
    ring_send,
    ring_recv,
    piece_send,
    far_send,
    far_recv,
    part_send,
    part_recv,
    swap_send,
    swap_recv,
    edge_send,
    edge_recv,
    near_send,
    near_recv,
    scan_send,
    scan_recv,
    back_send,
    back_recv,
):
    y, zh, x = lax.axis_index("y"), lax.axis_index("zh"), lax.axis_index("x")
    core, ch = lax.axis_index("core"), lax.axis_index("ch")
    place = {"x": x, "y": y, "zh": zh}
    pads = (pad_in, pad_out)
    started = []
    near = x * 2 + core
    block_at = (y * 4 + zh) * 8 + near
    first_block = block_at == 0

    def step(position, by):
        return lax.rem(position + by, 4)

    def copy(source, target, send, recv, device):
        return pltpu.make_async_remote_copy(
            src_ref=source,
            dst_ref=target,
            send_sem=send,
            recv_sem=recv,
            device_id=device,
            device_id_type=MESH,
        )

    def send(*arguments):
        made = copy(*arguments)
        made.start()
        started.append(made)

    def near_device(by):
        to = lax.rem(near + by, 8)
        return to, {"x": to // 2, "core": lax.rem(to, 2)}

    def block_device(by):
        to = lax.rem(block_at + by, 128)
        return {
            "y": to // 32,
            "zh": lax.rem(to // 8, 4),
            "x": lax.rem(to // 2, 4),
            "core": lax.rem(to, 2),
        }

    def send_edge(i, source):
        send(
            source.at[pl.ds(ROWS - 8, 8)],
            edges.at[i],
            edge_send.at[i],
            edge_recv.at[i],
            block_device(1),
        )

    def wait_edge(i):
        edge = edges.at[i]
        copy(edge, edge, edge_send.at[i], edge_recv.at[i], {"ch": ch}).wait_recv()

    barrier = pltpu.get_barrier_semaphore()
    greeted = [{"ch": 1 - ch}, block_device(1), block_device(127)]
    greeted += [near_device(by)[1] for by in range(1, 8)]
    greeted += [{axis: step(place[axis], by)} for axis in ("zh", "y") for by in (1, 2, 3)]
    for device in greeted:
        pl.semaphore_signal(barrier, inc=1, device_id=device, device_id_type=MESH)
    own_copy = pltpu.make_async_copy(tokens, chip_tokens.at[0], own_sem)
    own_copy.start()
    pl.semaphore_wait(barrier, len(greeted))

    for f in range(2):
        for by in (1, 3, 2):
            to = step(x, by)
            columns = pl.ds(pl.multiple_of(to * QUARTER, QUARTER), QUARTER)
            send(
                pads[f].at[:, columns],
                stage.at[f, x],
                stage_send.at[f, by - 1],
                stage_recv.at[f, by - 1],
                {"x": to},
            )
    send(tokens, chip_tokens.at[1], token_sems.at[0], token_sems.at[1], {"core": 1 - core})
    for i, source in enumerate((query_in, key_in)):
        send_edge(i, source)

    def settle(f):
        columns = pl.ds(pl.multiple_of(x * QUARTER, QUARTER), QUARTER)
        own = pltpu.make_async_copy(pads[f].at[:, columns], stage.at[f, x], own_sem)
        own.start()
        own.wait()
        for by in (1, 3, 2):
            came = stage.at[f, step(x, 4 - by)]
            copy(came, came, stage_send.at[f, by - 1], stage_recv.at[f, by - 1], {"x": x}).wait_recv()
        parts = [stage[f, i].astype(jnp.float32) for i in range(4)]
        weights[f, y, zh, x] = jnp.concatenate(parts, axis=0).astype(jnp.bfloat16)

    def ring(axis, item, send_sems, recv_sems, split=False, relayed=None):
        at = place[axis]
        plus, minus, far = step(at, 1), step(at, 3), step(at, 2)

        def out(ref, slot, to):
            send(ref, ref, send_sems(slot), recv_sems(slot), {axis: to})

        def landed(ref, slot):
            copy(ref, ref, send_sems(slot), recv_sems(slot), {axis: at}).wait_recv()

        def first():
            if split:
                out(item(at, 0), 0, plus)
                out(item(at, 1), 1, minus)
                out(item(at, 1), 4, plus)
                out(item(at, 0), 5, minus)
            else:
                out(item(at), 0, plus)
                out(item(at), 1, minus)

        def forward():
            landed(item(minus, 0 if split else None), 0)
            if relayed is None:
                out(item(minus, 0), 2, plus)
            landed(item(plus, 1 if split else None), 1)
            if relayed is None:
                out(item(plus, 1), 3, minus)

        def finish_near():
            if split:
                landed(item(minus, 1), 4)
                landed(item(plus, 0), 5)

        def finish_far():
            if relayed is None:
                landed(item(far, 0), 2)
                landed(item(far, 1), 3)
            else:
                came = item(far)
                copy(came, came, far_send.at[relayed], far_recv.at[relayed], {axis: at}).wait_recv()

        def finish():
            finish_near()
            finish_far()

        return first, forward, finish, finish_near, finish_far

    def half_columns(half):
        return slice(None) if half is None else slice(half * 512, half * 512 + 512)

    def half_blocks(half):
        return slice(None) if half is None else slice(half * 2, half * 2 + 2)

    def deep_ring(f):
        return ring(
            "zh",
            lambda i, half=None: weights.at[f, y, i, x, :, half_columns(half)],
            lambda slot: deep_send.at[f, slot],
            lambda slot: deep_recv.at[f, slot],
        )

    def unit_ring(unit, late):
        f, r = UNITS[unit]
        deep = step(zh, r)
        across = unit % 2 == 0

        def item(i, half=None):
            if late:
                if across:
                    return weights.at[f, i, deep, half_blocks(half)]
                return weights.at[f, half_blocks(half), deep, i]
            if across:
                return weights.at[f, y, deep, i, :, half_columns(half)]
            return weights.at[f, i, deep, x, :, half_columns(half)]

        base = 4 if late else 0
        return ring(
            "x" if across != late else "y",
            item,
            lambda slot: ring_send.at[unit, base + slot],
            lambda slot: ring_recv.at[unit, base + slot],
            late and unit >= 2,
            {7: 0, 6: 1}.get(unit) if late else None,
        )

    def relay_far():
        column = weights.at[1, :, zh, step(x, 2)]
        send(column, column, far_send.at[0], far_recv.at[0], {"zh": step(zh, 3)})
        strip = weights.at[1, step(y, 2), zh]
        send(strip, strip, far_send.at[1], far_recv.at[1], {"zh": step(zh, 1)})

    def open_late(unit, by):
        deep = zh
        if unit == 0:
            axis, piece = "y", weights.at[0, y, deep, step(x, by)]
        else:
            axis, piece = "x", weights.at[1, step(y, by), deep, x]
        for slot, to in ((0, 1), (1, 3)):
            send(
                piece,
                piece,
                piece_send.at[unit, by, slot],
                ring_recv.at[unit, 4 + slot],
                {axis: step(place[axis], to)},
            )

    deep = [deep_ring(f) for f in range(2)]
    early = [unit_ring(unit, False) for unit in range(8)]
    late = [unit_ring(unit, True) for unit in range(8)]

    def unit_weights(f, r, quarter):
        return weights[f, :, step(zh, r), quarter].reshape(4 * BLOCK, QUARTER)

    def quarter_dot(rows_in, quarter):
        columns = pl.ds(pl.multiple_of(quarter * QUARTER, QUARTER), QUARTER)
        return lax.dot_general(
            rows_in,
            chip_tokens[:, :, columns].reshape(2 * ROWS, QUARTER),
            (((1,), (1,)), ((), ())),
            preferred_element_type=jnp.float32,
        )

    def send_part(ref, other, i):
        send(ref, other, part_send.at[i], part_recv.at[i], {"ch": 1 - ch})

    def project(r):
        @pl.loop(0, 4)
        def _(quarter):
            part = quarter_dot(unit_weights(0, r, quarter), quarter)

            @pl.when(quarter == 0)
            def _():
                partial[r] = part

            @pl.when(quarter > 0)
            def _():
                partial[r] += part

        send_part(partial.at[r], theirs.at[r], r)

    def strip_of(by):
        return pl.ds(pl.multiple_of(step(y, by) * BLOCK, BLOCK), BLOCK)

    def project_strip(by):
        strip = strip_of(by)
        partial[2, strip, :] = summed(
            [quarter_dot(weights[0, step(y, by), step(zh, 2), q], q) for q in range(4)]
        )
        send_part(partial.at[2, strip], theirs.at[2, strip], 4 + by)

    def join(r):
        for by in range(4) if r == 2 else (None,):
            i = r if by is None else 4 + by
            came = theirs.at[r] if by is None else theirs.at[r, strip_of(by)]
            copy(came, came, part_send.at[i], part_recv.at[i], {"ch": ch}).wait_recv()
        low[r] = (partial[r] + theirs[r]).astype(jnp.bfloat16)

    def product(r, quarter):
        return lax.dot_general(
            low[r],
            unit_weights(1, r, quarter),
            (((0,), (0,)), ((), ())),
            preferred_element_type=jnp.float32,
        ).reshape(2, ROWS, QUARTER)

    def expand(r, opening):
        for quarter in range(4):
            if opening:
                total[:, quarter] = product(r, quarter)
            else:
                total[:, quarter] += product(r, quarter)

    def close(r, by):
        quarter = step(x, by)
        total[:, quarter] += product(r, quarter)
        send(
            total.at[1, quarter],
            arrived.at[quarter],
            swap_send.at[by],
            swap_recv.at[by],
            {"core": 1 - core},
        )

    def tap_of(branch, offset, group):
        start = (branch * TILES + group * 8) * 8 + offset
        return tap_rows[pl.ds(start, 8, stride=8), :]

    def mode_of(ref, n, group):
        half, row = n // 8, n % 8
        return ref[half, pl.ds(group * 64 + row, 8, stride=8), :]

    def state_of(ref, n, group):
        return ref[group // 2, n // 8, pl.ds(group % 2 * 8 + n % 8, 8, stride=16), :]

    def at_group(group):
        return slice(group * 8, group * 8 + 8)

    def filtered(branch, target, begin=0, end=ROWS // 8):
        for group in range(GROUPS):
            taps = [tap_of(branch, j, group) for j in range(TAPS)]

            @pl.loop(begin, end)
            def _(eight):
                window = [row_of(rows, eight, group, r) for r in range(-6, 8)]
                for i in range(8):
                    target(eight * 8 + i, group, short(window, taps, i))

    def prepare():
        for tile in range(TILES):
            for branch in range(3):
                base = (branch * TILES + tile) * 8
                tap_rows[base : base + TAPS, :] = short_taps[branch, :, lanes_of(tile)]
            for half in range(2):
                modes = slice(half * 8, half * 8 + 8)
                rate = mode_rates[modes, lanes_of(tile)]
                rate_rows[half, tile * 8 : tile * 8 + 8, :] = rate
                weight_rows[half, tile * 8 : tile * 8 + 8, :] = (
                    residues[modes, lanes_of(tile)] * jnp.sqrt(rate)
                )

        def keep_query(t, group, result):
            queries[t, at_group(group), :] = result

        def keep_key(t, group, result):
            mixed[t, at_group(group), :] = result

        wait_edge(0)
        spread(query_in, edges.at[0], first_block, rows)
        filtered(0, keep_query)
        wait_edge(1)
        spread(key_in, edges.at[1], first_block, rows)
        filtered(1, keep_key)

    def gather_value():
        for by in range(4):
            came = arrived.at[step(x, by)]
            copy(came, came, swap_send.at[by], swap_recv.at[by], {"ch": ch}).wait_recv()

        def block_rows(pair):
            for tile in range(TILES):
                quarter, columns = tile // 8, lanes_of(tile % 8)
                where = pl.ds(pl.multiple_of(pair * 16, 16), 16)
                block = total[0, quarter, where, columns] + arrived[quarter, where, columns]
                block = block.astype(jnp.bfloat16)
                if isinstance(pair, int):
                    last[:, lanes_of(tile)] = block[8:]
                block = block.astype(jnp.float32)
                base = pl.multiple_of((2 * pair + 1) * TILES * 8 + tile * 8, 8)
                rows[pl.ds(base, 8), :] = block[:8]
                rows[pl.ds(base + TILES * 8, 8), :] = block[8:]

        block_rows(ROWS // 16 - 1)
        send(last, edges.at[2], edge_send.at[2], edge_recv.at[2], block_device(1))
        pl.loop(0, ROWS // 16 - 1)(block_rows)

    def mix():
        def keep(t, group, result):
            product = mixed[t, at_group(group), :] * result
            mixed[t, at_group(group), :] = product.astype(jnp.bfloat16).astype(jnp.float32)

        filtered(2, keep, 1, ROWS // 8)

    def mix_first():
        def keep(t, group, result):
            product = mixed[t, at_group(group), :] * result
            mixed[t, at_group(group), :] = product.astype(jnp.bfloat16).astype(jnp.float32)

        wait_edge(2)
        spread_edge(edges.at[2], first_block, rows)
        filtered(2, keep, 0, 1)

    def decays(group):
        return [jnp.exp(-mode_of(rate_rows, n, group)) for n in range(MODES)]

    zeros = (jnp.zeros((8, LANES), jnp.float32),) * MODES

    def run_modes(group, rates, begin, end, held):
        def advance(eight, held):
            for i in range(8):
                entry = mixed[eight * 8 + i, at_group(group), :]
                held = tuple(rates[n] * held[n] + entry for n in range(MODES))
            return held

        return lax.fori_loop(begin, end, advance, held)

    def store_states(group, held):
        for n in range(MODES):
            states[group // 2, n // 8, pl.ds(group % 2 * 8 + n % 8, 8, stride=16), :] = held[n]

    def summarize(group):
        store_states(group, run_modes(group, decays(group), 1, ROWS // 8, zeros))

    def summarize_first(group):
        held = run_modes(group, decays(group), 0, 1, zeros)
        rest = [jnp.exp(-float(ROWS - 8) * mode_of(rate_rows, n, group)) for n in range(MODES)]
        store_states(
            group, [state_of(states, n, group) + rest[n] * held[n] for n in range(MODES)]
        )

    def localize(group):
        rates = decays(group)
        weighting = [mode_of(weight_rows, n, group) for n in range(MODES)]

        def advance(eight, held):
            for i in range(8):
                entry = mixed[eight * 8 + i, at_group(group), :]
                held = tuple(rates[n] * held[n] + entry for n in range(MODES))
                local[eight * 8 + i, at_group(group), :] = summed(
                    [weighting[n] * held[n] for n in range(MODES)]
                )
            return held

        lax.fori_loop(0, ROWS // 8, advance, zeros)

    def finish_group(group):
        rates = decays(group)
        skip = skip_gain[at_group(group), :]
        first = tuple(
            mode_of(weight_rows, n, group) * state_of(carried, n, group) for n in range(MODES)
        )

        def advance(eight, held):
            for i in range(8):
                held = tuple(rates[n] * held[n] for n in range(MODES))
                t = eight * 8 + i
                convolved = local[t, at_group(group), :] + summed(list(held))
                convolved = convolved.astype(jnp.bfloat16).astype(jnp.float32)
                result = queries[t, at_group(group), :] * (
                    convolved + skip * mixed[t, at_group(group), :]
                )
                out[pl.ds(eight * TILES * 8 + group * 64 + i, 8, stride=8), :] = result
            return held

        lax.fori_loop(0, ROWS // 8, advance, first)

    def near_part(at):
        return pl.ds(pl.multiple_of(at * 16, 16), 16)

    def near_rates(half):
        starts = [pl.multiple_of((2 * half + i) * 64 + near * 8, 8) for i in range(2)]
        return jnp.concatenate([rate_rows[:, pl.ds(start, 8), :] for start in starts], axis=1)

    def wait_all(buffer, sends, recvs, offsets, index):
        for by in offsets:
            came = buffer(index(by))
            copy(came, came, sends.at[by - 1], recvs.at[by - 1], {"ch": ch}).wait_recv()

    def send_near(half):
        for by in range(1, 8):
            to, device = near_device(by)
            send(
                states.at[half, :, near_part(to)],
                group_states.at[half, near],
                near_send.at[half, by - 1],
                near_recv.at[half, by - 1],
                device,
            )

    def send_across(buffer, slot, axis, half):
        own = buffer.at[half, place[axis]]
        for by in (2, 1, 3):
            send(
                own,
                own,
                scan_send.at[slot, half, by - 1],
                scan_recv.at[slot, half, by - 1],
                {axis: step(place[axis], by)},
            )

    def scan_across(buffer, slot, axis, half, decay):
        at = place[axis]
        wait_all(
            lambda i: buffer.at[half, i],
            scan_send.at[slot, half],
            scan_recv.at[slot, half],
            (1, 3, 2),
            lambda by: step(at, 4 - by),
        )
        running = jnp.zeros(decay.shape, jnp.float32)
        before = running
        for k in range(4):
            before = jnp.where(at == k, running, before)
            running = decay * running + buffer[half, k]
        return before, running

    def before_near(by):
        return lax.rem(near + 8 - by, 8)

    def scan_near(half):
        one = jnp.exp(-float(ROWS) * near_rates(half))
        group_states[half, near] = states[half, :, near_part(near), :]
        wait_all(
            lambda i: group_states.at[half, i],
            near_send.at[half],
            near_recv.at[half],
            range(1, 8),
            before_near,
        )
        held = jnp.zeros(one.shape, jnp.float32)
        for k in range(8):
            group_before[half, k] = held
            held = one * held + group_states[half, k]
        deep_states[half, zh] = held
        send_across(deep_states, 0, "zh", half)

    def scan_deep(half):
        decay = jnp.exp(-8.0 * ROWS * near_rates(half))
        before, running = scan_across(deep_states, 0, "zh", half, decay)
        wide_states[half, y] = running
        send_across(wide_states, 1, "y", half)
        return before

    def scan_wide(half, deep_before):
        rate = near_rates(half)
        one = jnp.exp(-float(ROWS) * rate)
        wide_before, _ = scan_across(wide_states, 1, "y", half, jnp.exp(-32.0 * ROWS * rate))
        shift = jnp.exp(rate * (-8.0 * ROWS * zh.astype(jnp.float32)))
        entering = deep_before + shift * wide_before
        for k in range(8):
            group_before[half, k] += entering
            entering = one * entering
        for by in range(1, 8):
            to, device = near_device(by)
            send(
                group_before.at[half, to],
                carried.at[half, :, near_part(near)],
                back_send.at[half, by - 1],
                back_recv.at[half, by - 1],
                device,
            )
        carried[half, :, near_part(near), :] = group_before[half, near]

    def wait_back(half):
        wait_all(
            lambda i: carried.at[half, :, near_part(i)],
            back_send.at[half],
            back_recv.at[half],
            range(1, 8),
            before_near,
        )

    FIRST, FORWARD, FINISH, NEAR, FAR = range(5)

    def both(rings, pair, action):
        for unit in (2 * pair, 2 * pair + 1):
            rings[unit][action]()

    own_copy.wait()
    settle(0)
    early[0][FIRST]()
    deep[0][FIRST]()
    open_late(0, 0)
    settle(1)
    early[1][FIRST]()
    deep[1][FIRST]()
    open_late(1, 0)
    for unit in (0, 1):
        early[unit][FORWARD]()
        open_late(unit, 1)
        open_late(unit, 3)
    deep[0][FORWARD]()
    both(early, 1, FIRST)
    for unit in (0, 1):
        early[unit][FINISH]()
        open_late(unit, 2)
    both(early, 1, FORWARD)
    deep[0][FINISH]()
    deep[1][FORWARD]()
    early[4][FIRST]()
    both(late, 0, FORWARD)
    both(early, 1, FINISH)
    deep[1][FINISH]()
    early[5][FIRST]()
    both(late, 1, FIRST)
    prepare()
    both(early, 2, FORWARD)
    both(early, 3, FIRST)
    copy(tokens, chip_tokens.at[1], token_sems.at[0], token_sems.at[1], {"core": core}).wait_recv()
    both(late, 0, FINISH)
    project(0)
    relay_far()
    both(late, 1, FORWARD)
    both(early, 2, FINISH)
    both(late, 2, FIRST)
    project_strip(0)
    both(early, 3, FORWARD)
    both(late, 1, FINISH)
    project(1)
    project(3)
    both(late, 2, FORWARD)
    both(early, 3, FINISH)
    both(late, 3, FIRST)
    join(0)
    expand(0, True)
    late[4][NEAR]()
    project_strip(1)
    project_strip(3)
    late[4][FAR]()
    project_strip(2)
    late[5][FINISH]()
    join(3)
    both(late, 3, FORWARD)
    late[6][FINISH]()
    expand(3, False)
    join(2)
    expand(2, False)
    join(1)
    close(1, 0)
    late[7][FAR]()
    close(1, 2)
    late[7][NEAR]()
    close(1, 1)
    close(1, 3)
    gather_value()
    mix()
    summarize(0)
    summarize(1)
    mix_first()
    summarize_first(0)
    summarize_first(1)
    send_near(0)
    summarize(2)
    summarize(3)
    summarize_first(2)
    summarize_first(3)
    send_near(1)
    localize(0)
    localize(1)
    scan_near(0)
    localize(2)
    scan_near(1)
    localize(3)
    deep_before = [scan_deep(0)]
    deep_before.append(scan_deep(1))
    scan_wide(0, deep_before[0])
    scan_wide(1, deep_before[1])
    wait_back(0)
    finish_group(0)
    finish_group(1)
    wait_back(1)
    finish_group(2)
    finish_group(3)
    for made in started:
        made.wait_send()


def per_device(
    tokens, query_in, key_in, proj_in, proj_out, short_taps, residues, mode_rates, skip_gain
):
    f32, bf16 = jnp.float32, jnp.bfloat16
    dma = pltpu.SemaphoreType.DMA
    tiles = pl.pallas_call(
        operator_kernel,
        out_shape=jax.ShapeDtypeStruct((ROWS * TILES, LANES), f32),
        in_specs=[pl.BlockSpec(memory_space=pltpu.VMEM)] * 9,
        out_specs=pl.BlockSpec(memory_space=pltpu.VMEM),
        scratch_shapes=[
            pltpu.VMEM((8, WIDE), bf16),
            pltpu.VMEM((2, ROWS, WIDE), bf16),
            pltpu.VMEM((2, 4, RANKS, QUARTER), bf16),
            pltpu.VMEM((2, 4, 4, 4, BLOCK, QUARTER), bf16),
            pltpu.VMEM((4, 4 * BLOCK, 2 * ROWS), f32),
            pltpu.VMEM((4, 4 * BLOCK, 2 * ROWS), f32),
            pltpu.VMEM((4, 4 * BLOCK, 2 * ROWS), bf16),
            pltpu.VMEM((2, 4, ROWS, QUARTER), f32),
            pltpu.VMEM((4, ROWS, QUARTER), f32),
            pltpu.VMEM((3, 8, WIDE), bf16),
            pltpu.VMEM(((ROWS + 8) * TILES, LANES), f32),
            pltpu.VMEM((3 * TILES * 8, LANES), f32),
            pltpu.VMEM((2, TILES * 8, LANES), f32),
            pltpu.VMEM((2, TILES * 8, LANES), f32),
            pltpu.VMEM((ROWS, TILES, LANES), f32),
            pltpu.VMEM((ROWS, TILES, LANES), f32),
            pltpu.VMEM((ROWS, TILES, LANES), f32),
            pltpu.VMEM((2, 2, TILES * 4, LANES), f32),
            pltpu.VMEM((2, 2, TILES * 4, LANES), f32),
            pltpu.VMEM((2, 8, 2, 16, LANES), f32),
            pltpu.VMEM((2, 8, 2, 16, LANES), f32),
            pltpu.VMEM((2, 4, 2, 16, LANES), f32),
            pltpu.VMEM((2, 4, 2, 16, LANES), f32),
            dma,
            dma((2,)),
            dma((2, 3)),
            dma((2, 3)),
            dma((2, 4)),
            dma((2, 4)),
            dma((8, 10)),
            dma((8, 10)),
            dma((2, 4, 2)),
            dma((2,)),
            dma((2,)),
            dma((8,)),
            dma((8,)),
            dma((4,)),
            dma((4,)),
            dma((3,)),
            dma((3,)),
            dma((2, 7)),
            dma((2, 7)),
            dma((2, 2, 3)),
            dma((2, 2, 3)),
            dma((2, 7)),
            dma((2, 7)),
        ],
        compiler_params=pltpu.CompilerParams(
            collective_id=0, has_side_effects=True, vmem_limit_bytes=60 * 2**20
        ),
    )(
        tokens,
        proj_in.T,
        proj_out,
        query_in,
        key_in,
        short_taps,
        residues,
        mode_rates,
        skip_gain.reshape(TILES, LANES),
    )
    tiles = tiles.reshape(ROWS // 8, TILES, 8, LANES).transpose(0, 2, 1, 3)
    return tiles.reshape(ROWS, WIDE).astype(bf16)


def solution(mesh):
    split = Mesh(mesh.devices.reshape(4, 4, 4, 2, 2), ("y", "zh", "x", "core", "ch"))
    both = P(SEQ_AXES, "ch")
    placed = (
        both,
        both,
        both,
        P("ch", SEQ_AXES),
        both,
        P(None, None, "ch"),
        P(None, "ch"),
        P(None, "ch"),
        P("ch"),
    )
    return jax.shard_map(
        per_device, mesh=split, in_specs=placed, out_specs=both, check_vma=False
    )
```

```python
import jax
import jax.numpy as jnp
from jax import lax
from jax.experimental import pallas as pl
from jax.experimental.pallas import tpu as pltpu
from jax.sharding import Mesh
from jax.sharding import PartitionSpec as P

ROWS = 128
WIDE = 4096
LANES = 128
TILES = WIDE // LANES
GROUPS = TILES // 8
MODES = 16
TAPS = 7
SEQ_AXES = ("y", "zh", "x", "core")
MESH = pl.DeviceIdType.MESH
BLOCK = 48
QUARTER = 1024
RANKS = 12
UNITS = ((0, 0), (1, 0), (0, 1), (0, 3), (0, 2), (1, 2), (1, 3), (1, 1))


def lanes_of(tile):
    return slice(tile * LANES, (tile + 1) * LANES)


def spread_edge(edge, first_block, scratch):
    for tile in range(TILES):
        above = edge[:, lanes_of(tile)].astype(jnp.float32)
        scratch[tile * 8 : tile * 8 + 8, :] = jnp.where(first_block, 0.0, above)


def spread(source, edge, first_block, scratch):
    spread_edge(edge, first_block, scratch)

    @pl.loop(0, ROWS // 16)
    def _(pair):
        for tile in range(TILES):
            rows = pl.ds(pl.multiple_of(pair * 16, 16), 16)
            block = source[rows, lanes_of(tile)].astype(jnp.float32)
            base = pl.multiple_of((2 * pair + 1) * TILES * 8 + tile * 8, 8)
            scratch[pl.ds(base, 8), :] = block[:8]
            scratch[pl.ds(base + TILES * 8, 8), :] = block[8:]


def row_of(scratch, eight, group, row):
    start = (eight + (1 if row >= 0 else 0)) * TILES * 8 + group * 64 + row % 8
    return scratch[pl.ds(start, 8, stride=8), :]


def short(rows, taps, step):
    result = taps[0] * rows[step + 6]
    for offset in range(1, TAPS):
        result = result + taps[offset] * rows[step + 6 - offset]
    return result


def summed(terms):
    while len(terms) > 1:
        terms = [terms[i] + terms[i + 1] for i in range(0, len(terms), 2)]
    return terms[0]


def operator_kernel(
    tokens,
    pad_in,
    pad_out,
    query_in,
    key_in,
    short_taps,
    residues,
    mode_rates,
    skip_gain,
    out,
    last,
    value_edges,
    chip_tokens,
    stage,
    weights,
    partial,
    theirs,
    low,
    total,
    arrived,
    edges,
    rows,
    tap_rows,
    rate_rows,
    weight_rows,
    queries,
    mixed,
    local,
    states,
    carried,
    group_states,
    group_before,
    deep_states,
    wide_states,
    own_sem,
    token_sems,
    stage_send,
    stage_recv,
    deep_send,
    deep_recv,
    ring_send,
    ring_recv,
    piece_send,
    far_send,
    far_recv,
    part_send,
    part_recv,
    swap_send,
    swap_recv,
    edge_send,
    edge_recv,
    late_send,
    late_recv,
    near_send,
    near_recv,
    scan_send,
    scan_recv,
    back_send,
    back_recv,
):
    y, zh, x = lax.axis_index("y"), lax.axis_index("zh"), lax.axis_index("x")
    core, ch = lax.axis_index("core"), lax.axis_index("ch")
    place = {"x": x, "y": y, "zh": zh}
    pads = (pad_in, pad_out)
    started = []
    near = x * 2 + core
    block_at = (y * 4 + zh) * 8 + near
    first_block = block_at == 0

    def step(position, by):
        return lax.rem(position + by, 4)

    def copy(source, target, send, recv, device):
        return pltpu.make_async_remote_copy(
            src_ref=source,
            dst_ref=target,
            send_sem=send,
            recv_sem=recv,
            device_id=device,
            device_id_type=MESH,
        )

    def send(*arguments):
        made = copy(*arguments)
        made.start()
        started.append(made)

    def near_device(by):
        to = lax.rem(near + by, 8)
        return to, {"x": to // 2, "core": lax.rem(to, 2)}

    def block_device(by):
        to = lax.rem(block_at + by, 128)
        return {
            "y": to // 32,
            "zh": lax.rem(to // 8, 4),
            "x": lax.rem(to // 2, 4),
            "core": lax.rem(to, 2),
        }

    def send_edge(i, source):
        send(
            source.at[pl.ds(ROWS - 8, 8)],
            edges.at[i],
            edge_send.at[i],
            edge_recv.at[i],
            block_device(1),
        )

    def wait_edge(i):
        edge = edges.at[i]
        copy(edge, edge, edge_send.at[i], edge_recv.at[i], {"ch": ch}).wait_recv()

    barrier = pltpu.get_barrier_semaphore()
    greeted = [{"ch": 1 - ch}, block_device(1), block_device(127)]
    greeted += [near_device(by)[1] for by in range(1, 8)]
    greeted += [{axis: step(place[axis], by)} for axis in ("zh", "y") for by in (1, 2, 3)]
    for device in greeted:
        pl.semaphore_signal(barrier, inc=1, device_id=device, device_id_type=MESH)
    own_copy = pltpu.make_async_copy(tokens, chip_tokens.at[0], own_sem)
    own_copy.start()
    pl.semaphore_wait(barrier, len(greeted))

    for f in range(2):
        for by in (1, 3, 2):
            to = step(x, by)
            columns = pl.ds(pl.multiple_of(to * QUARTER, QUARTER), QUARTER)
            send(
                pads[f].at[:, columns],
                stage.at[f, x],
                stage_send.at[f, by - 1],
                stage_recv.at[f, by - 1],
                {"x": to},
            )
    send(tokens, chip_tokens.at[1], token_sems.at[0], token_sems.at[1], {"core": 1 - core})
    for i, source in enumerate((query_in, key_in)):
        send_edge(i, source)

    def settle(f):
        columns = pl.ds(pl.multiple_of(x * QUARTER, QUARTER), QUARTER)
        own = pltpu.make_async_copy(pads[f].at[:, columns], stage.at[f, x], own_sem)
        own.start()
        own.wait()
        for by in (1, 3, 2):
            came = stage.at[f, step(x, 4 - by)]
            copy(came, came, stage_send.at[f, by - 1], stage_recv.at[f, by - 1], {"x": x}).wait_recv()
        parts = [stage[f, i].astype(jnp.float32) for i in range(4)]
        weights[f, y, zh, x] = jnp.concatenate(parts, axis=0).astype(jnp.bfloat16)

    def ring(axis, item, send_sems, recv_sems, split=False, relayed=None):
        at = place[axis]
        plus, minus, far = step(at, 1), step(at, 3), step(at, 2)

        def out(ref, slot, to):
            send(ref, ref, send_sems(slot), recv_sems(slot), {axis: to})

        def landed(ref, slot):
            copy(ref, ref, send_sems(slot), recv_sems(slot), {axis: at}).wait_recv()

        def first():
            if split:
                out(item(at, 0), 0, plus)
                out(item(at, 1), 1, minus)
                out(item(at, 1), 4, plus)
                out(item(at, 0), 5, minus)
            else:
                out(item(at), 0, plus)
                out(item(at), 1, minus)

        def forward():
            landed(item(minus, 0 if split else None), 0)
            if relayed is None:
                out(item(minus, 0), 2, plus)
            landed(item(plus, 1 if split else None), 1)
            if relayed is None:
                out(item(plus, 1), 3, minus)

        def finish_near():
            if split:
                landed(item(minus, 1), 4)
                landed(item(plus, 0), 5)

        def finish_far():
            if relayed is None:
                landed(item(far, 0), 2)
                landed(item(far, 1), 3)
            else:
                came = item(far)
                copy(came, came, far_send.at[relayed], far_recv.at[relayed], {axis: at}).wait_recv()

        def finish():
            finish_near()
            finish_far()

        return first, forward, finish, finish_near, finish_far

    def half_columns(half):
        return slice(None) if half is None else slice(half * 512, half * 512 + 512)

    def half_blocks(half):
        return slice(None) if half is None else slice(half * 2, half * 2 + 2)

    def deep_ring(f):
        return ring(
            "zh",
            lambda i, half=None: weights.at[f, y, i, x, :, half_columns(half)],
            lambda slot: deep_send.at[f, slot],
            lambda slot: deep_recv.at[f, slot],
        )

    def unit_ring(unit, late):
        f, r = UNITS[unit]
        deep = step(zh, r)
        across = unit % 2 == 0

        def item(i, half=None):
            if late:
                if across:
                    return weights.at[f, i, deep, half_blocks(half)]
                return weights.at[f, half_blocks(half), deep, i]
            if across:
                return weights.at[f, y, deep, i, :, half_columns(half)]
            return weights.at[f, i, deep, x, :, half_columns(half)]

        base = 4 if late else 0
        return ring(
            "x" if across != late else "y",
            item,
            lambda slot: ring_send.at[unit, base + slot],
            lambda slot: ring_recv.at[unit, base + slot],
            late and unit >= 2,
            {7: 0, 6: 1}.get(unit) if late else None,
        )

    def relay_far():
        column = weights.at[1, :, zh, step(x, 2)]
        send(column, column, far_send.at[0], far_recv.at[0], {"zh": step(zh, 3)})
        strip = weights.at[1, step(y, 2), zh]
        send(strip, strip, far_send.at[1], far_recv.at[1], {"zh": step(zh, 1)})

    def open_late(unit, by):
        deep = zh
        if unit == 0:
            axis, piece = "y", weights.at[0, y, deep, step(x, by)]
        else:
            axis, piece = "x", weights.at[1, step(y, by), deep, x]
        for slot, to in ((0, 1), (1, 3)):
            send(
                piece,
                piece,
                piece_send.at[unit, by, slot],
                ring_recv.at[unit, 4 + slot],
                {axis: step(place[axis], to)},
            )

    deep = [deep_ring(f) for f in range(2)]
    early = [unit_ring(unit, False) for unit in range(8)]
    late = [unit_ring(unit, True) for unit in range(8)]

    def unit_weights(f, r, quarter):
        return weights[f, :, step(zh, r), quarter].reshape(4 * BLOCK, QUARTER)

    def quarter_dot(rows_in, quarter):
        columns = pl.ds(pl.multiple_of(quarter * QUARTER, QUARTER), QUARTER)
        return lax.dot_general(
            rows_in,
            chip_tokens[:, :, columns].reshape(2 * ROWS, QUARTER),
            (((1,), (1,)), ((), ())),
            preferred_element_type=jnp.float32,
        )

    def send_part(ref, other, i):
        send(ref, other, part_send.at[i], part_recv.at[i], {"ch": 1 - ch})

    def project(r):
        @pl.loop(0, 4)
        def _(quarter):
            part = quarter_dot(unit_weights(0, r, quarter), quarter)

            @pl.when(quarter == 0)
            def _():
                partial[r] = part

            @pl.when(quarter > 0)
            def _():
                partial[r] += part

        send_part(partial.at[r], theirs.at[r], r)

    def strip_of(by):
        return pl.ds(pl.multiple_of(step(y, by) * BLOCK, BLOCK), BLOCK)

    def project_strip(by):
        strip = strip_of(by)
        partial[2, strip, :] = summed(
            [quarter_dot(weights[0, step(y, by), step(zh, 2), q], q) for q in range(4)]
        )
        send_part(partial.at[2, strip], theirs.at[2, strip], 4 + by)

    def join(r):
        for by in range(4) if r == 2 else (None,):
            i = r if by is None else 4 + by
            came = theirs.at[r] if by is None else theirs.at[r, strip_of(by)]
            copy(came, came, part_send.at[i], part_recv.at[i], {"ch": ch}).wait_recv()
        low[r] = (partial[r] + theirs[r]).astype(jnp.bfloat16)

    def product(r, quarter):
        return lax.dot_general(
            low[r],
            unit_weights(1, r, quarter),
            (((0,), (0,)), ((), ())),
            preferred_element_type=jnp.float32,
        ).reshape(2, ROWS, QUARTER)

    def expand(r, opening):
        for quarter in range(4):
            if opening:
                total[:, quarter] = product(r, quarter)
            else:
                total[:, quarter] += product(r, quarter)

    def close(r, by):
        quarter = step(x, by)
        total[:, quarter] += product(r, quarter)
        send(
            total.at[1, quarter],
            arrived.at[quarter],
            swap_send.at[by],
            swap_recv.at[by],
            {"core": 1 - core},
        )

    def tap_of(branch, offset, group):
        start = (branch * TILES + group * 8) * 8 + offset
        return tap_rows[pl.ds(start, 8, stride=8), :]

    def mode_of(ref, n, group):
        half, row = n // 8, n % 8
        return ref[half, pl.ds(group * 64 + row, 8, stride=8), :]

    def state_of(ref, n, group):
        return ref[group // 2, n // 8, pl.ds(group % 2 * 8 + n % 8, 8, stride=16), :]

    def at_group(group):
        return pl.ds(group * 8 if isinstance(group, int) else pl.multiple_of(group * 8, 8), 8)

    def filtered(branch, target, begin=0, end=ROWS // 8, groups=range(GROUPS)):
        for group in groups:
            taps = [tap_of(branch, j, group) for j in range(TAPS)]

            @pl.loop(begin, end)
            def _(eight):
                window = [row_of(rows, eight, group, r) for r in range(-6, 8)]
                for i in range(8):
                    target(eight * 8 + i, group, short(window, taps, i))

    def prepare():
        for tile in range(TILES):
            for branch in range(3):
                base = (branch * TILES + tile) * 8
                tap_rows[base : base + TAPS, :] = short_taps[branch, :, lanes_of(tile)]
            for half in range(2):
                modes = slice(half * 8, half * 8 + 8)
                rate = mode_rates[modes, lanes_of(tile)]
                rate_rows[half, tile * 8 : tile * 8 + 8, :] = rate
                weight_rows[half, tile * 8 : tile * 8 + 8, :] = (
                    residues[modes, lanes_of(tile)] * jnp.sqrt(rate)
                )

        def keep_query(t, group, result):
            queries[t, at_group(group), :] = result

        def keep_key(t, group, result):
            mixed[t, at_group(group), :] = result

        wait_edge(0)
        spread(query_in, edges.at[0], first_block, rows)
        filtered(0, keep_query)
        wait_edge(1)
        spread(key_in, edges.at[1], first_block, rows)
        filtered(1, keep_key)

    def gather_rows(pair, quarter, edge):
        where = pl.ds(pl.multiple_of(pair * 16, 16), 16)
        for tile in range(8):
            columns = lanes_of(tile)
            block = total[0, quarter, where, columns] + arrived[quarter, where, columns]
            block = block.astype(jnp.bfloat16)
            if edge:
                last[quarter, :, columns] = block[8:]
            block = block.astype(jnp.float32)
            base = pl.multiple_of((2 * pair + 1) * TILES * 8 + quarter * 64 + tile * 8, 8)
            rows[pl.ds(base, 8), :] = block[:8]
            rows[pl.ds(base + TILES * 8, 8), :] = block[8:]

    def gather_edge(by):
        quarter = step(x, by)
        came = arrived.at[quarter]
        copy(came, came, swap_send.at[by], swap_recv.at[by], {"ch": ch}).wait_recv()
        gather_rows(ROWS // 16 - 1, quarter, True)
        send(
            last.at[quarter],
            value_edges.at[quarter],
            late_send.at[by],
            late_recv.at[by],
            block_device(1),
        )

    def keep_product(t, group, result):
        product = mixed[t, at_group(group), :] * result
        mixed[t, at_group(group), :] = product.astype(jnp.bfloat16).astype(jnp.float32)

    def start_mix(by):
        group = step(x, by)
        pl.loop(0, ROWS // 16 - 1)(lambda pair: gather_rows(pair, group, False))
        filtered(2, keep_product, 1, ROWS // 8, (group,))
        summarize(group)

    def mix_first():
        from_x = block_device(127)["x"]
        for by in range(4):
            came = value_edges.at[step(from_x, by)]
            copy(came, came, late_send.at[by], late_recv.at[by], {"ch": ch}).wait_recv()
        for tile in range(TILES):
            above = value_edges[tile // 8, :, lanes_of(tile % 8)].astype(jnp.float32)
            rows[tile * 8 : tile * 8 + 8, :] = jnp.where(first_block, 0.0, above)
        filtered(2, keep_product, 0, 1)

    def decays(group):
        return [jnp.exp(-mode_of(rate_rows, n, group)) for n in range(MODES)]

    zeros = (jnp.zeros((8, LANES), jnp.float32),) * MODES

    def run_modes(group, rates, begin, end, held):
        def advance(eight, held):
            for i in range(8):
                entry = mixed[eight * 8 + i, at_group(group), :]
                held = tuple(rates[n] * held[n] + entry for n in range(MODES))
            return held

        return lax.fori_loop(begin, end, advance, held)

    def store_states(group, held):
        for n in range(MODES):
            half, part = lax.div(group, 2), lax.rem(group, 2)
            states[half, n // 8, pl.ds(part * 8 + n % 8, 8, stride=16), :] = held[n]

    def summarize(group):
        store_states(group, run_modes(group, decays(group), 1, ROWS // 8, zeros))

    def summarize_first(group):
        held = run_modes(group, decays(group), 0, 1, zeros)
        rest = [jnp.exp(-float(ROWS - 8) * mode_of(rate_rows, n, group)) for n in range(MODES)]
        store_states(
            group, [state_of(states, n, group) + rest[n] * held[n] for n in range(MODES)]
        )

    def localize(group):
        rates = decays(group)
        weighting = [mode_of(weight_rows, n, group) for n in range(MODES)]

        def advance(eight, held):
            for i in range(8):
                entry = mixed[eight * 8 + i, at_group(group), :]
                held = tuple(rates[n] * held[n] + entry for n in range(MODES))
                local[eight * 8 + i, at_group(group), :] = summed(
                    [weighting[n] * held[n] for n in range(MODES)]
                )
            return held

        lax.fori_loop(0, ROWS // 8, advance, zeros)

    def finish_group(group):
        rates = decays(group)
        skip = skip_gain[at_group(group), :]
        first = tuple(
            mode_of(weight_rows, n, group) * state_of(carried, n, group) for n in range(MODES)
        )

        def advance(eight, held):
            for i in range(8):
                held = tuple(rates[n] * held[n] for n in range(MODES))
                t = eight * 8 + i
                convolved = local[t, at_group(group), :] + summed(list(held))
                convolved = convolved.astype(jnp.bfloat16).astype(jnp.float32)
                result = queries[t, at_group(group), :] * (
                    convolved + skip * mixed[t, at_group(group), :]
                )
                out[pl.ds(eight * TILES * 8 + group * 64 + i, 8, stride=8), :] = result
            return held

        lax.fori_loop(0, ROWS // 8, advance, first)

    def near_part(at):
        return pl.ds(pl.multiple_of(at * 16, 16), 16)

    def near_rates(half):
        starts = [pl.multiple_of((2 * half + i) * 64 + near * 8, 8) for i in range(2)]
        return jnp.concatenate([rate_rows[:, pl.ds(start, 8), :] for start in starts], axis=1)

    def wait_all(buffer, sends, recvs, offsets, index):
        for by in offsets:
            came = buffer(index(by))
            copy(came, came, sends.at[by - 1], recvs.at[by - 1], {"ch": ch}).wait_recv()

    def send_near(half):
        for by in range(1, 8):
            to, device = near_device(by)
            send(
                states.at[half, :, near_part(to)],
                group_states.at[half, near],
                near_send.at[half, by - 1],
                near_recv.at[half, by - 1],
                device,
            )

    def send_across(buffer, slot, axis, half):
        own = buffer.at[half, place[axis]]
        for by in (2, 1, 3):
            send(
                own,
                own,
                scan_send.at[slot, half, by - 1],
                scan_recv.at[slot, half, by - 1],
                {axis: step(place[axis], by)},
            )

    def scan_across(buffer, slot, axis, half, decay):
        at = place[axis]
        wait_all(
            lambda i: buffer.at[half, i],
            scan_send.at[slot, half],
            scan_recv.at[slot, half],
            (1, 3, 2),
            lambda by: step(at, 4 - by),
        )
        running = jnp.zeros(decay.shape, jnp.float32)
        before = running
        for k in range(4):
            before = jnp.where(at == k, running, before)
            running = decay * running + buffer[half, k]
        return before, running

    def before_near(by):
        return lax.rem(near + 8 - by, 8)

    def scan_near(half):
        one = jnp.exp(-float(ROWS) * near_rates(half))
        group_states[half, near] = states[half, :, near_part(near), :]
        wait_all(
            lambda i: group_states.at[half, i],
            near_send.at[half],
            near_recv.at[half],
            range(1, 8),
            before_near,
        )
        held = jnp.zeros(one.shape, jnp.float32)
        for k in range(8):
            group_before[half, k] = held
            held = one * held + group_states[half, k]
        deep_states[half, zh] = held
        send_across(deep_states, 0, "zh", half)

    def scan_deep(half):
        decay = jnp.exp(-8.0 * ROWS * near_rates(half))
        before, running = scan_across(deep_states, 0, "zh", half, decay)
        wide_states[half, y] = running
        send_across(wide_states, 1, "y", half)
        return before

    def scan_wide(half, deep_before):
        rate = near_rates(half)
        one = jnp.exp(-float(ROWS) * rate)
        wide_before, _ = scan_across(wide_states, 1, "y", half, jnp.exp(-32.0 * ROWS * rate))
        shift = jnp.exp(rate * (-8.0 * ROWS * zh.astype(jnp.float32)))
        entering = deep_before + shift * wide_before
        for k in range(8):
            group_before[half, k] += entering
            entering = one * entering
        for by in range(1, 8):
            to, device = near_device(by)
            send(
                group_before.at[half, to],
                carried.at[half, :, near_part(near)],
                back_send.at[half, by - 1],
                back_recv.at[half, by - 1],
                device,
            )
        carried[half, :, near_part(near), :] = group_before[half, near]

    def wait_back(half):
        wait_all(
            lambda i: carried.at[half, :, near_part(i)],
            back_send.at[half],
            back_recv.at[half],
            range(1, 8),
            before_near,
        )

    FIRST, FORWARD, FINISH, NEAR, FAR = range(5)

    def both(rings, pair, action):
        for unit in (2 * pair, 2 * pair + 1):
            rings[unit][action]()

    own_copy.wait()
    settle(0)
    early[0][FIRST]()
    deep[0][FIRST]()
    open_late(0, 0)
    settle(1)
    early[1][FIRST]()
    deep[1][FIRST]()
    open_late(1, 0)
    for unit in (0, 1):
        early[unit][FORWARD]()
        open_late(unit, 1)
        open_late(unit, 3)
    deep[0][FORWARD]()
    both(early, 1, FIRST)
    for unit in (0, 1):
        early[unit][FINISH]()
        open_late(unit, 2)
    both(early, 1, FORWARD)
    deep[0][FINISH]()
    deep[1][FORWARD]()
    early[4][FIRST]()
    both(late, 0, FORWARD)
    both(early, 1, FINISH)
    deep[1][FINISH]()
    early[5][FIRST]()
    both(late, 1, FIRST)
    prepare()
    both(early, 2, FORWARD)
    both(early, 3, FIRST)
    copy(tokens, chip_tokens.at[1], token_sems.at[0], token_sems.at[1], {"core": core}).wait_recv()
    both(late, 0, FINISH)
    project(0)
    relay_far()
    both(late, 1, FORWARD)
    both(early, 2, FINISH)
    both(late, 2, FIRST)
    project_strip(0)
    both(early, 3, FORWARD)
    both(late, 1, FINISH)
    project(1)
    project(3)
    both(late, 2, FORWARD)
    both(early, 3, FINISH)
    both(late, 3, FIRST)
    join(0)
    expand(0, True)
    late[4][NEAR]()
    project_strip(1)
    project_strip(3)
    late[4][FAR]()
    project_strip(2)
    late[5][FINISH]()
    join(3)
    both(late, 3, FORWARD)
    join(2)
    expand(2, False)
    join(1)
    late[6][FINISH]()
    expand(3, False)
    close(1, 0)
    late[7][FAR]()
    close(1, 2)
    late[7][NEAR]()
    close(1, 1)
    close(1, 3)
    gather_edge(0)
    gather_edge(2)
    start_mix(0)
    gather_edge(1)
    gather_edge(3)
    start_mix(2)
    start_mix(1)
    start_mix(3)
    mix_first()
    summarize_first(0)
    summarize_first(1)
    send_near(0)
    summarize_first(2)
    summarize_first(3)
    send_near(1)
    localize(0)
    localize(1)
    scan_near(0)
    localize(2)
    scan_near(1)
    localize(3)
    deep_before = [scan_deep(0)]
    deep_before.append(scan_deep(1))
    scan_wide(0, deep_before[0])
    scan_wide(1, deep_before[1])
    wait_back(0)
    finish_group(0)
    finish_group(1)
    wait_back(1)
    finish_group(2)
    finish_group(3)
    for made in started:
        made.wait_send()


def per_device(
    tokens, query_in, key_in, proj_in, proj_out, short_taps, residues, mode_rates, skip_gain
):
    f32, bf16 = jnp.float32, jnp.bfloat16
    dma = pltpu.SemaphoreType.DMA
    tiles = pl.pallas_call(
        operator_kernel,
        out_shape=jax.ShapeDtypeStruct((ROWS * TILES, LANES), f32),
        in_specs=[pl.BlockSpec(memory_space=pltpu.VMEM)] * 9,
        out_specs=pl.BlockSpec(memory_space=pltpu.VMEM),
        scratch_shapes=[
            pltpu.VMEM((4, 8, QUARTER), bf16),
            pltpu.VMEM((4, 8, QUARTER), bf16),
            pltpu.VMEM((2, ROWS, WIDE), bf16),
            pltpu.VMEM((2, 4, RANKS, QUARTER), bf16),
            pltpu.VMEM((2, 4, 4, 4, BLOCK, QUARTER), bf16),
            pltpu.VMEM((4, 4 * BLOCK, 2 * ROWS), f32),
            pltpu.VMEM((4, 4 * BLOCK, 2 * ROWS), f32),
            pltpu.VMEM((4, 4 * BLOCK, 2 * ROWS), bf16),
            pltpu.VMEM((2, 4, ROWS, QUARTER), f32),
            pltpu.VMEM((4, ROWS, QUARTER), f32),
            pltpu.VMEM((2, 8, WIDE), bf16),
            pltpu.VMEM(((ROWS + 8) * TILES, LANES), f32),
            pltpu.VMEM((3 * TILES * 8, LANES), f32),
            pltpu.VMEM((2, TILES * 8, LANES), f32),
            pltpu.VMEM((2, TILES * 8, LANES), f32),
            pltpu.VMEM((ROWS, TILES, LANES), f32),
            pltpu.VMEM((ROWS, TILES, LANES), f32),
            pltpu.VMEM((ROWS, TILES, LANES), f32),
            pltpu.VMEM((2, 2, TILES * 4, LANES), f32),
            pltpu.VMEM((2, 2, TILES * 4, LANES), f32),
            pltpu.VMEM((2, 8, 2, 16, LANES), f32),
            pltpu.VMEM((2, 8, 2, 16, LANES), f32),
            pltpu.VMEM((2, 4, 2, 16, LANES), f32),
            pltpu.VMEM((2, 4, 2, 16, LANES), f32),
            dma,
            dma((2,)),
            dma((2, 3)),
            dma((2, 3)),
            dma((2, 4)),
            dma((2, 4)),
            dma((8, 10)),
            dma((8, 10)),
            dma((2, 4, 2)),
            dma((2,)),
            dma((2,)),
            dma((8,)),
            dma((8,)),
            dma((4,)),
            dma((4,)),
            dma((2,)),
            dma((2,)),
            dma((4,)),
            dma((4,)),
            dma((2, 7)),
            dma((2, 7)),
            dma((2, 2, 3)),
            dma((2, 2, 3)),
            dma((2, 7)),
            dma((2, 7)),
        ],
        compiler_params=pltpu.CompilerParams(
            collective_id=0, has_side_effects=True, vmem_limit_bytes=60 * 2**20
        ),
    )(
        tokens,
        proj_in.T,
        proj_out,
        query_in,
        key_in,
        short_taps,
        residues,
        mode_rates,
        skip_gain.reshape(TILES, LANES),
    )
    tiles = tiles.reshape(ROWS // 8, TILES, 8, LANES).transpose(0, 2, 1, 3)
    return tiles.reshape(ROWS, WIDE).astype(bf16)


def solution(mesh):
    split = Mesh(mesh.devices.reshape(4, 4, 4, 2, 2), ("y", "zh", "x", "core", "ch"))
    both = P(SEQ_AXES, "ch")
    placed = (
        both,
        both,
        both,
        P("ch", SEQ_AXES),
        both,
        P(None, None, "ch"),
        P(None, "ch"),
        P(None, "ch"),
        P("ch"),
    )
    return jax.shard_map(
        per_device, mesh=split, in_specs=placed, out_specs=both, check_vma=False
    )
```

```python
import jax
import jax.numpy as jnp
from jax import lax
from jax.experimental import pallas as pl
from jax.experimental.pallas import tpu as pltpu
from jax.sharding import Mesh
from jax.sharding import PartitionSpec as P

ROWS = 128
WIDE = 4096
LANES = 128
TILES = WIDE // LANES
GROUPS = TILES // 8
MODES = 16
TAPS = 7
SEQ_AXES = ("y", "zh", "x", "core")
MESH = pl.DeviceIdType.MESH
BLOCK = 48
QUARTER = 1024
RANKS = 12
UNITS = ((0, 0), (1, 0), (0, 1), (0, 3), (0, 2), (1, 2), (1, 3), (1, 1))


def lanes_of(tile):
    return slice(tile * LANES, (tile + 1) * LANES)


def spread_edge(edge, first_block, scratch):
    for tile in range(TILES):
        above = edge[:, lanes_of(tile)].astype(jnp.float32)
        scratch[tile * 8 : tile * 8 + 8, :] = jnp.where(first_block, 0.0, above)


def spread(source, edge, first_block, scratch):
    spread_edge(edge, first_block, scratch)

    @pl.loop(0, ROWS // 16)
    def _(pair):
        for tile in range(TILES):
            rows = pl.ds(pl.multiple_of(pair * 16, 16), 16)
            block = source[rows, lanes_of(tile)].astype(jnp.float32)
            base = pl.multiple_of((2 * pair + 1) * TILES * 8 + tile * 8, 8)
            scratch[pl.ds(base, 8), :] = block[:8]
            scratch[pl.ds(base + TILES * 8, 8), :] = block[8:]


def row_of(scratch, eight, group, row):
    start = (eight + (1 if row >= 0 else 0)) * TILES * 8 + group * 64 + row % 8
    return scratch[pl.ds(start, 8, stride=8), :]


def short(rows, taps, step):
    result = taps[0] * rows[step + 6]
    for offset in range(1, TAPS):
        result = result + taps[offset] * rows[step + 6 - offset]
    return result


def summed(terms):
    while len(terms) > 1:
        terms = [terms[i] + terms[i + 1] for i in range(0, len(terms), 2)]
    return terms[0]


def operator_kernel(
    tokens,
    pad_in,
    pad_out,
    query_far,
    key_far,
    taps_far,
    residues_far,
    rates_far,
    skip_far,
    out,
    query_in,
    key_in,
    short_taps,
    residues,
    mode_rates,
    skip_gain,
    last,
    value_edges,
    chip_tokens,
    stage,
    weights,
    partial,
    theirs,
    low,
    total,
    arrived,
    edges,
    rows,
    tap_rows,
    rate_rows,
    weight_rows,
    queries,
    mixed,
    local,
    states,
    carried,
    group_states,
    group_before,
    deep_states,
    wide_states,
    own_sem,
    load_sems,
    token_sems,
    stage_send,
    stage_recv,
    deep_send,
    deep_recv,
    ring_send,
    ring_recv,
    piece_send,
    far_send,
    far_recv,
    part_send,
    part_recv,
    swap_send,
    swap_recv,
    edge_send,
    edge_recv,
    late_send,
    late_recv,
    near_send,
    near_recv,
    scan_send,
    scan_recv,
    back_send,
    back_recv,
):
    y, zh, x = lax.axis_index("y"), lax.axis_index("zh"), lax.axis_index("x")
    core, ch = lax.axis_index("core"), lax.axis_index("ch")
    place = {"x": x, "y": y, "zh": zh}
    pads = (pad_in, pad_out)
    started = []
    near = x * 2 + core
    block_at = (y * 4 + zh) * 8 + near
    first_block = block_at == 0

    def step(position, by):
        return lax.rem(position + by, 4)

    def copy(source, target, send, recv, device):
        return pltpu.make_async_remote_copy(
            src_ref=source,
            dst_ref=target,
            send_sem=send,
            recv_sem=recv,
            device_id=device,
            device_id_type=MESH,
        )

    def send(*arguments):
        made = copy(*arguments)
        made.start()
        started.append(made)

    def near_device(by):
        to = lax.rem(near + by, 8)
        return to, {"x": to // 2, "core": lax.rem(to, 2)}

    def block_device(by):
        to = lax.rem(block_at + by, 128)
        return {
            "y": to // 32,
            "zh": lax.rem(to // 8, 4),
            "x": lax.rem(to // 2, 4),
            "core": lax.rem(to, 2),
        }

    def send_edge(i, source):
        send(
            source.at[pl.ds(ROWS - 8, 8)],
            edges.at[i],
            edge_send.at[i],
            edge_recv.at[i],
            block_device(1),
        )

    def wait_edge(i):
        edge = edges.at[i]
        copy(edge, edge, edge_send.at[i], edge_recv.at[i], {"ch": ch}).wait_recv()

    own_copy = pltpu.make_async_copy(tokens, chip_tokens.at[0], own_sem)
    own_copy.start()
    loads = [
        pltpu.make_async_copy(source, target, load_sems.at[i])
        for i, (source, target) in enumerate(
            (
                (query_far, query_in),
                (key_far, key_in),
                (taps_far, short_taps),
                (residues_far, residues),
                (rates_far, mode_rates),
                (skip_far, skip_gain),
            )
        )
    ]
    for load in loads:
        load.start()
    barrier = pltpu.get_barrier_semaphore()
    greeted = [{"ch": 1 - ch}, block_device(1), block_device(127)]
    greeted += [near_device(by)[1] for by in range(1, 8)]
    greeted += [{axis: step(place[axis], by)} for axis in ("zh", "y") for by in (1, 2, 3)]
    for device in greeted:
        pl.semaphore_signal(barrier, inc=1, device_id=device, device_id_type=MESH)
    pl.semaphore_wait(barrier, len(greeted))

    for f in range(2):
        for by in (1, 3, 2):
            to = step(x, by)
            columns = pl.ds(pl.multiple_of(to * QUARTER, QUARTER), QUARTER)
            send(
                pads[f].at[:, columns],
                stage.at[f, x],
                stage_send.at[f, by - 1],
                stage_recv.at[f, by - 1],
                {"x": to},
            )
    own_copy.wait()
    send(
        chip_tokens.at[0],
        chip_tokens.at[1],
        token_sems.at[0],
        token_sems.at[1],
        {"core": 1 - core},
    )
    for i, source in enumerate((query_in, key_in)):
        loads[i].wait()
        send_edge(i, source)

    def settle(f):
        columns = pl.ds(pl.multiple_of(x * QUARTER, QUARTER), QUARTER)
        own = pltpu.make_async_copy(pads[f].at[:, columns], stage.at[f, x], own_sem)
        own.start()
        own.wait()
        for by in (1, 3, 2):
            came = stage.at[f, step(x, 4 - by)]
            copy(came, came, stage_send.at[f, by - 1], stage_recv.at[f, by - 1], {"x": x}).wait_recv()
        parts = [stage[f, i].astype(jnp.float32) for i in range(4)]
        weights[f, y, zh, x] = jnp.concatenate(parts, axis=0).astype(jnp.bfloat16)

    def ring(axis, item, send_sems, recv_sems, split=False, relayed=None):
        at = place[axis]
        plus, minus, far = step(at, 1), step(at, 3), step(at, 2)

        def out(ref, slot, to):
            send(ref, ref, send_sems(slot), recv_sems(slot), {axis: to})

        def landed(ref, slot):
            copy(ref, ref, send_sems(slot), recv_sems(slot), {axis: at}).wait_recv()

        def first():
            if split:
                out(item(at, 0), 0, plus)
                out(item(at, 1), 1, minus)
                out(item(at, 1), 4, plus)
                out(item(at, 0), 5, minus)
            else:
                out(item(at), 0, plus)
                out(item(at), 1, minus)

        def forward():
            landed(item(minus, 0 if split else None), 0)
            if relayed is None:
                out(item(minus, 0), 2, plus)
            landed(item(plus, 1 if split else None), 1)
            if relayed is None:
                out(item(plus, 1), 3, minus)

        def finish_near():
            if split:
                landed(item(minus, 1), 4)
                landed(item(plus, 0), 5)

        def finish_far():
            if relayed is None:
                landed(item(far, 0), 2)
                landed(item(far, 1), 3)
            else:
                came = item(far)
                copy(came, came, far_send.at[relayed], far_recv.at[relayed], {axis: at}).wait_recv()

        def finish():
            finish_near()
            finish_far()

        return first, forward, finish, finish_near, finish_far

    def half_columns(half):
        return slice(None) if half is None else slice(half * 512, half * 512 + 512)

    def half_blocks(half):
        return slice(None) if half is None else slice(half * 2, half * 2 + 2)

    def deep_ring(f):
        return ring(
            "zh",
            lambda i, half=None: weights.at[f, y, i, x, :, half_columns(half)],
            lambda slot: deep_send.at[f, slot],
            lambda slot: deep_recv.at[f, slot],
        )

    def unit_ring(unit, late):
        f, r = UNITS[unit]
        deep = step(zh, r)
        across = unit % 2 == 0

        def item(i, half=None):
            if late:
                if across:
                    return weights.at[f, i, deep, half_blocks(half)]
                return weights.at[f, half_blocks(half), deep, i]
            if across:
                return weights.at[f, y, deep, i, :, half_columns(half)]
            return weights.at[f, i, deep, x, :, half_columns(half)]

        base = 4 if late else 0
        return ring(
            "x" if across != late else "y",
            item,
            lambda slot: ring_send.at[unit, base + slot],
            lambda slot: ring_recv.at[unit, base + slot],
            late and unit >= 2,
            {7: 0, 6: 1}.get(unit) if late else None,
        )

    def relay_far():
        column = weights.at[1, :, zh, step(x, 2)]
        send(column, column, far_send.at[0], far_recv.at[0], {"zh": step(zh, 3)})
        strip = weights.at[1, step(y, 2), zh]
        send(strip, strip, far_send.at[1], far_recv.at[1], {"zh": step(zh, 1)})

    def open_late(unit, by):
        deep = zh
        if unit == 0:
            axis, piece = "y", weights.at[0, y, deep, step(x, by)]
        else:
            axis, piece = "x", weights.at[1, step(y, by), deep, x]
        for slot, to in ((0, 1), (1, 3)):
            send(
                piece,
                piece,
                piece_send.at[unit, by, slot],
                ring_recv.at[unit, 4 + slot],
                {axis: step(place[axis], to)},
            )

    deep = [deep_ring(f) for f in range(2)]
    early = [unit_ring(unit, False) for unit in range(8)]
    late = [unit_ring(unit, True) for unit in range(8)]

    def unit_weights(f, r, quarter):
        return weights[f, :, step(zh, r), quarter].reshape(4 * BLOCK, QUARTER)

    def quarter_dot(rows_in, quarter):
        columns = pl.ds(pl.multiple_of(quarter * QUARTER, QUARTER), QUARTER)
        return lax.dot_general(
            rows_in,
            chip_tokens[:, :, columns].reshape(2 * ROWS, QUARTER),
            (((1,), (1,)), ((), ())),
            preferred_element_type=jnp.float32,
        )

    def send_part(ref, other, i):
        send(ref, other, part_send.at[i], part_recv.at[i], {"ch": 1 - ch})

    def project(r):
        @pl.loop(0, 4)
        def _(quarter):
            part = quarter_dot(unit_weights(0, r, quarter), quarter)

            @pl.when(quarter == 0)
            def _():
                partial[r] = part

            @pl.when(quarter > 0)
            def _():
                partial[r] += part

        send_part(partial.at[r], theirs.at[r], r)

    def strip_of(by):
        return pl.ds(pl.multiple_of(step(y, by) * BLOCK, BLOCK), BLOCK)

    def project_strip(by):
        strip = strip_of(by)
        partial[2, strip, :] = summed(
            [quarter_dot(weights[0, step(y, by), step(zh, 2), q], q) for q in range(4)]
        )
        send_part(partial.at[2, strip], theirs.at[2, strip], 4 + by)

    def join(r):
        for by in range(4) if r == 2 else (None,):
            i = r if by is None else 4 + by
            came = theirs.at[r] if by is None else theirs.at[r, strip_of(by)]
            copy(came, came, part_send.at[i], part_recv.at[i], {"ch": ch}).wait_recv()
        low[r] = (partial[r] + theirs[r]).astype(jnp.bfloat16)

    def product(r, quarter):
        return lax.dot_general(
            low[r],
            unit_weights(1, r, quarter),
            (((0,), (0,)), ((), ())),
            preferred_element_type=jnp.float32,
        ).reshape(2, ROWS, QUARTER)

    def expand(r, opening):
        for quarter in range(4):
            if opening:
                total[:, quarter] = product(r, quarter)
            else:
                total[:, quarter] += product(r, quarter)

    def close(r, by):
        quarter = step(x, by)
        total[:, quarter] += product(r, quarter)
        send(
            total.at[1, quarter],
            arrived.at[quarter],
            swap_send.at[by],
            swap_recv.at[by],
            {"core": 1 - core},
        )

    def tap_of(branch, offset, group):
        start = (branch * TILES + group * 8) * 8 + offset
        return tap_rows[pl.ds(start, 8, stride=8), :]

    def mode_of(ref, n, group):
        half, row = n // 8, n % 8
        return ref[half, pl.ds(group * 64 + row, 8, stride=8), :]

    def state_of(ref, n, group):
        return ref[group // 2, n // 8, pl.ds(group % 2 * 8 + n % 8, 8, stride=16), :]

    def at_group(group):
        return pl.ds(group * 8 if isinstance(group, int) else pl.multiple_of(group * 8, 8), 8)

    def filtered(branch, target, begin=0, end=ROWS // 8, groups=range(GROUPS)):
        for group in groups:
            taps = [tap_of(branch, j, group) for j in range(TAPS)]

            @pl.loop(begin, end)
            def _(eight):
                window = [row_of(rows, eight, group, r) for r in range(-6, 8)]
                for i in range(8):
                    target(eight * 8 + i, group, short(window, taps, i))

    def prepare():
        for load in loads[2:]:
            load.wait()
        for tile in range(TILES):
            for branch in range(3):
                base = (branch * TILES + tile) * 8
                tap_rows[base : base + TAPS, :] = short_taps[branch, :, lanes_of(tile)]
            for half in range(2):
                modes = slice(half * 8, half * 8 + 8)
                rate = mode_rates[modes, lanes_of(tile)]
                rate_rows[half, tile * 8 : tile * 8 + 8, :] = rate
                weight_rows[half, tile * 8 : tile * 8 + 8, :] = (
                    residues[modes, lanes_of(tile)] * jnp.sqrt(rate)
                )

        def keep_query(t, group, result):
            queries[t, at_group(group), :] = result

        def keep_key(t, group, result):
            mixed[t, at_group(group), :] = result

        wait_edge(0)
        spread(query_in, edges.at[0], first_block, rows)
        filtered(0, keep_query)
        wait_edge(1)
        spread(key_in, edges.at[1], first_block, rows)
        filtered(1, keep_key)

    def gather_rows(pair, quarter, edge):
        where = pl.ds(pl.multiple_of(pair * 16, 16), 16)
        for tile in range(8):
            columns = lanes_of(tile)
            block = total[0, quarter, where, columns] + arrived[quarter, where, columns]
            block = block.astype(jnp.bfloat16)
            if edge:
                last[quarter, :, columns] = block[8:]
            block = block.astype(jnp.float32)
            base = pl.multiple_of((2 * pair + 1) * TILES * 8 + quarter * 64 + tile * 8, 8)
            rows[pl.ds(base, 8), :] = block[:8]
            rows[pl.ds(base + TILES * 8, 8), :] = block[8:]

    def gather_edge(by):
        quarter = step(x, by)
        came = arrived.at[quarter]
        copy(came, came, swap_send.at[by], swap_recv.at[by], {"ch": ch}).wait_recv()
        gather_rows(ROWS // 16 - 1, quarter, True)
        send(
            last.at[quarter],
            value_edges.at[quarter],
            late_send.at[by],
            late_recv.at[by],
            block_device(1),
        )

    def keep_product(t, group, result):
        product = mixed[t, at_group(group), :] * result
        mixed[t, at_group(group), :] = product.astype(jnp.bfloat16).astype(jnp.float32)

    def start_mix(by):
        group = step(x, by)
        pl.loop(0, ROWS // 16 - 1)(lambda pair: gather_rows(pair, group, False))
        filtered(2, keep_product, 1, ROWS // 8, (group,))
        summarize(group)

    def mix_first():
        from_x = block_device(127)["x"]
        for by in range(4):
            came = value_edges.at[step(from_x, by)]
            copy(came, came, late_send.at[by], late_recv.at[by], {"ch": ch}).wait_recv()
        for tile in range(TILES):
            above = value_edges[tile // 8, :, lanes_of(tile % 8)].astype(jnp.float32)
            rows[tile * 8 : tile * 8 + 8, :] = jnp.where(first_block, 0.0, above)
        filtered(2, keep_product, 0, 1)

    def decays(group):
        return [jnp.exp(-mode_of(rate_rows, n, group)) for n in range(MODES)]

    zeros = (jnp.zeros((8, LANES), jnp.float32),) * MODES

    def run_modes(group, rates, begin, end, held):
        def advance(eight, held):
            for i in range(8):
                entry = mixed[eight * 8 + i, at_group(group), :]
                held = tuple(rates[n] * held[n] + entry for n in range(MODES))
            return held

        return lax.fori_loop(begin, end, advance, held)

    def store_states(group, held):
        for n in range(MODES):
            half, part = lax.div(group, 2), lax.rem(group, 2)
            states[half, n // 8, pl.ds(part * 8 + n % 8, 8, stride=16), :] = held[n]

    def summarize(group):
        store_states(group, run_modes(group, decays(group), 1, ROWS // 8, zeros))

    def summarize_first(group):
        held = run_modes(group, decays(group), 0, 1, zeros)
        rest = [jnp.exp(-float(ROWS - 8) * mode_of(rate_rows, n, group)) for n in range(MODES)]
        store_states(
            group, [state_of(states, n, group) + rest[n] * held[n] for n in range(MODES)]
        )

    def localize(group):
        rates = decays(group)
        weighting = [mode_of(weight_rows, n, group) for n in range(MODES)]

        def advance(eight, held):
            for i in range(8):
                entry = mixed[eight * 8 + i, at_group(group), :]
                held = tuple(rates[n] * held[n] + entry for n in range(MODES))
                local[eight * 8 + i, at_group(group), :] = summed(
                    [weighting[n] * held[n] for n in range(MODES)]
                )
            return held

        lax.fori_loop(0, ROWS // 8, advance, zeros)

    def finish_group(group):
        rates = decays(group)
        skip = skip_gain[at_group(group), :]
        first = tuple(
            mode_of(weight_rows, n, group) * state_of(carried, n, group) for n in range(MODES)
        )

        def advance(eight, held):
            for i in range(8):
                held = tuple(rates[n] * held[n] for n in range(MODES))
                t = eight * 8 + i
                convolved = local[t, at_group(group), :] + summed(list(held))
                convolved = convolved.astype(jnp.bfloat16).astype(jnp.float32)
                result = queries[t, at_group(group), :] * (
                    convolved + skip * mixed[t, at_group(group), :]
                )
                out[pl.ds(eight * TILES * 8 + group * 64 + i, 8, stride=8), :] = result
            return held

        lax.fori_loop(0, ROWS // 8, advance, first)

    def near_part(at):
        return pl.ds(pl.multiple_of(at * 16, 16), 16)

    def near_rates(half):
        starts = [pl.multiple_of((2 * half + i) * 64 + near * 8, 8) for i in range(2)]
        return jnp.concatenate([rate_rows[:, pl.ds(start, 8), :] for start in starts], axis=1)

    def wait_all(buffer, sends, recvs, offsets, index):
        for by in offsets:
            came = buffer(index(by))
            copy(came, came, sends.at[by - 1], recvs.at[by - 1], {"ch": ch}).wait_recv()

    def send_near(half):
        for by in range(1, 8):
            to, device = near_device(by)
            send(
                states.at[half, :, near_part(to)],
                group_states.at[half, near],
                near_send.at[half, by - 1],
                near_recv.at[half, by - 1],
                device,
            )

    def send_across(buffer, slot, axis, half):
        own = buffer.at[half, place[axis]]
        for by in (2, 1, 3):
            send(
                own,
                own,
                scan_send.at[slot, half, by - 1],
                scan_recv.at[slot, half, by - 1],
                {axis: step(place[axis], by)},
            )

    def scan_across(buffer, slot, axis, half, decay):
        at = place[axis]
        wait_all(
            lambda i: buffer.at[half, i],
            scan_send.at[slot, half],
            scan_recv.at[slot, half],
            (1, 3, 2),
            lambda by: step(at, 4 - by),
        )
        running = jnp.zeros(decay.shape, jnp.float32)
        before = running
        for k in range(4):
            before = jnp.where(at == k, running, before)
            running = decay * running + buffer[half, k]
        return before, running

    def before_near(by):
        return lax.rem(near + 8 - by, 8)

    def scan_near(half):
        one = jnp.exp(-float(ROWS) * near_rates(half))
        group_states[half, near] = states[half, :, near_part(near), :]
        wait_all(
            lambda i: group_states.at[half, i],
            near_send.at[half],
            near_recv.at[half],
            range(1, 8),
            before_near,
        )
        held = jnp.zeros(one.shape, jnp.float32)
        for k in range(8):
            group_before[half, k] = held
            held = one * held + group_states[half, k]
        deep_states[half, zh] = held
        send_across(deep_states, 0, "zh", half)

    def scan_deep(half):
        decay = jnp.exp(-8.0 * ROWS * near_rates(half))
        before, running = scan_across(deep_states, 0, "zh", half, decay)
        wide_states[half, y] = running
        send_across(wide_states, 1, "y", half)
        return before

    def scan_wide(half, deep_before):
        rate = near_rates(half)
        one = jnp.exp(-float(ROWS) * rate)
        wide_before, _ = scan_across(wide_states, 1, "y", half, jnp.exp(-32.0 * ROWS * rate))
        shift = jnp.exp(rate * (-8.0 * ROWS * zh.astype(jnp.float32)))
        entering = deep_before + shift * wide_before
        for k in range(8):
            group_before[half, k] += entering
            entering = one * entering
        for by in range(1, 8):
            to, device = near_device(by)
            send(
                group_before.at[half, to],
                carried.at[half, :, near_part(near)],
                back_send.at[half, by - 1],
                back_recv.at[half, by - 1],
                device,
            )
        carried[half, :, near_part(near), :] = group_before[half, near]

    def wait_back(half):
        wait_all(
            lambda i: carried.at[half, :, near_part(i)],
            back_send.at[half],
            back_recv.at[half],
            range(1, 8),
            before_near,
        )

    FIRST, FORWARD, FINISH, NEAR, FAR = range(5)

    def both(rings, pair, action):
        for unit in (2 * pair, 2 * pair + 1):
            rings[unit][action]()

    settle(0)
    early[0][FIRST]()
    deep[0][FIRST]()
    open_late(0, 0)
    settle(1)
    early[1][FIRST]()
    deep[1][FIRST]()
    open_late(1, 0)
    for unit in (0, 1):
        early[unit][FORWARD]()
        open_late(unit, 1)
        open_late(unit, 3)
    deep[0][FORWARD]()
    both(early, 1, FIRST)
    for unit in (0, 1):
        early[unit][FINISH]()
        open_late(unit, 2)
    both(early, 1, FORWARD)
    deep[0][FINISH]()
    deep[1][FORWARD]()
    early[4][FIRST]()
    both(late, 0, FORWARD)
    both(early, 1, FINISH)
    deep[1][FINISH]()
    early[5][FIRST]()
    both(late, 1, FIRST)
    prepare()
    both(early, 2, FORWARD)
    both(early, 3, FIRST)
    copy(chip_tokens.at[0], chip_tokens.at[1], token_sems.at[0], token_sems.at[1], {"core": core}).wait_recv()
    both(late, 0, FINISH)
    project(0)
    relay_far()
    both(late, 1, FORWARD)
    both(early, 2, FINISH)
    both(late, 2, FIRST)
    project_strip(0)
    both(early, 3, FORWARD)
    both(late, 1, FINISH)
    project(1)
    project(3)
    both(late, 2, FORWARD)
    both(early, 3, FINISH)
    both(late, 3, FIRST)
    join(0)
    expand(0, True)
    late[4][NEAR]()
    project_strip(1)
    project_strip(3)
    late[4][FAR]()
    project_strip(2)
    late[5][FINISH]()
    join(3)
    both(late, 3, FORWARD)
    join(2)
    expand(2, False)
    join(1)
    late[6][FINISH]()
    expand(3, False)
    close(1, 0)
    late[7][FAR]()
    close(1, 2)
    late[7][NEAR]()
    close(1, 1)
    close(1, 3)
    gather_edge(0)
    gather_edge(2)
    start_mix(0)
    gather_edge(1)
    gather_edge(3)
    start_mix(2)
    start_mix(1)
    start_mix(3)
    mix_first()
    summarize_first(0)
    summarize_first(1)
    send_near(0)
    summarize_first(2)
    summarize_first(3)
    send_near(1)
    localize(0)
    localize(1)
    scan_near(0)
    localize(2)
    scan_near(1)
    localize(3)
    deep_before = [scan_deep(0)]
    deep_before.append(scan_deep(1))
    scan_wide(0, deep_before[0])
    scan_wide(1, deep_before[1])
    wait_back(0)
    finish_group(0)
    finish_group(1)
    wait_back(1)
    finish_group(2)
    finish_group(3)
    for made in started:
        made.wait_send()


def per_device(
    tokens, query_in, key_in, proj_in, proj_out, short_taps, residues, mode_rates, skip_gain
):
    f32, bf16 = jnp.float32, jnp.bfloat16
    dma = pltpu.SemaphoreType.DMA
    tiles = pl.pallas_call(
        operator_kernel,
        out_shape=jax.ShapeDtypeStruct((ROWS * TILES, LANES), f32),
        in_specs=[pl.BlockSpec(memory_space=pl.ANY)]
        + [pl.BlockSpec(memory_space=pltpu.VMEM)] * 2
        + [pl.BlockSpec(memory_space=pl.ANY)] * 6,
        out_specs=pl.BlockSpec(memory_space=pltpu.VMEM),
        scratch_shapes=[
            pltpu.VMEM((ROWS, WIDE), bf16),
            pltpu.VMEM((ROWS, WIDE), bf16),
            pltpu.VMEM((3, TAPS, WIDE), f32),
            pltpu.VMEM((MODES, WIDE), f32),
            pltpu.VMEM((MODES, WIDE), f32),
            pltpu.VMEM((TILES, LANES), f32),
            pltpu.VMEM((4, 8, QUARTER), bf16),
            pltpu.VMEM((4, 8, QUARTER), bf16),
            pltpu.VMEM((2, ROWS, WIDE), bf16),
            pltpu.VMEM((2, 4, RANKS, QUARTER), bf16),
            pltpu.VMEM((2, 4, 4, 4, BLOCK, QUARTER), bf16),
            pltpu.VMEM((4, 4 * BLOCK, 2 * ROWS), f32),
            pltpu.VMEM((4, 4 * BLOCK, 2 * ROWS), f32),
            pltpu.VMEM((4, 4 * BLOCK, 2 * ROWS), bf16),
            pltpu.VMEM((2, 4, ROWS, QUARTER), f32),
            pltpu.VMEM((4, ROWS, QUARTER), f32),
            pltpu.VMEM((2, 8, WIDE), bf16),
            pltpu.VMEM(((ROWS + 8) * TILES, LANES), f32),
            pltpu.VMEM((3 * TILES * 8, LANES), f32),
            pltpu.VMEM((2, TILES * 8, LANES), f32),
            pltpu.VMEM((2, TILES * 8, LANES), f32),
            pltpu.VMEM((ROWS, TILES, LANES), f32),
            pltpu.VMEM((ROWS, TILES, LANES), f32),
            pltpu.VMEM((ROWS, TILES, LANES), f32),
            pltpu.VMEM((2, 2, TILES * 4, LANES), f32),
            pltpu.VMEM((2, 2, TILES * 4, LANES), f32),
            pltpu.VMEM((2, 8, 2, 16, LANES), f32),
            pltpu.VMEM((2, 8, 2, 16, LANES), f32),
            pltpu.VMEM((2, 4, 2, 16, LANES), f32),
            pltpu.VMEM((2, 4, 2, 16, LANES), f32),
            dma,
            dma((6,)),
            dma((2,)),
            dma((2, 3)),
            dma((2, 3)),
            dma((2, 4)),
            dma((2, 4)),
            dma((8, 10)),
            dma((8, 10)),
            dma((2, 4, 2)),
            dma((2,)),
            dma((2,)),
            dma((8,)),
            dma((8,)),
            dma((4,)),
            dma((4,)),
            dma((2,)),
            dma((2,)),
            dma((4,)),
            dma((4,)),
            dma((2, 7)),
            dma((2, 7)),
            dma((2, 2, 3)),
            dma((2, 2, 3)),
            dma((2, 7)),
            dma((2, 7)),
        ],
        compiler_params=pltpu.CompilerParams(
            collective_id=0, has_side_effects=True, vmem_limit_bytes=60 * 2**20
        ),
    )(
        tokens,
        proj_in.T,
        proj_out,
        query_in,
        key_in,
        short_taps,
        residues,
        mode_rates,
        skip_gain.reshape(TILES, LANES),
    )
    tiles = tiles.reshape(ROWS // 8, TILES, 8, LANES).transpose(0, 2, 1, 3)
    return tiles.reshape(ROWS, WIDE).astype(bf16)


def solution(mesh):
    split = Mesh(mesh.devices.reshape(4, 4, 4, 2, 2), ("y", "zh", "x", "core", "ch"))
    both = P(SEQ_AXES, "ch")
    placed = (
        both,
        both,
        both,
        P("ch", SEQ_AXES),
        both,
        P(None, None, "ch"),
        P(None, "ch"),
        P(None, "ch"),
        P("ch"),
    )
    return jax.shard_map(
        per_device, mesh=split, in_specs=placed, out_specs=both, check_vma=False
    )
```

```python
import jax
import jax.numpy as jnp
from jax import lax
from jax.experimental import pallas as pl
from jax.experimental.pallas import tpu as pltpu
from jax.sharding import Mesh
from jax.sharding import PartitionSpec as P

ROWS = 128
WIDE = 4096
LANES = 128
TILES = WIDE // LANES
GROUPS = TILES // 8
MODES = 16
TAPS = 7
SEQ_AXES = ("y", "zh", "x", "core")
MESH = pl.DeviceIdType.MESH
BLOCK = 48
QUARTER = 1024
RANKS = 12
UNITS = ((0, 0), (1, 0), (0, 1), (0, 3), (0, 2), (1, 2), (1, 3), (1, 1))


def lanes_of(tile):
    return slice(tile * LANES, (tile + 1) * LANES)


def spread_edge(edge, first_block, scratch):
    for tile in range(TILES):
        above = edge[:, lanes_of(tile)].astype(jnp.float32)
        scratch[tile * 8 : tile * 8 + 8, :] = jnp.where(first_block, 0.0, above)


def spread(source, edge, first_block, scratch):
    spread_edge(edge, first_block, scratch)

    @pl.loop(0, ROWS // 16)
    def _(pair):
        for tile in range(TILES):
            rows = pl.ds(pl.multiple_of(pair * 16, 16), 16)
            block = source[rows, lanes_of(tile)].astype(jnp.float32)
            base = pl.multiple_of((2 * pair + 1) * TILES * 8 + tile * 8, 8)
            scratch[pl.ds(base, 8), :] = block[:8]
            scratch[pl.ds(base + TILES * 8, 8), :] = block[8:]


def row_of(scratch, eight, group, row):
    start = (eight + (1 if row >= 0 else 0)) * TILES * 8 + group * 64 + row % 8
    return scratch[pl.ds(start, 8, stride=8), :]


def short(rows, taps, step):
    result = taps[0] * rows[step + 6]
    for offset in range(1, TAPS):
        result = result + taps[offset] * rows[step + 6 - offset]
    return result


def summed(terms):
    while len(terms) > 1:
        terms = [terms[i] + terms[i + 1] for i in range(0, len(terms), 2)]
    return terms[0]


def operator_kernel(
    tokens,
    pad_in,
    pad_out,
    query_far,
    key_far,
    taps_far,
    residues_far,
    rates_far,
    skip_far,
    out,
    query_in,
    key_in,
    short_taps,
    residues,
    mode_rates,
    skip_gain,
    last,
    value_edges,
    chip_tokens,
    stage,
    weights,
    partial,
    theirs,
    low,
    total,
    arrived,
    edges,
    rows,
    tap_rows,
    rate_rows,
    weight_rows,
    queries,
    mixed,
    local,
    states,
    carried,
    group_states,
    group_before,
    deep_states,
    wide_states,
    own_sem,
    load_sems,
    token_sems,
    stage_send,
    stage_recv,
    deep_send,
    deep_recv,
    ring_send,
    ring_recv,
    piece_send,
    far_send,
    far_recv,
    part_send,
    part_recv,
    swap_send,
    swap_recv,
    edge_send,
    edge_recv,
    late_send,
    late_recv,
    near_send,
    near_recv,
    scan_send,
    scan_recv,
    back_send,
    back_recv,
):
    y, zh, x = lax.axis_index("y"), lax.axis_index("zh"), lax.axis_index("x")
    core, ch = lax.axis_index("core"), lax.axis_index("ch")
    place = {"x": x, "y": y, "zh": zh}
    pads = (pad_in, pad_out)
    started = []
    near = x * 2 + core
    block_at = (y * 4 + zh) * 8 + near
    first_block = block_at == 0

    def step(position, by):
        return lax.rem(position + by, 4)

    def copy(source, target, send, recv, device):
        return pltpu.make_async_remote_copy(
            src_ref=source,
            dst_ref=target,
            send_sem=send,
            recv_sem=recv,
            device_id=device,
            device_id_type=MESH,
        )

    def send(*arguments):
        made = copy(*arguments)
        made.start()
        started.append(made)

    def near_device(by):
        to = lax.rem(near + by, 8)
        return to, {"x": to // 2, "core": lax.rem(to, 2)}

    def block_device(by):
        to = lax.rem(block_at + by, 128)
        return {
            "y": to // 32,
            "zh": lax.rem(to // 8, 4),
            "x": lax.rem(to // 2, 4),
            "core": lax.rem(to, 2),
        }

    def send_edge(i, source):
        send(
            source.at[pl.ds(ROWS - 8, 8)],
            edges.at[i],
            edge_send.at[i],
            edge_recv.at[i],
            block_device(1),
        )

    def wait_edge(i):
        edge = edges.at[i]
        copy(edge, edge, edge_send.at[i], edge_recv.at[i], {"ch": ch}).wait_recv()

    own_copy = pltpu.make_async_copy(tokens, chip_tokens.at[0], own_sem)
    own_copy.start()
    loads = [
        pltpu.make_async_copy(source, target, load_sems.at[i])
        for i, (source, target) in enumerate(
            (
                (query_far, query_in),
                (key_far, key_in),
                (taps_far, short_taps),
                (residues_far, residues),
                (rates_far, mode_rates),
                (skip_far, skip_gain),
            )
        )
    ]
    for load in loads:
        load.start()
    barrier = pltpu.get_barrier_semaphore()
    greeted = [{"ch": 1 - ch}, block_device(1), block_device(127)]
    greeted += [near_device(by)[1] for by in range(1, 8)]
    greeted += [{axis: step(place[axis], by)} for axis in ("zh", "y") for by in (1, 2, 3)]
    for device in greeted:
        pl.semaphore_signal(barrier, inc=1, device_id=device, device_id_type=MESH)
    pl.semaphore_wait(barrier, len(greeted))

    for f in range(2):
        for by in (1, 3, 2):
            to = step(x, by)
            columns = pl.ds(pl.multiple_of(to * QUARTER, QUARTER), QUARTER)
            send(
                pads[f].at[:, columns],
                stage.at[f, x],
                stage_send.at[f, by - 1],
                stage_recv.at[f, by - 1],
                {"x": to},
            )
    own_copy.wait()
    send(
        chip_tokens.at[0],
        chip_tokens.at[1],
        token_sems.at[0],
        token_sems.at[1],
        {"core": 1 - core},
    )
    for i, source in enumerate((query_in, key_in)):
        loads[i].wait()
        send_edge(i, source)

    def settle(f):
        columns = pl.ds(pl.multiple_of(x * QUARTER, QUARTER), QUARTER)
        own = pltpu.make_async_copy(pads[f].at[:, columns], stage.at[f, x], own_sem)
        own.start()
        own.wait()
        for by in (1, 3, 2):
            came = stage.at[f, step(x, 4 - by)]
            copy(came, came, stage_send.at[f, by - 1], stage_recv.at[f, by - 1], {"x": x}).wait_recv()
        parts = [stage[f, i].astype(jnp.float32) for i in range(4)]
        weights[f, y, zh, x] = jnp.concatenate(parts, axis=0).astype(jnp.bfloat16)

    def ring(axis, item, send_sems, recv_sems, split=False, relayed=None):
        at = place[axis]
        plus, minus, far = step(at, 1), step(at, 3), step(at, 2)

        def out(ref, slot, to):
            send(ref, ref, send_sems(slot), recv_sems(slot), {axis: to})

        def landed(ref, slot):
            copy(ref, ref, send_sems(slot), recv_sems(slot), {axis: at}).wait_recv()

        def first():
            if split:
                out(item(at, 0), 0, plus)
                out(item(at, 1), 1, minus)
                out(item(at, 1), 4, plus)
                out(item(at, 0), 5, minus)
            else:
                out(item(at), 0, plus)
                out(item(at), 1, minus)

        def forward():
            landed(item(minus, 0 if split else None), 0)
            if relayed is None:
                out(item(minus, 0), 2, plus)
            landed(item(plus, 1 if split else None), 1)
            if relayed is None:
                out(item(plus, 1), 3, minus)

        def finish_near():
            if split:
                landed(item(minus, 1), 4)
                landed(item(plus, 0), 5)

        def finish_far():
            if relayed is None:
                landed(item(far, 0), 2)
                landed(item(far, 1), 3)
            else:
                came = item(far)
                copy(came, came, far_send.at[relayed], far_recv.at[relayed], {axis: at}).wait_recv()

        def finish():
            finish_near()
            finish_far()

        return first, forward, finish, finish_near, finish_far

    def half_columns(half):
        return slice(None) if half is None else slice(half * 512, half * 512 + 512)

    def half_blocks(half):
        return slice(None) if half is None else slice(half * 2, half * 2 + 2)

    def deep_ring(f):
        return ring(
            "zh",
            lambda i, half=None: weights.at[f, y, i, x, :, half_columns(half)],
            lambda slot: deep_send.at[f, slot],
            lambda slot: deep_recv.at[f, slot],
        )

    def unit_ring(unit, late):
        f, r = UNITS[unit]
        deep = step(zh, r)
        across = unit % 2 == 0

        def item(i, half=None):
            if late:
                if across:
                    return weights.at[f, i, deep, half_blocks(half)]
                return weights.at[f, half_blocks(half), deep, i]
            if across:
                return weights.at[f, y, deep, i, :, half_columns(half)]
            return weights.at[f, i, deep, x, :, half_columns(half)]

        base = 4 if late else 0
        return ring(
            "x" if across != late else "y",
            item,
            lambda slot: ring_send.at[unit, base + slot],
            lambda slot: ring_recv.at[unit, base + slot],
            late and unit >= 2,
            {7: 0, 6: 1}.get(unit) if late else None,
        )

    def relay_far():
        column = weights.at[1, :, zh, step(x, 2)]
        send(column, column, far_send.at[0], far_recv.at[0], {"zh": step(zh, 3)})
        strip = weights.at[1, step(y, 2), zh]
        send(strip, strip, far_send.at[1], far_recv.at[1], {"zh": step(zh, 1)})

    def open_late(unit, by):
        deep = zh
        if unit == 0:
            axis, piece = "y", weights.at[0, y, deep, step(x, by)]
        else:
            axis, piece = "x", weights.at[1, step(y, by), deep, x]
        for slot, to in ((0, 1), (1, 3)):
            send(
                piece,
                piece,
                piece_send.at[unit, by, slot],
                ring_recv.at[unit, 4 + slot],
                {axis: step(place[axis], to)},
            )

    deep = [deep_ring(f) for f in range(2)]
    early = [unit_ring(unit, False) for unit in range(8)]
    late = [unit_ring(unit, True) for unit in range(8)]

    def unit_weights(f, r, quarter):
        return weights[f, :, step(zh, r), quarter].reshape(4 * BLOCK, QUARTER)

    def quarter_dot(rows_in, quarter):
        columns = pl.ds(pl.multiple_of(quarter * QUARTER, QUARTER), QUARTER)
        return lax.dot_general(
            rows_in,
            chip_tokens[:, :, columns].reshape(2 * ROWS, QUARTER),
            (((1,), (1,)), ((), ())),
            preferred_element_type=jnp.float32,
        )

    def send_part(ref, other, i):
        send(ref, other, part_send.at[i], part_recv.at[i], {"ch": 1 - ch})

    def project(r):
        @pl.loop(0, 4)
        def _(quarter):
            part = quarter_dot(unit_weights(0, r, quarter), quarter)

            @pl.when(quarter == 0)
            def _():
                partial[r] = part

            @pl.when(quarter > 0)
            def _():
                partial[r] += part

        send_part(partial.at[r], theirs.at[r], r)

    def strip_of(by):
        return pl.ds(pl.multiple_of(step(y, by) * BLOCK, BLOCK), BLOCK)

    def project_strip(by):
        strip = strip_of(by)
        partial[2, strip, :] = summed(
            [quarter_dot(weights[0, step(y, by), step(zh, 2), q], q) for q in range(4)]
        )
        send_part(partial.at[2, strip], theirs.at[2, strip], 4 + by)

    def join(r):
        for by in range(4) if r == 2 else (None,):
            i = r if by is None else 4 + by
            came = theirs.at[r] if by is None else theirs.at[r, strip_of(by)]
            copy(came, came, part_send.at[i], part_recv.at[i], {"ch": ch}).wait_recv()
        low[r] = (partial[r] + theirs[r]).astype(jnp.bfloat16)

    def product(r, quarter):
        return lax.dot_general(
            low[r],
            unit_weights(1, r, quarter),
            (((0,), (0,)), ((), ())),
            preferred_element_type=jnp.float32,
        ).reshape(2, ROWS, QUARTER)

    def expand(r, opening):
        for quarter in range(4):
            if opening:
                total[:, quarter] = product(r, quarter)
            else:
                total[:, quarter] += product(r, quarter)

    def close(units, by):
        quarter = step(x, by)
        total[:, quarter] += summed([product(r, quarter) for r in units])
        send(
            total.at[1, quarter],
            arrived.at[quarter],
            swap_send.at[by],
            swap_recv.at[by],
            {"core": 1 - core},
        )

    def tap_of(branch, offset, group):
        start = (branch * TILES + group * 8) * 8 + offset
        return tap_rows[pl.ds(start, 8, stride=8), :]

    def mode_of(ref, n, group):
        half, row = n // 8, n % 8
        return ref[half, pl.ds(group * 64 + row, 8, stride=8), :]

    def state_of(ref, n, group):
        return ref[group // 2, n // 8, pl.ds(group % 2 * 8 + n % 8, 8, stride=16), :]

    def at_group(group):
        return pl.ds(group * 8 if isinstance(group, int) else pl.multiple_of(group * 8, 8), 8)

    def filtered(branch, target, begin=0, end=ROWS // 8, groups=range(GROUPS)):
        for group in groups:
            taps = [tap_of(branch, j, group) for j in range(TAPS)]

            @pl.loop(begin, end)
            def _(eight):
                window = [row_of(rows, eight, group, r) for r in range(-6, 8)]
                for i in range(8):
                    target(eight * 8 + i, group, short(window, taps, i))

    def prepare():
        for load in loads[2:]:
            load.wait()
        for tile in range(TILES):
            for branch in range(3):
                base = (branch * TILES + tile) * 8
                tap_rows[base : base + TAPS, :] = short_taps[branch, :, lanes_of(tile)]
            for half in range(2):
                modes = slice(half * 8, half * 8 + 8)
                rate = mode_rates[modes, lanes_of(tile)]
                rate_rows[half, tile * 8 : tile * 8 + 8, :] = rate
                weight_rows[half, tile * 8 : tile * 8 + 8, :] = (
                    residues[modes, lanes_of(tile)] * jnp.sqrt(rate)
                )

        def keep_query(t, group, result):
            queries[t, at_group(group), :] = result

        def keep_key(t, group, result):
            mixed[t, at_group(group), :] = result

        wait_edge(0)
        spread(query_in, edges.at[0], first_block, rows)
        filtered(0, keep_query)
        wait_edge(1)
        spread(key_in, edges.at[1], first_block, rows)
        filtered(1, keep_key)

    def gather_rows(pair, quarter, edge):
        where = pl.ds(pl.multiple_of(pair * 16, 16), 16)
        for tile in range(8):
            columns = lanes_of(tile)
            block = total[0, quarter, where, columns] + arrived[quarter, where, columns]
            block = block.astype(jnp.bfloat16)
            if edge:
                last[quarter, :, columns] = block[8:]
            block = block.astype(jnp.float32)
            base = pl.multiple_of((2 * pair + 1) * TILES * 8 + quarter * 64 + tile * 8, 8)
            rows[pl.ds(base, 8), :] = block[:8]
            rows[pl.ds(base + TILES * 8, 8), :] = block[8:]

    def gather_edge(by):
        quarter = step(x, by)
        came = arrived.at[quarter]
        copy(came, came, swap_send.at[by], swap_recv.at[by], {"ch": ch}).wait_recv()
        gather_rows(ROWS // 16 - 1, quarter, True)
        send(
            last.at[quarter],
            value_edges.at[quarter],
            late_send.at[by],
            late_recv.at[by],
            block_device(1),
        )

    def keep_product(t, group, result):
        product = mixed[t, at_group(group), :] * result
        mixed[t, at_group(group), :] = product.astype(jnp.bfloat16).astype(jnp.float32)

    def start_mix(by):
        group = step(x, by)
        pl.loop(0, ROWS // 16 - 1)(lambda pair: gather_rows(pair, group, False))
        filtered(2, keep_product, 1, ROWS // 8, (group,))
        summarize(group)

    def mix_first():
        from_x = block_device(127)["x"]
        for by in range(4):
            came = value_edges.at[step(from_x, by)]
            copy(came, came, late_send.at[by], late_recv.at[by], {"ch": ch}).wait_recv()
        for tile in range(TILES):
            above = value_edges[tile // 8, :, lanes_of(tile % 8)].astype(jnp.float32)
            rows[tile * 8 : tile * 8 + 8, :] = jnp.where(first_block, 0.0, above)
        filtered(2, keep_product, 0, 1)

    def decays(group):
        return [jnp.exp(-mode_of(rate_rows, n, group)) for n in range(MODES)]

    zeros = (jnp.zeros((8, LANES), jnp.float32),) * MODES

    def run_modes(group, rates, begin, end, held):
        def advance(eight, held):
            for i in range(8):
                entry = mixed[eight * 8 + i, at_group(group), :]
                held = tuple(rates[n] * held[n] + entry for n in range(MODES))
            return held

        return lax.fori_loop(begin, end, advance, held)

    def store_states(group, held):
        for n in range(MODES):
            half, part = lax.div(group, 2), lax.rem(group, 2)
            states[half, n // 8, pl.ds(part * 8 + n % 8, 8, stride=16), :] = held[n]

    def summarize(group):
        store_states(group, run_modes(group, decays(group), 1, ROWS // 8, zeros))

    def summarize_first(group):
        held = run_modes(group, decays(group), 0, 1, zeros)
        rest = [jnp.exp(-float(ROWS - 8) * mode_of(rate_rows, n, group)) for n in range(MODES)]
        store_states(
            group, [state_of(states, n, group) + rest[n] * held[n] for n in range(MODES)]
        )

    def localize(group):
        rates = decays(group)
        weighting = [mode_of(weight_rows, n, group) for n in range(MODES)]

        def advance(eight, held):
            for i in range(8):
                entry = mixed[eight * 8 + i, at_group(group), :]
                held = tuple(rates[n] * held[n] + entry for n in range(MODES))
                local[eight * 8 + i, at_group(group), :] = summed(
                    [weighting[n] * held[n] for n in range(MODES)]
                )
            return held

        lax.fori_loop(0, ROWS // 8, advance, zeros)

    def finish_group(group):
        rates = decays(group)
        skip = skip_gain[at_group(group), :]
        first = tuple(
            mode_of(weight_rows, n, group) * state_of(carried, n, group) for n in range(MODES)
        )

        def advance(eight, held):
            for i in range(8):
                held = tuple(rates[n] * held[n] for n in range(MODES))
                t = eight * 8 + i
                convolved = local[t, at_group(group), :] + summed(list(held))
                convolved = convolved.astype(jnp.bfloat16).astype(jnp.float32)
                result = queries[t, at_group(group), :] * (
                    convolved + skip * mixed[t, at_group(group), :]
                )
                out[pl.ds(eight * TILES * 8 + group * 64 + i, 8, stride=8), :] = result
            return held

        lax.fori_loop(0, ROWS // 8, advance, first)

    def near_part(at):
        return pl.ds(pl.multiple_of(at * 16, 16), 16)

    def near_rates(half):
        starts = [pl.multiple_of((2 * half + i) * 64 + near * 8, 8) for i in range(2)]
        return jnp.concatenate([rate_rows[:, pl.ds(start, 8), :] for start in starts], axis=1)

    def wait_all(buffer, sends, recvs, offsets, index):
        for by in offsets:
            came = buffer(index(by))
            copy(came, came, sends.at[by - 1], recvs.at[by - 1], {"ch": ch}).wait_recv()

    def send_near(half):
        for by in range(1, 8):
            to, device = near_device(by)
            send(
                states.at[half, :, near_part(to)],
                group_states.at[half, near],
                near_send.at[half, by - 1],
                near_recv.at[half, by - 1],
                device,
            )

    def send_across(buffer, slot, axis, half):
        own = buffer.at[half, place[axis]]
        for by in (2, 1, 3):
            send(
                own,
                own,
                scan_send.at[slot, half, by - 1],
                scan_recv.at[slot, half, by - 1],
                {axis: step(place[axis], by)},
            )

    def scan_across(buffer, slot, axis, half, decay):
        at = place[axis]
        wait_all(
            lambda i: buffer.at[half, i],
            scan_send.at[slot, half],
            scan_recv.at[slot, half],
            (1, 3, 2),
            lambda by: step(at, 4 - by),
        )
        running = jnp.zeros(decay.shape, jnp.float32)
        before = running
        for k in range(4):
            before = jnp.where(at == k, running, before)
            running = decay * running + buffer[half, k]
        return before, running

    def before_near(by):
        return lax.rem(near + 8 - by, 8)

    def scan_near(half):
        one = jnp.exp(-float(ROWS) * near_rates(half))
        group_states[half, near] = states[half, :, near_part(near), :]
        wait_all(
            lambda i: group_states.at[half, i],
            near_send.at[half],
            near_recv.at[half],
            range(1, 8),
            before_near,
        )
        held = jnp.zeros(one.shape, jnp.float32)
        for k in range(8):
            group_before[half, k] = held
            held = one * held + group_states[half, k]
        deep_states[half, zh] = held
        send_across(deep_states, 0, "zh", half)

    def scan_deep(half):
        decay = jnp.exp(-8.0 * ROWS * near_rates(half))
        before, running = scan_across(deep_states, 0, "zh", half, decay)
        wide_states[half, y] = running
        send_across(wide_states, 1, "y", half)
        return before

    def scan_wide(half, deep_before):
        rate = near_rates(half)
        one = jnp.exp(-float(ROWS) * rate)
        wide_before, _ = scan_across(wide_states, 1, "y", half, jnp.exp(-32.0 * ROWS * rate))
        shift = jnp.exp(rate * (-8.0 * ROWS * zh.astype(jnp.float32)))
        entering = deep_before + shift * wide_before
        for k in range(8):
            group_before[half, k] += entering
            entering = one * entering
        for by in range(1, 8):
            to, device = near_device(by)
            send(
                group_before.at[half, to],
                carried.at[half, :, near_part(near)],
                back_send.at[half, by - 1],
                back_recv.at[half, by - 1],
                device,
            )
        carried[half, :, near_part(near), :] = group_before[half, near]

    def wait_back(half):
        wait_all(
            lambda i: carried.at[half, :, near_part(i)],
            back_send.at[half],
            back_recv.at[half],
            range(1, 8),
            before_near,
        )

    FIRST, FORWARD, FINISH, NEAR, FAR = range(5)

    def both(rings, pair, action):
        for unit in (2 * pair, 2 * pair + 1):
            rings[unit][action]()

    settle(0)
    early[0][FIRST]()
    deep[0][FIRST]()
    open_late(0, 0)
    settle(1)
    early[1][FIRST]()
    deep[1][FIRST]()
    open_late(1, 0)
    for unit in (0, 1):
        early[unit][FORWARD]()
        open_late(unit, 1)
        open_late(unit, 3)
    deep[0][FORWARD]()
    both(early, 1, FIRST)
    for unit in (0, 1):
        early[unit][FINISH]()
        open_late(unit, 2)
    both(early, 1, FORWARD)
    deep[0][FINISH]()
    deep[1][FORWARD]()
    early[4][FIRST]()
    both(late, 0, FORWARD)
    both(early, 1, FINISH)
    deep[1][FINISH]()
    early[5][FIRST]()
    both(late, 1, FIRST)
    prepare()
    both(early, 2, FORWARD)
    both(early, 3, FIRST)
    copy(chip_tokens.at[0], chip_tokens.at[1], token_sems.at[0], token_sems.at[1], {"core": core}).wait_recv()
    both(late, 0, FINISH)
    project(0)
    relay_far()
    both(late, 1, FORWARD)
    both(early, 2, FINISH)
    both(late, 2, FIRST)
    project_strip(0)
    both(early, 3, FORWARD)
    both(late, 1, FINISH)
    project(1)
    project(3)
    both(late, 2, FORWARD)
    both(early, 3, FINISH)
    both(late, 3, FIRST)
    join(0)
    expand(0, True)
    late[4][NEAR]()
    project_strip(1)
    project_strip(3)
    late[4][FAR]()
    project_strip(2)
    late[5][FINISH]()
    join(3)
    both(late, 3, FORWARD)
    join(2)
    expand(2, False)
    join(1)
    late[6][FINISH]()
    close((3, 1), 0)
    late[7][FAR]()
    close((3, 1), 2)
    late[7][NEAR]()
    close((3, 1), 1)
    close((3, 1), 3)
    gather_edge(0)
    gather_edge(2)
    start_mix(0)
    gather_edge(1)
    gather_edge(3)
    start_mix(2)
    start_mix(1)
    start_mix(3)
    mix_first()
    summarize_first(0)
    summarize_first(1)
    send_near(0)
    summarize_first(2)
    summarize_first(3)
    send_near(1)
    localize(0)
    localize(1)
    scan_near(0)
    localize(2)
    scan_near(1)
    localize(3)
    deep_before = [scan_deep(0)]
    deep_before.append(scan_deep(1))
    scan_wide(0, deep_before[0])
    scan_wide(1, deep_before[1])
    wait_back(0)
    finish_group(0)
    finish_group(1)
    wait_back(1)
    finish_group(2)
    finish_group(3)
    for made in started:
        made.wait_send()


def per_device(
    tokens, query_in, key_in, proj_in, proj_out, short_taps, residues, mode_rates, skip_gain
):
    f32, bf16 = jnp.float32, jnp.bfloat16
    dma = pltpu.SemaphoreType.DMA
    tiles = pl.pallas_call(
        operator_kernel,
        out_shape=jax.ShapeDtypeStruct((ROWS * TILES, LANES), f32),
        in_specs=[pl.BlockSpec(memory_space=pl.ANY)]
        + [pl.BlockSpec(memory_space=pltpu.VMEM)] * 2
        + [pl.BlockSpec(memory_space=pl.ANY)] * 6,
        out_specs=pl.BlockSpec(memory_space=pltpu.VMEM),
        scratch_shapes=[
            pltpu.VMEM((ROWS, WIDE), bf16),
            pltpu.VMEM((ROWS, WIDE), bf16),
            pltpu.VMEM((3, TAPS, WIDE), f32),
            pltpu.VMEM((MODES, WIDE), f32),
            pltpu.VMEM((MODES, WIDE), f32),
            pltpu.VMEM((TILES, LANES), f32),
            pltpu.VMEM((4, 8, QUARTER), bf16),
            pltpu.VMEM((4, 8, QUARTER), bf16),
            pltpu.VMEM((2, ROWS, WIDE), bf16),
            pltpu.VMEM((2, 4, RANKS, QUARTER), bf16),
            pltpu.VMEM((2, 4, 4, 4, BLOCK, QUARTER), bf16),
            pltpu.VMEM((4, 4 * BLOCK, 2 * ROWS), f32),
            pltpu.VMEM((4, 4 * BLOCK, 2 * ROWS), f32),
            pltpu.VMEM((4, 4 * BLOCK, 2 * ROWS), bf16),
            pltpu.VMEM((2, 4, ROWS, QUARTER), f32),
            pltpu.VMEM((4, ROWS, QUARTER), f32),
            pltpu.VMEM((2, 8, WIDE), bf16),
            pltpu.VMEM(((ROWS + 8) * TILES, LANES), f32),
            pltpu.VMEM((3 * TILES * 8, LANES), f32),
            pltpu.VMEM((2, TILES * 8, LANES), f32),
            pltpu.VMEM((2, TILES * 8, LANES), f32),
            pltpu.VMEM((ROWS, TILES, LANES), f32),
            pltpu.VMEM((ROWS, TILES, LANES), f32),
            pltpu.VMEM((ROWS, TILES, LANES), f32),
            pltpu.VMEM((2, 2, TILES * 4, LANES), f32),
            pltpu.VMEM((2, 2, TILES * 4, LANES), f32),
            pltpu.VMEM((2, 8, 2, 16, LANES), f32),
            pltpu.VMEM((2, 8, 2, 16, LANES), f32),
            pltpu.VMEM((2, 4, 2, 16, LANES), f32),
            pltpu.VMEM((2, 4, 2, 16, LANES), f32),
            dma,
            dma((6,)),
            dma((2,)),
            dma((2, 3)),
            dma((2, 3)),
            dma((2, 4)),
            dma((2, 4)),
            dma((8, 10)),
            dma((8, 10)),
            dma((2, 4, 2)),
            dma((2,)),
            dma((2,)),
            dma((8,)),
            dma((8,)),
            dma((4,)),
            dma((4,)),
            dma((2,)),
            dma((2,)),
            dma((4,)),
            dma((4,)),
            dma((2, 7)),
            dma((2, 7)),
            dma((2, 2, 3)),
            dma((2, 2, 3)),
            dma((2, 7)),
            dma((2, 7)),
        ],
        compiler_params=pltpu.CompilerParams(
            collective_id=0, has_side_effects=True, vmem_limit_bytes=60 * 2**20
        ),
    )(
        tokens,
        proj_in.T,
        proj_out,
        query_in,
        key_in,
        short_taps,
        residues,
        mode_rates,
        skip_gain.reshape(TILES, LANES),
    )
    tiles = tiles.reshape(ROWS // 8, TILES, 8, LANES).transpose(0, 2, 1, 3)
    return tiles.reshape(ROWS, WIDE).astype(bf16)


def solution(mesh):
    split = Mesh(mesh.devices.reshape(4, 4, 4, 2, 2), ("y", "zh", "x", "core", "ch"))
    both = P(SEQ_AXES, "ch")
    placed = (
        both,
        both,
        both,
        P("ch", SEQ_AXES),
        both,
        P(None, None, "ch"),
        P(None, "ch"),
        P(None, "ch"),
        P("ch"),
    )
    return jax.shard_map(
        per_device, mesh=split, in_specs=placed, out_specs=both, check_vma=False
    )
```
